8 devices in a mesh: ep: 2 (over z, y), dp: 4 (over x, core).
Axes of the slice: x: 2, y: 2, z: 1, core: 2. Of those that a mesh axis runs over, the one named last changes fastest.
Arguments:
- tokens: bfloat16 [4096, 512], P(('dp', 'ep'))
- dy_out: bfloat16 [4096, 512], P(('dp', 'ep'))
- dense_w1: bfloat16 [512, 512], replicated
- route_idx1: int32 [4096, 8], P(('dp', 'ep'))
- route_gate1: float32 [4096, 8], P(('dp', 'ep'))
- w_gate1: bfloat16 [128, 512, 192], P('ep')
- w_up1: bfloat16 [128, 512, 192], P('ep')
- w_down1: bfloat16 [128, 192, 512], P('ep')
- dense_w2: bfloat16 [512, 512], replicated
- route_idx2: int32 [4096, 8], P(('dp', 'ep'))
- route_gate2: float32 [4096, 8], P(('dp', 'ep'))
- w_gate2: bfloat16 [128, 512, 192], P('ep')
- w_up2: bfloat16 [128, 512, 192], P('ep')
- w_down2: bfloat16 [128, 192, 512], P('ep')
Outputs:
- output 1: bfloat16 [4096, 512], P(('dp', 'ep'))
- output 2: bfloat16 [512, 512], P(('dp', 'ep'))
- output 3: bfloat16 [128, 512, 192], P('ep', 'dp')
- output 4: bfloat16 [128, 512, 192], P('ep', 'dp')
- output 5: bfloat16 [128, 192, 512], P('ep', None, 'dp')
- output 6: bfloat16 [512, 512], P(('dp', 'ep'))
- output 7: bfloat16 [128, 512, 192], P('ep', 'dp')
- output 8: bfloat16 [128, 512, 192], P('ep', 'dp')
- output 9: bfloat16 [128, 192, 512], P('ep', None, 'dp')
All inputs are finite; a program needn't handle non-finite values.
Results may differ from the reference program's by a relative error of at most 0.02.
Values are sent between devices in bfloat16 or wider.
A program may use at most 1 GiB of HBM per device.

```python
import jax
import jax.numpy as jnp

TOK = 512
D = 512
FF = 192
EXPERTS = 128
TOP = 8
SOURCES = 8
BASE = TOK * TOP // EXPERTS
CAPACITY = 2 * BASE


def draw_routing(key):
    key_tok, key_exp, key_shift = jax.random.split(key, 3)
    tok_order = jax.vmap(lambda src_key: jax.random.permutation(src_key, TOK))(jax.random.split(key_tok, SOURCES))
    exp_order = jax.vmap(lambda src_key: jax.random.permutation(src_key, EXPERTS))(jax.random.split(key_exp, SOURCES))
    shift = jax.random.randint(key_shift, (SOURCES, EXPERTS // 2), 0, BASE // 2 + 1, dtype=jnp.int32)
    shift = shift.at[:, 0].set(BASE)
    sizes = jnp.stack([BASE + shift, BASE - shift], axis=2).reshape(SOURCES, EXPERTS)
    block_end = jnp.cumsum(sizes, axis=1, dtype=jnp.int32)
    place = jnp.arange(TOP, dtype=jnp.int32)[None, None, :] * TOK + tok_order[:, :, None].astype(jnp.int32)
    block = jax.vmap(lambda end_row, place_row: jnp.searchsorted(end_row, place_row, side='right'))(block_end, place)
    expert = jnp.take_along_axis(exp_order, block.reshape(SOURCES, TOK * TOP), axis=1)
    return expert.reshape(SOURCES * TOK, TOP).astype(jnp.int32)


def setup_inputs(seed: int = 0) -> dict:
    keys = jax.random.split(jax.random.key(seed), 14)
    n_all = SOURCES * TOK

    def normal(key, shape, scale):
        return (scale * jax.random.normal(key, shape, jnp.float32)).astype(jnp.bfloat16)

    def gates(key):
        return jax.random.uniform(key, (n_all, TOP), jnp.float32, 0.5, 1.5) * TOP ** -0.5

    return {
        'tokens': normal(keys[0], (n_all, D), 1.0),
        'dy_out': normal(keys[1], (n_all, D), 1.0),
        'dense_w1': normal(keys[2], (D, D), 0.5 * D ** -0.5),
        'route_idx1': draw_routing(keys[3]),
        'route_gate1': gates(keys[4]),
        'w_gate1': normal(keys[5], (EXPERTS, D, FF), D ** -0.5),
        'w_up1': normal(keys[6], (EXPERTS, D, FF), D ** -0.5),
        'w_down1': normal(keys[7], (EXPERTS, FF, D), FF ** -0.5),
        'dense_w2': normal(keys[8], (D, D), 0.5 * D ** -0.5),
        'route_idx2': draw_routing(keys[9]),
        'route_gate2': gates(keys[10]),
        'w_gate2': normal(keys[11], (EXPERTS, D, FF), D ** -0.5),
        'w_up2': normal(keys[12], (EXPERTS, D, FF), D ** -0.5),
        'w_down2': normal(keys[13], (EXPERTS, FF, D), FF ** -0.5),
    }


def group_rows(route_idx, n_rows):
    flat_exp = route_idx.reshape(-1)
    n_copies = flat_exp.shape[0]
    order = jnp.argsort(flat_exp, stable=True).astype(jnp.int32)
    sorted_exp = jnp.take(flat_exp, order)
    counts = jnp.zeros((EXPERTS,), jnp.int32).at[flat_exp].add(1)
    starts = jnp.cumsum(counts, dtype=jnp.int32) - counts
    dest_row = (sorted_exp * n_rows + jnp.arange(n_copies, dtype=jnp.int32) - jnp.take(starts, sorted_exp)).astype(jnp.int32)
    return jnp.zeros((n_copies,), jnp.int32).at[order].set(dest_row).reshape(route_idx.shape)


def moe_layer(x_tok, dense_w, route_idx, route_gate, w_gate, w_up, w_down):
    n_all = x_tok.shape[0]
    n_rows = SOURCES * CAPACITY
    x_wide = x_tok.astype(jnp.float32)
    mixed = (x_wide + jnp.dot(x_wide, dense_w.astype(jnp.float32), preferred_element_type=jnp.float32)).astype(jnp.bfloat16)
    flat_pos = group_rows(route_idx, n_rows)
    tok_ids = jnp.broadcast_to(jnp.arange(n_all, dtype=jnp.int32)[:, None], route_idx.shape)
    row_tok = jnp.full((EXPERTS * n_rows,), n_all, jnp.int32).at[flat_pos.reshape(-1)].set(tok_ids.reshape(-1))
    buffer = jnp.take(mixed, row_tok, axis=0, mode='fill', fill_value=0).reshape(EXPERTS, n_rows, D).astype(jnp.float32)
    a_pre = jnp.einsum('erd,edf->erf', buffer, w_gate.astype(jnp.float32))
    b_pre = jnp.einsum('erd,edf->erf', buffer, w_up.astype(jnp.float32))
    hidden = (jax.nn.silu(a_pre) * b_pre).astype(jnp.bfloat16)
    expert_out = jnp.einsum('erf,efd->erd', hidden.astype(jnp.float32), w_down.astype(jnp.float32)).astype(jnp.bfloat16)
    picked = jnp.take(expert_out.reshape(EXPERTS * n_rows, D), flat_pos, axis=0).astype(jnp.float32)
    return (mixed.astype(jnp.float32) + jnp.sum(route_gate[:, :, None] * picked, axis=1)).astype(jnp.bfloat16)


def reference(tokens, dy_out, dense_w1, route_idx1, route_gate1, w_gate1, w_up1, w_down1, dense_w2, route_idx2, route_gate2, w_gate2, w_up2, w_down2):
    def forward(x_tok, dense_a, gate_a, up_a, down_a, dense_b, gate_b, up_b, down_b):
        mid_tok = moe_layer(x_tok, dense_a, route_idx1, route_gate1, gate_a, up_a, down_a)
        return moe_layer(mid_tok, dense_b, route_idx2, route_gate2, gate_b, up_b, down_b)

    y_out, pullback = jax.vjp(forward, tokens, dense_w1, w_gate1, w_up1, w_down1, dense_w2, w_gate2, w_up2, w_down2)
    (grad_tok, grad_dense1, grad_gate1, grad_up1, grad_down1, grad_dense2, grad_gate2, grad_up2, grad_down2) = pullback(dy_out)
    return (grad_tok, grad_dense1, grad_gate1, grad_up1, grad_down1, grad_dense2, grad_gate2, grad_up2, grad_down2)
```

```python
import jax
import jax.numpy as jnp
from jax import lax
from jax.experimental import pallas as pl
from jax.experimental.pallas import tpu as pltpu
from jax.sharding import Mesh, PartitionSpec as P

F32 = jnp.float32
BF16 = jnp.bfloat16
CAP = 64
GROUP = 4
CORES = 2
CHIPS = 2
ALL = ('x', 'c', 'y')


def matmul(lhs, rhs, lhs_dim=1, rhs_dim=0):
    return lax.dot_general(lhs, rhs, (((lhs_dim,), (rhs_dim,)), ((), ())), preferred_element_type=F32)


def gate_hidden(x_rows, w_gate, w_up):
    a_pre = matmul(x_rows, w_gate)
    b_pre = matmul(x_rows, w_up)
    return a_pre, b_pre, jax.nn.sigmoid(a_pre)


def select_rows(rank_ref, gate_ref, src, n_src):
    n_tok = rank_ref.shape[-1]
    slot = lax.broadcasted_iota(jnp.int32, (CAP, n_tok), 0)
    picks, gates = [], []
    for exp in range(GROUP):
        row = pl.ds(exp * n_src + src, 1)
        hit = slot == rank_ref[row, :]
        picks.append(jnp.where(hit, 1.0, 0.0).astype(BF16))
        gates.append(jnp.sum(jnp.where(hit, gate_ref[row, :], 0.0), axis=1, keepdims=True))
    return jnp.concatenate(picks, axis=0), jnp.concatenate(gates, axis=0)


def forward_kernel(where_ref, u_ref, rank_ref, gate_ref, wg_ref, wu_ref, wd_ref, out_ref, pick_ref, row_ref, x_ref, part_ref):
    n_src = u_ref.shape[0]
    own = n_src // CHIPS
    first = where_ref[1] * own

    @pl.when(pl.program_id(0) == 0)
    def _():
        out_ref[...] = jnp.zeros_like(out_ref)

    @pl.loop(0, own)
    def _(src):
        pick, gate = select_rows(rank_ref, gate_ref, first + src, n_src)
        pick_ref[src] = pick
        rows = matmul(pick, u_ref[first + src]).astype(BF16)
        at = pl.ds(pl.multiple_of(src * CAP, CAP), CAP)
        for exp in range(GROUP):
            x_ref[exp, at, :] = rows[exp * CAP:(exp + 1) * CAP]
            row_ref[exp, at, :] = jnp.broadcast_to(gate[exp * CAP:(exp + 1) * CAP], (CAP, 128))

    @pl.loop(0, GROUP)
    def _(exp):
        a_pre, b_pre, sigma = gate_hidden(x_ref[exp], wg_ref[exp], wu_ref[exp])
        hidden = (a_pre * sigma * b_pre).astype(BF16)
        out = matmul(hidden, wd_ref[exp]).astype(BF16).astype(F32) * row_ref[exp][:, :1]
        high = out.astype(BF16)
        rest = out - high.astype(F32)
        mid = rest.astype(BF16)
        low = (rest - mid.astype(F32)).astype(BF16)
        at = pl.ds(pl.multiple_of(exp * CAP, CAP), CAP)
        for src in range(own):
            here = slice(src * CAP, (src + 1) * CAP)
            part_ref[src, 0, at, :] = high[here]
            part_ref[src, 1, at, :] = mid[here]
            part_ref[src, 2, at, :] = low[here]

    @pl.loop(0, own)
    def _(src):
        pick = pick_ref[src]
        total = matmul(pick, part_ref[src, 0], 0, 0)
        total += matmul(pick, part_ref[src, 1], 0, 0) + matmul(pick, part_ref[src, 2], 0, 0)
        out_ref[src] += total


def backward_kernel(where_ref, u_ref, dy_ref, rank_ref, gate_ref, wg_ref, wu_ref, wd_ref,
                    out_ref, gg_ref, gu_ref, gd_ref, pick_ref, x_ref, d_ref, gx_ref):
    n_src, _, dim = u_ref.shape
    own = n_src // CHIPS
    first = where_ref[1] * own
    half = dim // CHIPS
    piece = half // CORES
    cols = pl.ds(pl.multiple_of(where_ref[1] * half, half), half)

    @pl.when(pl.program_id(0) == 0)
    def _():
        out_ref[...] = jnp.zeros_like(out_ref)

    @pl.loop(0, n_src)
    def _(step):
        src = lax.rem(first + step, n_src)
        pick, gate = select_rows(rank_ref, gate_ref, src, n_src)
        pick_ref[step] = pick
        x_rows = matmul(pick, u_ref[src]).astype(BF16)
        d_rows = (matmul(pick, dy_ref[src]) * gate).astype(BF16)
        at = pl.ds(pl.multiple_of(step * CAP, CAP), CAP)
        for exp in range(GROUP):
            x_ref[exp, at, :] = x_rows[exp * CAP:(exp + 1) * CAP]
            d_ref[exp, at, :] = d_rows[exp * CAP:(exp + 1) * CAP]

    @pl.loop(0, GROUP)
    def _(exp):
        w_gate, w_up = wg_ref[exp], wu_ref[exp]
        a_pre, b_pre, sigma = gate_hidden(x_ref[exp], w_gate, w_up)
        silu = a_pre * sigma
        hidden = (silu * b_pre).astype(BF16)
        grad_hidden = matmul(d_ref[exp], wd_ref[exp], 1, 1).astype(BF16).astype(F32)
        grad_a = (grad_hidden * b_pre * sigma * (1.0 + a_pre * (1.0 - sigma))).astype(BF16)
        grad_b = (grad_hidden * silu).astype(BF16)
        x_half = x_ref[exp, :, cols]
        grad_gate = matmul(x_half, grad_a, 0, 0).astype(BF16)
        grad_up = matmul(x_half, grad_b, 0, 0).astype(BF16)
        grad_down = matmul(hidden, d_ref[exp, :, cols], 0, 0).astype(BF16)
        for core in range(CORES):
            here = slice(core * piece, (core + 1) * piece)
            gg_ref[core, exp] = grad_gate[here]
            gu_ref[core, exp] = grad_up[here]
            gd_ref[core, exp] = grad_down[:, here]
        kept = own * CAP
        grad_x = (matmul(grad_a[:kept], w_gate, 1, 1) + matmul(grad_b[:kept], w_up, 1, 1)).astype(BF16)
        at = pl.ds(pl.multiple_of(exp * CAP, CAP), CAP)
        for src in range(own):
            gx_ref[src, at, :] = grad_x[src * CAP:(src + 1) * CAP]

    @pl.loop(0, own)
    def _(src):
        out_ref[src] += matmul(pick_ref[src], gx_ref[src], 0, 0)


def call_specs(n_src, n_tok, dim, ff, n_exp):
    groups = n_exp // GROUP
    whole = pl.BlockSpec((n_src, n_tok, dim), lambda g, w: (0, 0, 0), pipeline_mode=pl.Buffered(1))
    table = pl.BlockSpec((GROUP * n_src, n_tok), lambda g, w: (g, 0))
    wide = pl.BlockSpec((GROUP, dim, ff), lambda g, w: (w[0] * groups + g, 0, 0))
    tall = pl.BlockSpec((GROUP, ff, dim), lambda g, w: (w[0] * groups + g, 0, 0))
    total = pl.BlockSpec((n_src // CHIPS, n_tok, dim), lambda g, w: (0, 0, 0), pipeline_mode=pl.Buffered(1))
    return groups, whole, table, wide, tall, total


def expert_forward(where, u_all, rank, gate, w_gate, w_up, w_down):
    n_src, n_tok, dim = u_all.shape
    ff = w_gate.shape[2]
    n_exp = rank.shape[0] // n_src
    own = n_src // CHIPS
    groups, whole, table, wide, tall, total = call_specs(n_src, n_tok, dim, ff, n_exp)
    rows = n_exp * own * CAP
    return pl.pallas_call(
        forward_kernel,
        out_shape=jax.ShapeDtypeStruct((own, n_tok, dim), F32),
        grid_spec=pltpu.PrefetchScalarGridSpec(
            num_scalar_prefetch=1, grid=(groups,), in_specs=[whole, table, table, wide, wide, tall], out_specs=total,
            scratch_shapes=[pltpu.VMEM((own, GROUP * CAP, n_tok), BF16), pltpu.VMEM((GROUP, own * CAP, 128), F32),
                            pltpu.VMEM((GROUP, own * CAP, dim), BF16), pltpu.VMEM((own, 3, GROUP * CAP, dim), BF16)]),
        compiler_params=pltpu.CompilerParams(dimension_semantics=('arbitrary',), vmem_limit_bytes=56 << 20),
        cost_estimate=pl.CostEstimate(flops=rows * dim * (8 * n_tok + 6 * ff), bytes_accessed=40 << 20, transcendentals=0),
    )(where, u_all, rank, gate, w_gate, w_up, w_down)


def expert_backward(where, u_all, dy_all, rank, gate, w_gate, w_up, w_down):
    n_src, n_tok, dim = u_all.shape
    ff = w_gate.shape[2]
    n_exp = rank.shape[0] // n_src
    own = n_src // CHIPS
    piece = dim // (CHIPS * CORES)
    groups, whole, table, wide, tall, total = call_specs(n_src, n_tok, dim, ff, n_exp)
    rows = n_exp * n_src * CAP
    wide_out = pl.BlockSpec((CORES, GROUP, piece, ff), lambda g, w: (0, g, 0, 0))
    tall_out = pl.BlockSpec((CORES, GROUP, ff, piece), lambda g, w: (0, g, 0, 0))
    wide_shape = jax.ShapeDtypeStruct((CORES, n_exp, piece, ff), BF16)
    return pl.pallas_call(
        backward_kernel,
        out_shape=(jax.ShapeDtypeStruct((own, n_tok, dim), F32), wide_shape, wide_shape,
                   jax.ShapeDtypeStruct((CORES, n_exp, ff, piece), BF16)),
        grid_spec=pltpu.PrefetchScalarGridSpec(
            num_scalar_prefetch=1, grid=(groups,), in_specs=[whole, whole, table, table, wide, wide, tall],
            out_specs=(total, wide_out, wide_out, tall_out),
            scratch_shapes=[pltpu.VMEM((n_src, GROUP * CAP, n_tok), BF16), pltpu.VMEM((GROUP, n_src * CAP, dim), BF16),
                            pltpu.VMEM((GROUP, n_src * CAP, dim), BF16), pltpu.VMEM((own, GROUP * CAP, dim), BF16)]),
        compiler_params=pltpu.CompilerParams(dimension_semantics=('arbitrary',), vmem_limit_bytes=56 << 20),
        cost_estimate=pl.CostEstimate(flops=rows * dim * (5 * n_tok + 11 * ff), bytes_accessed=60 << 20, transcendentals=0),
    )(where, u_all, dy_all, rank, gate, w_gate, w_up, w_down)


def route_tables(idx, gate, first_exp, n_exp):
    n_src, _, n_tok = idx.shape
    experts = (first_exp + jnp.arange(n_exp, dtype=jnp.int32)).astype(F32)
    hit = idx[None] == experts[:, None, None, None]
    member = jnp.any(hit, axis=2)
    gates = jnp.sum(jnp.where(hit, gate[None], 0.0), axis=2)
    before = jnp.triu(jnp.ones((n_tok, n_tok), BF16), 1)
    count = jnp.einsum('est,tv->esv', member.astype(BF16), before, preferred_element_type=F32)
    rank = jnp.where(member, count.astype(jnp.int32), -1)
    return rank.reshape(n_exp * n_src, n_tok), gates.reshape(n_exp * n_src, n_tok)


def mix(x, weight):
    return (x.astype(F32) + jnp.einsum('...d,de->...e', x, weight, preferred_element_type=F32)).astype(BF16)


def mix_back(grad, weight):
    return (grad.astype(F32) + jnp.einsum('...e,de->...d', grad, weight, preferred_element_type=F32)).astype(BF16)


def swap_cores(parts):
    moved = lax.all_to_all(parts, 'c', 0, 0, tiled=True)
    return moved.reshape((-1,) + moved.shape[2:])


def solution(mesh):
    fine = Mesh(mesh.devices.reshape(2, CHIPS, CORES), ('y', 'x', 'c'))
    tok_spec = P(ALL, None)
    exp_spec = P('y', None, None)
    layer_specs = (P(None, None), tok_spec, tok_spec, exp_spec, exp_spec, exp_spec)
    grad_specs = (P(ALL, None), P('y', ('x', 'c'), None), P('y', ('x', 'c'), None), P('y', None, ('x', 'c')))

    def local_step(tokens, dy_out, dense_w1, route_idx1, route_gate1, w_gate1, w_up1, w_down1, dense_w2, route_idx2, route_gate2, w_gate2, w_up2, w_down2):
        n_exp = w_gate1.shape[0] // CORES
        ix, ic, iy = (lax.axis_index(name) for name in ALL)
        where = jnp.stack([ic, ix]).astype(jnp.int32)
        first_exp = (iy * CORES + ic) * n_exp
        me = (ix * CORES + ic) * 2 + iy

        def gather(value):
            return lax.all_gather(value, ALL, axis=0, tiled=False)

        def reduce_own(total):
            return lax.psum_scatter(total, ('c', 'y'), scatter_dimension=0, tiled=False)

        routes = jnp.concatenate([route_idx1.astype(F32), route_idx2.astype(F32), route_gate1, route_gate2], axis=1).T
        routes = gather(routes)
        idx1, idx2, gate1, gate2 = jnp.split(routes, 4, axis=1)
        rank1, gates1 = route_tables(idx1, gate1, first_exp, n_exp)
        rank2, gates2 = route_tables(idx2, gate2, first_exp, n_exp)

        tok_all = gather(tokens)
        dy_all = gather(dy_out)
        u_one = mix(tok_all, dense_w1)
        y_sum = reduce_own(expert_forward(where, u_one, rank1, gates1, w_gate1, w_up1, w_down1))
        y_one = (mix(tokens, dense_w1).astype(F32) + y_sum).astype(BF16)
        y_all = gather(y_one)
        u_two = mix(y_all, dense_w2)
        back, gg, gu, gd = expert_backward(where, u_two, dy_all, rank2, gates2, w_gate2, w_up2, w_down2)
        gm_two = (dy_out.astype(F32) + reduce_own(back)).astype(BF16)
        gate_two, up_two, down_two = swap_cores(gg), swap_cores(gu), swap_cores(gd)
        gm_all = gather(gm_two)
        rows = dense_w2.shape[0] // 8
        y_cols = lax.dynamic_slice_in_dim(y_all, me * rows, rows, 2)
        dense_two = jnp.einsum('std,ste->de', y_cols, gm_all, preferred_element_type=F32).astype(BF16)
        grad_mid = mix_back(gm_all, dense_w2)
        back, gg, gu, gd = expert_backward(where, u_one, grad_mid, rank1, gates1, w_gate1, w_up1, w_down1)
        gm_one = (lax.dynamic_index_in_dim(grad_mid, me, 0, keepdims=False).astype(F32) + reduce_own(back)).astype(BF16)
        gate_one, up_one, down_one = swap_cores(gg), swap_cores(gu), swap_cores(gd)
        grad_tok = mix_back(gm_one, dense_w1)
        dense_part = jnp.einsum('td,te->de', tokens, gm_one, preferred_element_type=F32).astype(BF16)
        dense_one = lax.psum_scatter(dense_part, ALL, scatter_dimension=0, tiled=True)
        return (grad_tok, dense_one, gate_one, up_one, down_one, dense_two, gate_two, up_two, down_two)

    return jax.shard_map(local_step, mesh=fine, in_specs=(tok_spec, tok_spec) + layer_specs + layer_specs,
                         out_specs=(tok_spec,) + grad_specs + grad_specs, check_vma=False)
```

```python
import jax
import jax.numpy as jnp
from jax import lax
from jax.experimental import pallas as pl
from jax.experimental.pallas import tpu as pltpu
from jax.sharding import Mesh, PartitionSpec as P

F32 = jnp.float32
BF16 = jnp.bfloat16
CAP = 64
GROUP = 4
CORES = 2
CHIPS = 2
ALL = ('x', 'c', 'y')


def matmul(lhs, rhs, lhs_dim=1, rhs_dim=0):
    return lax.dot_general(lhs, rhs, (((lhs_dim,), (rhs_dim,)), ((), ())), preferred_element_type=F32)


def gate_hidden(x_rows, w_gate, w_up):
    a_pre = matmul(x_rows, w_gate, 1, 1)
    b_pre = matmul(x_rows, w_up, 1, 1)
    return a_pre, b_pre, jax.nn.sigmoid(a_pre)


def select_rows(rank_ref, gate_ref, src, n_src):
    n_tok = rank_ref.shape[-1]
    slot = lax.broadcasted_iota(jnp.int32, (CAP, n_tok), 0)
    picks, gates = [], []
    for exp in range(GROUP):
        row = pl.ds(exp * n_src + src, 1)
        hit = slot == rank_ref[row, :]
        picks.append(jnp.where(hit, 1.0, 0.0).astype(BF16))
        gates.append(jnp.sum(jnp.where(hit, gate_ref[row, :], 0.0), axis=1, keepdims=True))
    return jnp.concatenate(picks, axis=0), jnp.concatenate(gates, axis=0)


def forward_kernel(where_ref, u_ref, rank_ref, gate_ref, wg_ref, wu_ref, wd_ref, out_ref, pick_ref, row_ref, x_ref, part_ref):
    n_src = u_ref.shape[0]
    own = n_src // CHIPS
    first = where_ref[1] * own

    @pl.when(pl.program_id(0) == 0)
    def _():
        out_ref[...] = jnp.zeros_like(out_ref)

    @pl.loop(0, own)
    def _(src):
        pick, gate = select_rows(rank_ref, gate_ref, first + src, n_src)
        pick_ref[src] = pick
        rows = matmul(pick, u_ref[first + src]).astype(BF16)
        at = pl.ds(pl.multiple_of(src * CAP, CAP), CAP)
        for exp in range(GROUP):
            x_ref[exp, at, :] = rows[exp * CAP:(exp + 1) * CAP]
            row_ref[exp, at, :] = jnp.broadcast_to(gate[exp * CAP:(exp + 1) * CAP], (CAP, 128))

    @pl.loop(0, GROUP)
    def _(exp):
        a_pre, b_pre, sigma = gate_hidden(x_ref[exp], wg_ref[exp], wu_ref[exp])
        hidden = (a_pre * sigma * b_pre).astype(BF16)
        out = matmul(hidden, wd_ref[exp]).astype(BF16).astype(F32) * row_ref[exp][:, :1]
        high = out.astype(BF16)
        rest = out - high.astype(F32)
        mid = rest.astype(BF16)
        low = (rest - mid.astype(F32)).astype(BF16)
        at = pl.ds(pl.multiple_of(exp * CAP, CAP), CAP)
        for src in range(own):
            here = slice(src * CAP, (src + 1) * CAP)
            part_ref[src, 0, at, :] = high[here]
            part_ref[src, 1, at, :] = mid[here]
            part_ref[src, 2, at, :] = low[here]

    @pl.loop(0, own)
    def _(src):
        pick = pick_ref[src]
        total = matmul(pick, part_ref[src, 0], 0, 0)
        total += matmul(pick, part_ref[src, 1], 0, 0) + matmul(pick, part_ref[src, 2], 0, 0)
        out_ref[src] += total


def backward_kernel(where_ref, u_ref, dy_ref, rank_ref, gate_ref, wg_ref, wu_ref, wd_ref,
                    out_ref, gg_ref, gu_ref, gd_ref, pick_ref, x_ref, d_ref, gx_ref):
    n_src, _, dim = u_ref.shape
    own = n_src // CHIPS
    first = where_ref[1] * own
    half = dim // CHIPS
    piece = half // CORES
    cols = pl.ds(pl.multiple_of(where_ref[1] * half, half), half)

    @pl.when(pl.program_id(0) == 0)
    def _():
        out_ref[...] = jnp.zeros_like(out_ref)

    @pl.loop(0, n_src)
    def _(step):
        src = lax.rem(first + step, n_src)
        pick, gate = select_rows(rank_ref, gate_ref, src, n_src)
        pick_ref[step] = pick
        x_rows = matmul(pick, u_ref[src]).astype(BF16)
        d_rows = (matmul(pick, dy_ref[src]) * gate).astype(BF16)
        at = pl.ds(pl.multiple_of(step * CAP, CAP), CAP)
        for exp in range(GROUP):
            x_ref[exp, at, :] = x_rows[exp * CAP:(exp + 1) * CAP]
            d_ref[exp, at, :] = d_rows[exp * CAP:(exp + 1) * CAP]

    @pl.loop(0, GROUP)
    def _(exp):
        w_gate, w_up = wg_ref[exp], wu_ref[exp]
        a_pre, b_pre, sigma = gate_hidden(x_ref[exp], w_gate, w_up)
        silu = a_pre * sigma
        hidden = (silu * b_pre).astype(BF16)
        grad_hidden = matmul(d_ref[exp], wd_ref[exp], 1, 1).astype(BF16).astype(F32)
        grad_a = (grad_hidden * b_pre * sigma * (1.0 + a_pre * (1.0 - sigma))).astype(BF16)
        grad_b = (grad_hidden * silu).astype(BF16)
        x_half = x_ref[exp, :, cols]
        grad_gate = matmul(grad_a, x_half, 0, 0).astype(BF16)
        grad_up = matmul(grad_b, x_half, 0, 0).astype(BF16)
        grad_down = matmul(hidden, d_ref[exp, :, cols], 0, 0).astype(BF16)
        for core in range(CORES):
            here = slice(core * piece, (core + 1) * piece)
            gg_ref[core, exp] = grad_gate[:, here]
            gu_ref[core, exp] = grad_up[:, here]
            gd_ref[core, exp] = grad_down[:, here]
        kept = own * CAP
        grad_x = (matmul(grad_a[:kept], w_gate) + matmul(grad_b[:kept], w_up)).astype(BF16)
        at = pl.ds(pl.multiple_of(exp * CAP, CAP), CAP)
        for src in range(own):
            gx_ref[src, at, :] = grad_x[src * CAP:(src + 1) * CAP]

    @pl.loop(0, own)
    def _(src):
        out_ref[src] += matmul(pick_ref[src], gx_ref[src], 0, 0)


def call_specs(n_src, n_tok, dim, ff, n_exp):
    groups = n_exp // GROUP
    whole = pl.BlockSpec((n_src, n_tok, dim), lambda g, w: (0, 0, 0), pipeline_mode=pl.Buffered(1))
    table = pl.BlockSpec((GROUP * n_src, n_tok), lambda g, w: (g, 0))
    tall = pl.BlockSpec((GROUP, ff, dim), lambda g, w: (w[0] * groups + g, 0, 0))
    total = pl.BlockSpec((n_src // CHIPS, n_tok, dim), lambda g, w: (0, 0, 0), pipeline_mode=pl.Buffered(1))
    return groups, whole, table, tall, total


def expert_forward(where, u_all, rank, gate, w_gate, w_up, w_down):
    n_src, n_tok, dim = u_all.shape
    ff = w_gate.shape[1]
    n_exp = rank.shape[0] // n_src
    own = n_src // CHIPS
    groups, whole, table, tall, total = call_specs(n_src, n_tok, dim, ff, n_exp)
    rows = n_exp * own * CAP
    return pl.pallas_call(
        forward_kernel,
        out_shape=jax.ShapeDtypeStruct((own, n_tok, dim), F32),
        grid_spec=pltpu.PrefetchScalarGridSpec(
            num_scalar_prefetch=1, grid=(groups,), in_specs=[whole, table, table, tall, tall, tall], out_specs=total,
            scratch_shapes=[pltpu.VMEM((own, GROUP * CAP, n_tok), BF16), pltpu.VMEM((GROUP, own * CAP, 128), F32),
                            pltpu.VMEM((GROUP, own * CAP, dim), BF16), pltpu.VMEM((own, 3, GROUP * CAP, dim), BF16)]),
        compiler_params=pltpu.CompilerParams(dimension_semantics=('arbitrary',), vmem_limit_bytes=56 << 20),
        cost_estimate=pl.CostEstimate(flops=rows * dim * (8 * n_tok + 6 * ff), bytes_accessed=40 << 20, transcendentals=0),
    )(where, u_all, rank, gate, w_gate, w_up, w_down)


def expert_backward(where, u_all, dy_all, rank, gate, w_gate, w_up, w_down):
    n_src, n_tok, dim = u_all.shape
    ff = w_gate.shape[1]
    n_exp = rank.shape[0] // n_src
    own = n_src // CHIPS
    piece = dim // (CHIPS * CORES)
    groups, whole, table, tall, total = call_specs(n_src, n_tok, dim, ff, n_exp)
    rows = n_exp * n_src * CAP
    tall_out = pl.BlockSpec((CORES, GROUP, ff, piece), lambda g, w: (0, g, 0, 0))
    tall_shape = jax.ShapeDtypeStruct((CORES, n_exp, ff, piece), BF16)
    return pl.pallas_call(
        backward_kernel,
        out_shape=(jax.ShapeDtypeStruct((own, n_tok, dim), F32), tall_shape, tall_shape, tall_shape),
        grid_spec=pltpu.PrefetchScalarGridSpec(
            num_scalar_prefetch=1, grid=(groups,), in_specs=[whole, whole, table, table, tall, tall, tall],
            out_specs=(total, tall_out, tall_out, tall_out),
            scratch_shapes=[pltpu.VMEM((n_src, GROUP * CAP, n_tok), BF16), pltpu.VMEM((GROUP, n_src * CAP, dim), BF16),
                            pltpu.VMEM((GROUP, n_src * CAP, dim), BF16), pltpu.VMEM((own, GROUP * CAP, dim), BF16)]),
        compiler_params=pltpu.CompilerParams(dimension_semantics=('arbitrary',), vmem_limit_bytes=56 << 20),
        cost_estimate=pl.CostEstimate(flops=rows * dim * (5 * n_tok + 11 * ff), bytes_accessed=60 << 20, transcendentals=0),
    )(where, u_all, dy_all, rank, gate, w_gate, w_up, w_down)


def route_tables(idx, gate, first_exp, n_exp):
    n_src, _, n_tok = idx.shape
    experts = (first_exp + jnp.arange(n_exp, dtype=jnp.int32)).astype(F32)
    hit = idx[None] == experts[:, None, None, None]
    member = jnp.any(hit, axis=2)
    gates = jnp.sum(jnp.where(hit, gate[None], 0.0), axis=2)
    before = jnp.triu(jnp.ones((n_tok, n_tok), BF16), 1)
    count = jnp.einsum('est,tv->esv', member.astype(BF16), before, preferred_element_type=F32)
    rank = jnp.where(member, count.astype(jnp.int32), -1)
    return rank.reshape(n_exp * n_src, n_tok), gates.reshape(n_exp * n_src, n_tok)


def mix(x, weight):
    return (x.astype(F32) + jnp.einsum('...d,de->...e', x, weight, preferred_element_type=F32)).astype(BF16)


def mix_back(grad, weight):
    return (grad.astype(F32) + jnp.einsum('...e,de->...d', grad, weight, preferred_element_type=F32)).astype(BF16)


def swap_cores(parts):
    moved = lax.all_to_all(parts, 'c', 0, 0, tiled=True)
    return moved.reshape((-1,) + moved.shape[2:])


def solution(mesh):
    fine = Mesh(mesh.devices.reshape(2, CHIPS, CORES), ('y', 'x', 'c'))
    tok_spec = P(ALL, None)
    exp_spec = P('y', None, None)
    layer_specs = (P(None, None), tok_spec, tok_spec, exp_spec, exp_spec, exp_spec)
    grad_specs = (P(ALL, None), P('y', ('x', 'c'), None), P('y', ('x', 'c'), None), P('y', None, ('x', 'c')))

    def local_step(tokens, dy_out, dense_w1, route_idx1, route_gate1, w_gate1, w_up1, w_down1, dense_w2, route_idx2, route_gate2, w_gate2, w_up2, w_down2):
        n_exp = w_gate1.shape[0] // CORES
        w_gate1, w_up1, w_gate2, w_up2 = (jnp.swapaxes(w, 1, 2) for w in (w_gate1, w_up1, w_gate2, w_up2))
        ix, ic, iy = (lax.axis_index(name) for name in ALL)
        where = jnp.stack([ic, ix]).astype(jnp.int32)
        first_exp = (iy * CORES + ic) * n_exp
        me = (ix * CORES + ic) * 2 + iy

        def gather(value):
            return lax.all_gather(value, ALL, axis=0, tiled=False)

        def reduce_own(total):
            return lax.psum_scatter(total, ('c', 'y'), scatter_dimension=0, tiled=False)

        routes = jnp.concatenate([route_idx1.astype(F32), route_idx2.astype(F32), route_gate1, route_gate2], axis=1).T
        routes = gather(routes)
        idx1, idx2, gate1, gate2 = jnp.split(routes, 4, axis=1)
        rank1, gates1 = route_tables(idx1, gate1, first_exp, n_exp)
        rank2, gates2 = route_tables(idx2, gate2, first_exp, n_exp)

        tok_all = gather(tokens)
        dy_all = gather(dy_out)
        u_one = mix(tok_all, dense_w1)
        y_sum = reduce_own(expert_forward(where, u_one, rank1, gates1, w_gate1, w_up1, w_down1))
        y_one = (mix(tokens, dense_w1).astype(F32) + y_sum).astype(BF16)
        y_all = gather(y_one)
        u_two = mix(y_all, dense_w2)
        back, gg, gu, gd = expert_backward(where, u_two, dy_all, rank2, gates2, w_gate2, w_up2, w_down2)
        gm_two = (dy_out.astype(F32) + reduce_own(back)).astype(BF16)
        gate_two, up_two, down_two = jnp.swapaxes(swap_cores(gg), 1, 2), jnp.swapaxes(swap_cores(gu), 1, 2), swap_cores(gd)
        gm_all = gather(gm_two)
        rows = dense_w2.shape[0] // 8
        y_cols = lax.dynamic_slice_in_dim(y_all, me * rows, rows, 2)
        dense_two = jnp.einsum('std,ste->de', y_cols, gm_all, preferred_element_type=F32).astype(BF16)
        grad_mid = mix_back(gm_all, dense_w2)
        back, gg, gu, gd = expert_backward(where, u_one, grad_mid, rank1, gates1, w_gate1, w_up1, w_down1)
        gm_one = (lax.dynamic_index_in_dim(grad_mid, me, 0, keepdims=False).astype(F32) + reduce_own(back)).astype(BF16)
        gate_one, up_one, down_one = jnp.swapaxes(swap_cores(gg), 1, 2), jnp.swapaxes(swap_cores(gu), 1, 2), swap_cores(gd)
        grad_tok = mix_back(gm_one, dense_w1)
        dense_part = jnp.einsum('td,te->de', tokens, gm_one, preferred_element_type=F32).astype(BF16)
        dense_one = lax.psum_scatter(dense_part, ALL, scatter_dimension=0, tiled=True)
        return (grad_tok, dense_one, gate_one, up_one, down_one, dense_two, gate_two, up_two, down_two)

    return jax.shard_map(local_step, mesh=fine, in_specs=(tok_spec, tok_spec) + layer_specs + layer_specs,
                         out_specs=(tok_spec,) + grad_specs + grad_specs, check_vma=False)
```

```python
import functools

import jax
import jax.numpy as jnp
from jax import lax
from jax.experimental import pallas as pl
from jax.experimental.pallas import tpu as pltpu
from jax.sharding import Mesh, PartitionSpec as P

F32 = jnp.float32
BF16 = jnp.bfloat16
CAP = 64
GROUP = 4
CORES = 2
CHIPS = 2
ALL = ('x', 'c', 'y')


def matmul(lhs, rhs, lhs_dim=1, rhs_dim=0):
    return lax.dot_general(lhs, rhs, (((lhs_dim,), (rhs_dim,)), ((), ())), preferred_element_type=F32)


def gate_hidden(x_rows, w_gate, w_up):
    a_pre = matmul(x_rows, w_gate, 1, 1)
    b_pre = matmul(x_rows, w_up, 1, 1)
    return a_pre, b_pre, jax.nn.sigmoid(a_pre)


def select_rows(rank_ref, gate_ref, group, src):
    n_tok = rank_ref.shape[-1]
    slot = lax.broadcasted_iota(jnp.int32, (CAP, n_tok), 0)
    picks, gates = [], []
    for exp in range(GROUP):
        row = pl.ds(group * GROUP + exp, 1)
        hit = slot == rank_ref[src, row, :]
        picks.append(jnp.where(hit, 1.0, 0.0).astype(BF16))
        gates.append(jnp.sum(jnp.where(hit, gate_ref[src, row, :], 0.0), axis=1, keepdims=True))
    return jnp.concatenate(picks, axis=0), jnp.concatenate(gates, axis=0)


def forward_kernel(where_ref, u_ref, rank_ref, gate_ref, wg_ref, wu_ref, wd_ref, out_ref, pick_ref, row_ref, x_ref, part_ref):
    n_src = u_ref.shape[0]
    own = n_src // CHIPS
    first = where_ref[1] * own

    @pl.when(pl.program_id(0) == 0)
    def _():
        out_ref[...] = jnp.zeros_like(out_ref)

    @pl.loop(0, own)
    def _(src):
        pick, gate = select_rows(rank_ref, gate_ref, pl.program_id(0), first + src)
        pick_ref[src] = pick
        rows = matmul(pick, u_ref[first + src]).astype(BF16)
        at = pl.ds(pl.multiple_of(src * CAP, CAP), CAP)
        for exp in range(GROUP):
            x_ref[exp, at, :] = rows[exp * CAP:(exp + 1) * CAP]
            row_ref[exp, at, :] = jnp.broadcast_to(gate[exp * CAP:(exp + 1) * CAP], (CAP, 128))

    @pl.loop(0, GROUP)
    def _(exp):
        a_pre, b_pre, sigma = gate_hidden(x_ref[exp], wg_ref[exp], wu_ref[exp])
        hidden = (a_pre * sigma * b_pre).astype(BF16)
        out = matmul(hidden, wd_ref[exp]).astype(BF16).astype(F32) * row_ref[exp][:, :1]
        high = out.astype(BF16)
        rest = out - high.astype(F32)
        mid = rest.astype(BF16)
        low = (rest - mid.astype(F32)).astype(BF16)
        at = pl.ds(pl.multiple_of(exp * CAP, CAP), CAP)
        for src in range(own):
            here = slice(src * CAP, (src + 1) * CAP)
            part_ref[src, 0, at, :] = high[here]
            part_ref[src, 1, at, :] = mid[here]
            part_ref[src, 2, at, :] = low[here]

    @pl.loop(0, own)
    def _(src):
        pick = pick_ref[src]
        total = matmul(pick, part_ref[src, 0], 0, 0)
        total += matmul(pick, part_ref[src, 1], 0, 0) + matmul(pick, part_ref[src, 2], 0, 0)
        out_ref[src] += total


def layer_kernel(gather_input, whole_ref, mine_ref, rank_ref, gate_ref, wg_ref, wu_ref, wd_ref,
                 total_ref, gg_ref, gu_ref, gd_ref,
                 peer_ref, xo_ref, do_ref, h_ref, ga_ref, gb_ref, pick_ref, gx_ref, p_ref, rs_ref, x_ref, d_ref, stage_ref,
                 ag_send, ag_recv, rs_send, rs_recv, keep_sem, give_send, give_recv):
    n_src, _, dim = whole_ref.shape
    own = n_src // CHIPS
    n_group = xo_ref.shape[0] // GROUP
    half = dim // CHIPS
    piece = half // CORES
    step = pl.program_id(0)
    ix, ic, iy = (lax.axis_index(name) for name in ALL)
    cols = pl.ds(pl.multiple_of(ix * half, half), half)
    u_ref, dy_ref = (peer_ref, whole_ref) if gather_input else (whole_ref, peer_ref)
    outs = (gg_ref, gu_ref, gd_ref)

    def slot(flip_x=False, flip_y=False):
        x = 1 - ix if flip_x else ix
        y = 1 - iy if flip_y else iy
        return (x * CORES + ic) * 2 + y

    def send(src, dst, sems, at, axis):
        other = 1 - lax.axis_index(axis)
        return pltpu.make_async_remote_copy(src, dst, sems[0].at[at], sems[1].at[at], device_id={axis: other},
                                            device_id_type=pl.DeviceIdType.MESH)

    def spread(at):
        flips = ((0, 0), (0, 0), (0, 1), (0, 0), (0, 1), (1, 0), (1, 1))[at]
        block = peer_ref.at[slot(*flips)]
        return send(block if any(flips) else mine_ref, block, (ag_send, ag_recv), at, 'yxxcccc'[at])

    def add_up(at):
        part = ((1 - ic) * 2 + 1 - iy, (1 - ic) * 2 + iy, ic * 2 + 1 - iy)[at]
        return send(p_ref.at[part], rs_ref.at[at], (rs_send, rs_recv), at, 'ccy'[at])

    def store_copies(group):
        buf = lax.rem(group, 2)
        rows = pl.ds(ic * n_group * GROUP + group * GROUP, GROUP)
        pairs = []
        for kind in range(3):
            dst = outs[kind].at[rows]
            pairs.append(pltpu.make_async_copy(stage_ref.at[buf, ic, kind], dst, keep_sem.at[buf, kind]))
            pairs.append(pltpu.make_async_remote_copy(
                stage_ref.at[buf, 1 - ic, kind], dst, give_send.at[buf, kind], give_recv.at[group, kind],
                device_id={'c': 1 - ic}, device_id_type=pl.DeviceIdType.MESH))
        return pairs

    def store_start(group):
        for copy in store_copies(group):
            copy.start()

    def store_wait(group):
        keep = store_copies(group)
        for at in range(0, len(keep), 2):
            keep[at].wait()
            keep[at + 1].wait_send()

    def pull(first, group, x_dst, d_dst, base, keep_pick):
        @pl.loop(0, own)
        def _(src):
            pick, gate = select_rows(rank_ref, gate_ref, group, first + src)
            if keep_pick:
                pick_ref[src] = pick
            x_rows = matmul(pick, u_ref[first + src]).astype(BF16)
            d_rows = (matmul(pick, dy_ref[first + src]) * gate).astype(BF16)
            at = pl.ds(pl.multiple_of(src * CAP, CAP), CAP)
            for exp in range(GROUP):
                x_dst[base + exp, at, :] = x_rows[exp * CAP:(exp + 1) * CAP]
                d_dst[base + exp, at, :] = d_rows[exp * CAP:(exp + 1) * CAP]

    def hidden_grads(x_rows, d_rows, exp):
        a_pre, b_pre, sigma = gate_hidden(x_rows, wg_ref[exp], wu_ref[exp])
        silu = a_pre * sigma
        grad_hidden = matmul(d_rows, wd_ref[exp], 1, 1).astype(BF16).astype(F32)
        grad_a = (grad_hidden * b_pre * sigma * (1.0 + a_pre * (1.0 - sigma))).astype(BF16)
        return (silu * b_pre).astype(BF16), grad_a, (grad_hidden * silu).astype(BF16)

    @pl.when(step == 0)
    def _():
        barrier = pltpu.get_barrier_semaphore()
        for axis in ALL:
            pl.semaphore_signal(barrier, inc=1, device_id={axis: 1 - lax.axis_index(axis)}, device_id_type=pl.DeviceIdType.MESH)
        pl.semaphore_wait(barrier, len(ALL))
        for at in (0, 1, 3):
            spread(at).start()
        peer_ref[slot()] = mine_ref[...]
        p_ref[...] = jnp.zeros_like(p_ref)
        spread(0).wait_recv()
        spread(4).start()
        spread(2).start()
        spread(3).wait_recv()
        spread(4).wait_recv()

    @pl.when(step == n_group // 2)
    def _():
        spread(1).wait_recv()
        spread(5).start()

    @pl.when(step == n_group - 1)
    def _():
        spread(2).wait_recv()
        spread(6).start()

    @pl.when(step < n_group)
    def _():
        base = step * GROUP
        pull(ix * own, step, xo_ref, do_ref, base, True)

        @pl.loop(0, GROUP)
        def _(exp):
            hidden, grad_a, grad_b = hidden_grads(xo_ref[base + exp], do_ref[base + exp], exp)
            h_ref[base + exp] = hidden
            ga_ref[base + exp] = grad_a
            gb_ref[base + exp] = grad_b
            grad_x = (matmul(grad_a, wg_ref[exp]) + matmul(grad_b, wu_ref[exp])).astype(BF16)
            at = pl.ds(pl.multiple_of(exp * CAP, CAP), CAP)
            for src in range(own):
                gx_ref[src, at, :] = grad_x[src * CAP:(src + 1) * CAP]

        @pl.loop(0, own)
        def _(src):
            p_ref[src] += matmul(pick_ref[src], gx_ref[src], 0, 0)

    @pl.when(step == n_group)
    def _():
        add_up(0).start()
        add_up(1).start()
        spread(5).wait_recv()
        spread(6).wait_recv()

    @pl.when(step == n_group + 1)
    def _():
        add_up(0).wait_recv()
        p_ref[ic * 2 + 1 - iy] += rs_ref[0]

    @pl.when(step == n_group + 2)
    def _():
        add_up(2).start()

    @pl.when(step >= n_group)
    def _():
        group = step - n_group

        @pl.when(group >= 1)
        def _():
            store_start(group - 1)

        pull((1 - ix) * own, group, x_ref, d_ref, 0, False)

        @pl.when(group >= 2)
        def _():
            store_wait(group - 2)

        buf = lax.rem(group, 2)

        @pl.loop(0, GROUP)
        def _(exp):
            base = group * GROUP + exp
            hidden, grad_a, grad_b = hidden_grads(x_ref[exp], d_ref[exp], exp)
            x_own, x_far = xo_ref[base, :, cols], x_ref[exp, :, cols]
            d_own, d_far = do_ref[base, :, cols], d_ref[exp, :, cols]
            grads = (matmul(ga_ref[base], x_own, 0, 0) + matmul(grad_a, x_far, 0, 0),
                     matmul(gb_ref[base], x_own, 0, 0) + matmul(grad_b, x_far, 0, 0),
                     matmul(h_ref[base], d_own, 0, 0) + matmul(hidden, d_far, 0, 0))
            for kind in range(3):
                for core in range(CORES):
                    stage_ref[buf, core, kind, exp] = grads[kind][:, core * piece:(core + 1) * piece].astype(BF16)

    @pl.when(step == 2 * n_group - 1)
    def _():
        last = n_group - 1
        store_wait(last - 1)
        add_up(1).wait_recv()
        add_up(2).wait_recv()
        total_ref[...] = p_ref[ic * 2 + iy] + rs_ref[1] + rs_ref[2]
        store_start(last)
        for at in range(7):
            spread(at).wait_send()
        for at in range(3):
            add_up(at).wait_send()
        store_wait(last)
        for group in range(n_group):
            for copy in store_copies(group)[1::2]:
                copy.wait_recv()


def expert_forward(where, u_all, rank, gate, w_gate, w_up, w_down):
    n_src, n_tok, dim = u_all.shape
    ff = w_gate.shape[1]
    n_exp = rank.shape[1]
    own = n_src // CHIPS
    groups = n_exp // GROUP
    rows = n_exp * own * CAP
    whole = pl.BlockSpec((n_src, n_tok, dim), lambda g, w: (0, 0, 0), pipeline_mode=pl.Buffered(1))
    table = pl.BlockSpec((n_src, n_exp, n_tok), lambda g, w: (0, 0, 0), pipeline_mode=pl.Buffered(1))
    tall = pl.BlockSpec((GROUP, ff, dim), lambda g, w: (w[0] * groups + g, 0, 0))
    total = pl.BlockSpec((own, n_tok, dim), lambda g, w: (0, 0, 0), pipeline_mode=pl.Buffered(1))
    return pl.pallas_call(
        forward_kernel,
        out_shape=jax.ShapeDtypeStruct((own, n_tok, dim), F32),
        grid_spec=pltpu.PrefetchScalarGridSpec(
            num_scalar_prefetch=1, grid=(groups,), in_specs=[whole, table, table, tall, tall, tall], out_specs=total,
            scratch_shapes=[pltpu.VMEM((own, GROUP * CAP, n_tok), BF16), pltpu.VMEM((GROUP, own * CAP, 128), F32),
                            pltpu.VMEM((GROUP, own * CAP, dim), BF16), pltpu.VMEM((own, 3, GROUP * CAP, dim), BF16)]),
        compiler_params=pltpu.CompilerParams(dimension_semantics=('arbitrary',), vmem_limit_bytes=56 << 20),
        cost_estimate=pl.CostEstimate(flops=rows * dim * (8 * n_tok + 6 * ff), bytes_accessed=40 << 20, transcendentals=0),
    )(where, u_all, rank, gate, w_gate, w_up, w_down)


def layer_backward(gather_input, whole, mine, rank, gate, w_gate, w_up, w_down):
    n_src, n_tok, dim = whole.shape
    n_all, ff, _ = w_gate.shape
    n_exp = rank.shape[1]
    own = n_src // CHIPS
    piece = dim // (CHIPS * CORES)
    groups = n_exp // GROUP
    rows = n_exp * n_src * CAP

    def fixed(*shape):
        return pl.BlockSpec(shape, lambda s: (0,) * len(shape), pipeline_mode=pl.Buffered(1))

    tall = pl.BlockSpec((GROUP, ff, dim), lambda s: (lax.axis_index('c') * groups + lax.rem(s, groups), 0, 0))
    grad_shape = jax.ShapeDtypeStruct((n_all, ff, piece), BF16)
    kept = own * CAP
    return pl.pallas_call(
        functools.partial(layer_kernel, gather_input),
        out_shape=(jax.ShapeDtypeStruct((n_tok, dim), F32), grad_shape, grad_shape, grad_shape),
        grid_spec=pltpu.PrefetchScalarGridSpec(
            num_scalar_prefetch=0, grid=(2 * groups,),
            in_specs=[fixed(n_src, n_tok, dim), fixed(n_tok, dim), fixed(n_src, n_exp, n_tok), fixed(n_src, n_exp, n_tok), tall, tall, tall],
            out_specs=(fixed(n_tok, dim),) + (pl.BlockSpec(memory_space=pl.ANY),) * 3,
            scratch_shapes=[pltpu.VMEM((n_src, n_tok, dim), BF16), pltpu.VMEM((n_exp, kept, dim), BF16),
                            pltpu.VMEM((n_exp, kept, dim), BF16), pltpu.VMEM((n_exp, kept, ff), BF16),
                            pltpu.VMEM((n_exp, kept, ff), BF16), pltpu.VMEM((n_exp, kept, ff), BF16),
                            pltpu.VMEM((own, GROUP * CAP, n_tok), BF16), pltpu.VMEM((own, GROUP * CAP, dim), BF16),
                            pltpu.VMEM((own, n_tok, dim), F32), pltpu.VMEM((3, n_tok, dim), F32),
                            pltpu.VMEM((GROUP, kept, dim), BF16), pltpu.VMEM((GROUP, kept, dim), BF16),
                            pltpu.VMEM((2, CORES, 3, GROUP, ff, piece), BF16),
                            pltpu.SemaphoreType.DMA((7,)), pltpu.SemaphoreType.DMA((7,)),
                            pltpu.SemaphoreType.DMA((3,)), pltpu.SemaphoreType.DMA((3,)),
                            pltpu.SemaphoreType.DMA((2, 3)), pltpu.SemaphoreType.DMA((2, 3)), pltpu.SemaphoreType.DMA((groups, 3))]),
        compiler_params=pltpu.CompilerParams(dimension_semantics=('arbitrary',), vmem_limit_bytes=62 << 20,
                                             collective_id=int(gather_input), has_side_effects=True),
        cost_estimate=pl.CostEstimate(flops=rows * dim * (5 * n_tok + 11 * ff), bytes_accessed=60 << 20, transcendentals=0),
    )(whole, mine, rank, gate, w_gate, w_up, w_down)


def route_tables(idx, gate, first_exp, n_exp):
    n_src, _, n_tok = idx.shape
    experts = (first_exp + jnp.arange(n_exp, dtype=jnp.int32)).astype(F32)
    hit = idx[:, None] == experts[None, :, None, None]
    member = jnp.any(hit, axis=2)
    gates = jnp.sum(jnp.where(hit, gate[:, None], 0.0), axis=2)
    before = jnp.triu(jnp.ones((n_tok, n_tok), BF16), 1)
    count = jnp.einsum('set,tv->sev', member.astype(BF16), before, preferred_element_type=F32)
    return jnp.where(member, count.astype(jnp.int32), -1), gates


def mix(x, weight):
    return (x.astype(F32) + jnp.einsum('...d,de->...e', x, weight, preferred_element_type=F32)).astype(BF16)


def mix_back(grad, weight):
    return (grad.astype(F32) + jnp.einsum('...e,de->...d', grad, weight, preferred_element_type=F32)).astype(BF16)


def solution(mesh):
    fine = Mesh(mesh.devices.reshape(2, CHIPS, CORES), ('y', 'x', 'c'))
    tok_spec = P(ALL, None)
    exp_spec = P('y', None, None)
    layer_specs = (P(None, None), tok_spec, tok_spec, exp_spec, exp_spec, exp_spec)
    grad_specs = (P(ALL, None), P('y', ('x', 'c'), None), P('y', ('x', 'c'), None), P('y', None, ('x', 'c')))

    def local_step(tokens, dy_out, dense_w1, route_idx1, route_gate1, w_gate1, w_up1, w_down1, dense_w2, route_idx2, route_gate2, w_gate2, w_up2, w_down2):
        n_exp = w_gate1.shape[0] // CORES
        w_gate1, w_up1, w_gate2, w_up2 = (jnp.swapaxes(w, 1, 2) for w in (w_gate1, w_up1, w_gate2, w_up2))
        ix, ic, iy = (lax.axis_index(name) for name in ALL)
        where = jnp.stack([ic, ix]).astype(jnp.int32)
        first_exp = (iy * CORES + ic) * n_exp

        def gather(value):
            return lax.all_gather(value, ALL, axis=0, tiled=False)

        def reduce_own(total):
            return lax.psum_scatter(total, ('c', 'y'), scatter_dimension=0, tiled=False)

        def dense_grad(x, grad):
            part = jnp.einsum('td,te->de', x, grad, preferred_element_type=F32).astype(BF16)
            return lax.psum_scatter(part, ALL, scatter_dimension=0, tiled=True)

        routes = jnp.concatenate([route_idx1.astype(F32), route_idx2.astype(F32), route_gate1, route_gate2], axis=1).T
        routes = gather(routes)
        idx1, idx2, gate1, gate2 = jnp.split(routes, 4, axis=1)
        rank1, gates1 = route_tables(idx1, gate1, first_exp, n_exp)
        rank2, gates2 = route_tables(idx2, gate2, first_exp, n_exp)

        tok_all = gather(tokens)
        dy_all = gather(dy_out)
        u_one = mix(tok_all, dense_w1)
        y_sum = reduce_own(expert_forward(where, u_one, rank1, gates1, w_gate1, w_up1, w_down1))
        y_one = (mix(tokens, dense_w1).astype(F32) + y_sum).astype(BF16)
        u_two = mix(y_one, dense_w2)
        back, gg, gu, gd = layer_backward(True, dy_all, u_two, rank2, gates2, w_gate2, w_up2, w_down2)
        gate_two, up_two, down_two = jnp.swapaxes(gg, 1, 2), jnp.swapaxes(gu, 1, 2), gd
        gm_two = (dy_out.astype(F32) + back).astype(BF16)
        dense_two = dense_grad(y_one, gm_two)
        grad_mid = mix_back(gm_two, dense_w2)
        back, gg, gu, gd = layer_backward(False, u_one, grad_mid, rank1, gates1, w_gate1, w_up1, w_down1)
        gate_one, up_one, down_one = jnp.swapaxes(gg, 1, 2), jnp.swapaxes(gu, 1, 2), gd
        gm_one = (grad_mid.astype(F32) + back).astype(BF16)
        dense_one = dense_grad(tokens, gm_one)
        grad_tok = mix_back(gm_one, dense_w1)
        return (grad_tok, dense_one, gate_one, up_one, down_one, dense_two, gate_two, up_two, down_two)

    return jax.shard_map(local_step, mesh=fine, in_specs=(tok_spec, tok_spec) + layer_specs + layer_specs,
                         out_specs=(tok_spec,) + grad_specs + grad_specs, check_vma=False)
```

```python
import functools

import jax
import jax.numpy as jnp
from jax import lax
from jax.experimental import pallas as pl
from jax.experimental.pallas import tpu as pltpu
from jax.sharding import Mesh, PartitionSpec as P

F32 = jnp.float32
BF16 = jnp.bfloat16
CAP = 64
GROUP = 4
CORES = 2
CHIPS = 2
ALL = ('x', 'c', 'y')
MESH = pl.DeviceIdType.MESH
FLIPS = ((0, 0), (0, 0), (0, 1), (0, 0), (0, 1), (1, 0), (1, 1))
ROUTE = 'yxxcccc'


def matmul(lhs, rhs, lhs_dim=1, rhs_dim=0):
    return lax.dot_general(lhs, rhs, (((lhs_dim,), (rhs_dim,)), ((), ())), preferred_element_type=F32)


def position():
    return tuple(lax.axis_index(name) for name in ALL)


def send(src, dst, sems, at, axis):
    return pltpu.make_async_remote_copy(src, dst, sems[0].at[at], sems[1].at[at],
                                        device_id={axis: 1 - lax.axis_index(axis)}, device_id_type=MESH)


def spreader(mine_ref, peer_ref, sems):
    ix, ic, iy = position()

    def copy(at):
        flip_x, flip_y = FLIPS[at]
        x = 1 - ix if flip_x else ix
        y = 1 - iy if flip_y else iy
        block = peer_ref.at[(x * CORES + ic) * 2 + y]
        return send(block if flip_x or flip_y else mine_ref, block, sems, at, ROUTE[at])

    return copy


def adder(p_ref, rs_ref, sems):
    ix, ic, iy = position()

    def copy(at):
        part = ((1 - ic) * 2 + 1 - iy, (1 - ic) * 2 + iy, ic * 2 + 1 - iy)[at]
        return send(p_ref.at[part], rs_ref.at[at], sems, at, 'ccy'[at])

    return copy


def greet(everyone):
    barrier = pltpu.get_barrier_semaphore()
    if everyone:
        others = [target(hop) for hop in range(1, 8)]
    else:
        others = [{axis: 1 - lax.axis_index(axis)} for axis in ALL]
    for other in others:
        pl.semaphore_signal(barrier, inc=1, device_id=other, device_id_type=MESH)
    pl.semaphore_wait(barrier, len(others))


def rank_of(x, c, y):
    return (x * CORES + c) * 2 + y


def target(hop):
    goal = lax.rem(rank_of(*position()) + hop, 8)
    return {'x': lax.div(goal, 4), 'c': lax.rem(lax.div(goal, 2), 2), 'y': lax.rem(goal, 2)}


def at_step(number):
    return pl.when(pl.program_id(0) == number)


def gate_hidden(x_rows, w_gate, w_up):
    a_pre = matmul(x_rows, w_gate, 1, 1)
    b_pre = matmul(x_rows, w_up, 1, 1)
    return a_pre, b_pre, jax.nn.sigmoid(a_pre)


def select_rows(rank_ref, gate_ref, group, src):
    n_tok = rank_ref.shape[-1]
    slot = lax.broadcasted_iota(jnp.int32, (CAP, n_tok), 0)
    picks, gates = [], []
    for exp in range(GROUP):
        row = pl.ds(group * GROUP + exp, 1)
        hit = slot == rank_ref[src, row, :]
        picks.append(jnp.where(hit, 1.0, 0.0).astype(BF16))
        gates.append(jnp.sum(jnp.where(hit, gate_ref[src, row, :], 0.0), axis=1, keepdims=True))
    return jnp.concatenate(picks, axis=0), jnp.concatenate(gates, axis=0)


def route_table(route_ref, before_ref, src, layer, rank_ref, gate_ref, n_exp):
    _, ic, iy = position()
    n_tok = route_ref.shape[-1]
    experts = ((iy * CORES + ic) * n_exp + lax.broadcasted_iota(jnp.int32, (n_exp, n_tok), 0)).astype(F32)
    member = jnp.zeros((n_exp, n_tok), F32)
    gates = jnp.zeros((n_exp, n_tok), F32)
    for top in range(8):
        hit = experts == route_ref[src, layer * 8 + top:layer * 8 + top + 1, :]
        member = jnp.where(hit, 1.0, member)
        gates = jnp.where(hit, route_ref[src, 16 + layer * 8 + top:17 + layer * 8 + top, :], gates)
    count = matmul(member.astype(BF16), before_ref[...])
    rank_ref[src] = jnp.where(member > 0.0, count, -1.0).astype(jnp.int32)
    gate_ref[src] = gates


def forward_kernel(mine_ref, grad_ref, routes_ref, dense_ref, wg_ref, wu_ref, wd_ref,
                   y_ref, u_ref, uall_ref, dall_ref, rank1_ref, gate1_ref, rank2_ref, gate2_ref,
                   us_ref, ds_ref, route_ref, before_ref, pick_ref, row_ref, x_ref, part_ref, p_ref, rs_ref,
                   u_send, u_recv, d_send, d_recv, t_send, t_recv, rs_send, rs_recv, out_sem):
    n_exp, n_tok = rank1_ref.shape[1:]
    n_group = n_exp // GROUP
    step = pl.program_id(0)
    ix, ic, iy = position()
    me = rank_of(ix, ic, iy)
    spread_u = spreader(mine_ref, us_ref, (u_send, u_recv))
    spread_d = spreader(grad_ref, ds_ref, (d_send, d_recv))
    spread_t = spreader(routes_ref, route_ref, (t_send, t_recv))
    add_up = adder(p_ref, rs_ref, (rs_send, rs_recv))
    stores = ((us_ref, uall_ref), (ds_ref, dall_ref))

    def pass_on(copy, arrived, onward):
        copy(arrived).wait_recv()
        for at in onward:
            copy(at).start()

    @at_step(0)
    def _():
        greet(False)
        for copy in (spread_t, spread_u):
            for at in (0, 3, 1):
                copy(at).start()
        us_ref[me] = mine_ref[...]
        ds_ref[me] = grad_ref[...]
        route_ref[me] = routes_ref[...]
        p_ref[...] = jnp.zeros_like(p_ref)
        before_ref[...] = jnp.where(lax.broadcasted_iota(jnp.int32, (n_tok, n_tok), 0)
                                    < lax.broadcasted_iota(jnp.int32, (n_tok, n_tok), 1), 1.0, 0.0).astype(BF16)
        pass_on(spread_t, 0, (4, 2))
        spread_t(3).wait_recv()
        spread_t(4).wait_recv()

        @pl.loop(0, 4)
        def _(src):
            route_table(route_ref, before_ref, ix * 4 + src, 0, rank1_ref, gate1_ref, n_exp)

        pass_on(spread_u, 0, (4, 2))
        for at in (0, 3, 1):
            spread_d(at).start()
        spread_u(3).wait_recv()
        spread_u(4).wait_recv()

    @at_step(n_group // 4)
    def _():
        pass_on(spread_t, 1, (5,))
        pass_on(spread_u, 1, (5,))

    @at_step(n_group // 2)
    def _():
        pass_on(spread_t, 2, (6,))
        pass_on(spread_u, 2, (6,))
        pass_on(spread_d, 0, (4, 2))

    @at_step(n_group - 1)
    def _():
        spread_t(5).wait_recv()
        spread_t(6).wait_recv()

        @pl.loop(0, 4)
        def _(src):
            route_table(route_ref, before_ref, (1 - ix) * 4 + src, 0, rank1_ref, gate1_ref, n_exp)

        @pl.loop(0, 8)
        def _(src):
            route_table(route_ref, before_ref, src, 1, rank2_ref, gate2_ref, n_exp)

    @at_step(n_group)
    def _():
        add_up(0).start()

    @at_step(n_group + 1)
    def _():
        add_up(2).start()

    @at_step(n_group + n_group // 2)
    def _():
        pass_on(spread_d, 1, (5,))

    @at_step(2 * n_group - 1)
    def _():
        pass_on(spread_d, 2, (6,))
        spread_u(5).wait_recv()
        spread_u(6).wait_recv()
        pltpu.make_async_copy(us_ref, uall_ref, out_sem.at[0]).start()

    group = lax.rem(step, n_group)
    far = 1 - lax.div(step, n_group)
    y_now = jnp.where(far == 1, 1 - iy, iy)

    @pl.loop(0, CORES)
    def _(core):
        src = rank_of(ix, core, y_now)
        pick, gate = select_rows(rank1_ref, gate1_ref, group, src)
        pick_ref[core] = pick
        rows = matmul(pick, us_ref[src]).astype(BF16)
        at = pl.ds(pl.multiple_of(core * CAP, CAP), CAP)
        for exp in range(GROUP):
            x_ref[exp, at, :] = rows[exp * CAP:(exp + 1) * CAP]
            row_ref[exp, at, :] = jnp.broadcast_to(gate[exp * CAP:(exp + 1) * CAP], (CAP, 128))

    @pl.loop(0, GROUP)
    def _(exp):
        a_pre, b_pre, sigma = gate_hidden(x_ref[exp], wg_ref[exp], wu_ref[exp])
        hidden = (a_pre * sigma * b_pre).astype(BF16)
        out = matmul(hidden, wd_ref[exp]).astype(BF16).astype(F32) * row_ref[exp][:, :1]
        high = out.astype(BF16)
        rest = out - high.astype(F32)
        mid = rest.astype(BF16)
        low = (rest - mid.astype(F32)).astype(BF16)
        at = pl.ds(pl.multiple_of(exp * CAP, CAP), CAP)
        for core in range(CORES):
            here = slice(core * CAP, (core + 1) * CAP)
            part_ref[core, 0, at, :] = high[here]
            part_ref[core, 1, at, :] = mid[here]
            part_ref[core, 2, at, :] = low[here]

    @pl.loop(0, CORES)
    def _(core):
        pick = pick_ref[core]
        total = matmul(pick, part_ref[core, 0], 0, 0)
        total += matmul(pick, part_ref[core, 1], 0, 0) + matmul(pick, part_ref[core, 2], 0, 0)
        p_ref[core * 2 + y_now] += total

    @at_step(n_group)
    def _():
        add_up(0).wait_recv()
        p_ref[ic * 2 + 1 - iy] += rs_ref[0]

    @at_step(2 * n_group - 1)
    def _():
        for at in (3, 4, 5, 6):
            spread_d(at).wait_recv()
        pltpu.make_async_copy(ds_ref, dall_ref, out_sem.at[1]).start()
        add_up(1).start()
        add_up(1).wait_recv()
        add_up(2).wait_recv()
        y_own = (mine_ref[...].astype(F32) + (p_ref[ic * 2 + iy] + rs_ref[1] + rs_ref[2])).astype(BF16)
        y_ref[...] = y_own
        u_ref[...] = (y_own.astype(F32) + matmul(y_own, dense_ref[...])).astype(BF16)
        for copy in (spread_u, spread_d, spread_t):
            for at in range(7):
                copy(at).wait_send()
        for at in range(3):
            add_up(at).wait_send()
        for at in range(2):
            pltpu.make_async_copy(*stores[at], out_sem.at[at]).wait()


def layer_kernel(last_layer, *refs):
    refs = list(refs)
    whole_ref, mine_ref, rank_ref, gate_ref, x_own_ref, grad_own_ref, dense_ref, wg_ref, wu_ref, wd_ref = refs[:10]
    del refs[:10]
    if last_layer:
        other_ref = refs.pop(0)
        one_ref, two_ref = refs[1:3]
        del refs[1:3]
    else:
        part_ref = refs.pop(1)
    gx_out_ref, gg_ref, gu_ref, gd_ref = refs[:4]
    (peer_ref, xo_ref, do_ref, h_ref, ga_ref, gb_ref, pick_ref, gx_ref, p_ref, rs_ref, x_ref, d_ref, stage_ref,
     ag_send, ag_recv, rs_send, rs_recv, keep_sem, give_send, give_recv) = refs[4:24]
    if last_layer:
        part_ref, land_ref, land_send, land_recv = refs[24:]
    n_src, _, dim = whole_ref.shape
    own = n_src // CHIPS
    n_group = xo_ref.shape[0] // GROUP
    n_first = 2 * n_group
    n_step = 3 * n_group
    half = dim // CHIPS
    piece = half // CORES
    step = pl.program_id(0)
    ix, ic, iy = position()
    cols = pl.ds(pl.multiple_of(ix * half, half), half)
    u_ref, dy_ref = (whole_ref, peer_ref) if last_layer else (peer_ref, whole_ref)
    outs = (gg_ref, gu_ref, gd_ref)
    spread = spreader(mine_ref, peer_ref, (ag_send, ag_recv))
    add_up = adder(p_ref, rs_ref, (rs_send, rs_recv))

    def land_copy(layer, hop):
        goal = target(hop)
        rows = dim // 8
        src = (part_ref, other_ref)[layer]
        at = pl.ds(pl.multiple_of(rank_of(goal['x'], goal['c'], goal['y']) * rows, rows), rows)
        return pltpu.make_async_remote_copy(src.at[at, :], land_ref.at[layer, hop], land_send.at[layer, hop],
                                            land_recv.at[layer, hop], device_id=goal, device_id_type=MESH)

    def land_sum(layer, out_ref):
        rows = dim // 8
        at = pl.ds(pl.multiple_of(rank_of(ix, ic, iy) * rows, rows), rows)
        total = (part_ref, other_ref)[layer][at, :].astype(F32)
        for hop in range(1, 8):
            land_copy(layer, hop).wait_recv()
            total += land_ref[layer, hop].astype(F32)
        out_ref[...] = total.astype(BF16)

    def store_copies(group, moved):
        buf = lax.rem(group, 2)
        rows = pl.ds(ic * n_group * GROUP + group * GROUP, GROUP)
        for kind in range(3):
            dst = outs[kind].at[rows]
            if moved:
                yield pltpu.make_async_remote_copy(
                    stage_ref.at[buf, 1 - ic, kind], dst, give_send.at[buf, kind], give_recv.at[group, kind],
                    device_id={'c': 1 - ic}, device_id_type=MESH)
            else:
                yield pltpu.make_async_copy(stage_ref.at[buf, ic, kind], dst, keep_sem.at[buf, kind])

    def store_start(group):
        for moved in (True, False):
            for copy in store_copies(group, moved):
                copy.start()

    def store_wait(group):
        for copy in store_copies(group, True):
            copy.wait_send()
        for copy in store_copies(group, False):
            copy.wait()

    def pull(src, group, x_dst, d_dst, base, at, keep):
        pick, gate = select_rows(rank_ref, gate_ref, group, src)
        if keep is not None:
            pick_ref[keep] = pick
        x_rows = matmul(pick, u_ref[src]).astype(BF16)
        d_rows = (matmul(pick, dy_ref[src]) * gate).astype(BF16)
        rows = pl.ds(pl.multiple_of(at * CAP, CAP), CAP)
        for exp in range(GROUP):
            x_dst[base + exp, rows, :] = x_rows[exp * CAP:(exp + 1) * CAP]
            d_dst[base + exp, rows, :] = d_rows[exp * CAP:(exp + 1) * CAP]

    def hidden_grads(x_rows, d_rows, exp):
        a_pre, b_pre, sigma = gate_hidden(x_rows, wg_ref[exp], wu_ref[exp])
        silu = a_pre * sigma
        grad_hidden = matmul(d_rows, wd_ref[exp], 1, 1).astype(BF16).astype(F32)
        grad_a = (grad_hidden * b_pre * sigma * (1.0 + a_pre * (1.0 - sigma))).astype(BF16)
        return (silu * b_pre).astype(BF16), grad_a, (grad_hidden * silu).astype(BF16)

    @at_step(0)
    def _():
        greet(last_layer)
        for at in (0, 3, 1):
            spread(at).start()
        if last_layer:
            for hop in range(1, 8):
                land_copy(1, hop).start()
        peer_ref[rank_of(ix, ic, iy)] = mine_ref[...]
        p_ref[...] = jnp.zeros_like(p_ref)
        spread(3).wait_recv()

    @at_step(n_group // 2)
    def _():
        spread(0).wait_recv()
        spread(4).start()
        spread(2).start()

    @at_step(n_group)
    def _():
        spread(4).wait_recv()

    @at_step(n_group + n_group // 2)
    def _():
        spread(1).wait_recv()
        spread(5).start()

    @at_step(n_first - 1)
    def _():
        spread(2).wait_recv()
        spread(6).start()

    @pl.when(step < n_first)
    def _():
        group = lax.rem(step, n_group)
        late = lax.div(step, n_group)
        y_now = jnp.where(late == 1, 1 - iy, iy)
        base = group * GROUP
        rows = pl.ds(pl.multiple_of(late * CORES * CAP, CORES * CAP), CORES * CAP)

        @pl.loop(0, CORES)
        def _(core):
            pull(rank_of(ix, core, y_now), group, xo_ref, do_ref, base, late * CORES + core, core)

        @pl.loop(0, GROUP)
        def _(exp):
            hidden, grad_a, grad_b = hidden_grads(xo_ref[base + exp, rows, :], do_ref[base + exp, rows, :], exp)
            h_ref[base + exp, rows, :] = hidden
            ga_ref[base + exp, rows, :] = grad_a
            gb_ref[base + exp, rows, :] = grad_b
            grad_x = (matmul(grad_a, wg_ref[exp]) + matmul(grad_b, wu_ref[exp])).astype(BF16)
            at = pl.ds(pl.multiple_of(exp * CAP, CAP), CAP)
            for core in range(CORES):
                gx_ref[core, at, :] = grad_x[core * CAP:(core + 1) * CAP]

        @pl.loop(0, CORES)
        def _(core):
            p_ref[core * 2 + y_now] += matmul(pick_ref[core], gx_ref[core], 0, 0)

    @at_step(n_first)
    def _():
        add_up(0).start()
        add_up(1).start()
        spread(5).wait_recv()
        spread(6).wait_recv()

    @at_step(n_first + 1)
    def _():
        add_up(2).start()

    @at_step(n_step - 1)
    def _():
        add_up(1).wait_recv()
        add_up(2).wait_recv()
        total = p_ref[ic * 2 + iy] + rs_ref[1] + rs_ref[2]
        grad = (grad_own_ref[...].astype(F32) + total).astype(BF16)
        part_ref[...] = matmul(x_own_ref[...], grad, 0, 0).astype(BF16)
        gx_out_ref[...] = (grad.astype(F32) + matmul(grad, dense_ref[...], 1, 1)).astype(BF16)
        if last_layer:
            for hop in range(1, 8):
                land_copy(0, hop).start()

    @pl.when(step >= n_first)
    def _():
        group = step - n_first

        @pl.when(group >= 1)
        def _():
            store_start(group - 1)

        @pl.loop(0, own)
        def _(src):
            pull((1 - ix) * own + src, group, x_ref, d_ref, 0, src, None)

        @pl.when(group >= 2)
        def _():
            store_wait(group - 2)

        buf = lax.rem(group, 2)

        @pl.loop(0, GROUP)
        def _(exp):
            base = group * GROUP + exp
            hidden, grad_a, grad_b = hidden_grads(x_ref[exp], d_ref[exp], exp)
            x_own, x_far = xo_ref[base, :, cols], x_ref[exp, :, cols]
            d_own, d_far = do_ref[base, :, cols], d_ref[exp, :, cols]
            grads = (matmul(ga_ref[base], x_own, 0, 0) + matmul(grad_a, x_far, 0, 0),
                     matmul(gb_ref[base], x_own, 0, 0) + matmul(grad_b, x_far, 0, 0),
                     matmul(h_ref[base], d_own, 0, 0) + matmul(hidden, d_far, 0, 0))
            for kind in range(3):
                for core in range(CORES):
                    stage_ref[buf, core, kind, exp] = grads[kind][:, core * piece:(core + 1) * piece].astype(BF16)

    @at_step(n_first)
    def _():
        add_up(0).wait_recv()
        p_ref[ic * 2 + 1 - iy] += rs_ref[0]

    @at_step(n_step - 1)
    def _():
        last = n_group - 1
        store_wait(last - 1)
        store_start(last)
        if last_layer:
            land_sum(1, two_ref)
            land_sum(0, one_ref)
            for layer in range(2):
                for hop in range(1, 8):
                    land_copy(layer, hop).wait_send()
        for at in range(7):
            spread(at).wait_send()
        for at in range(3):
            add_up(at).wait_send()
        store_wait(last)
        for group in range(n_group):
            for copy in store_copies(group, True):
                copy.wait_recv()


def fixed(*shape):
    return pl.BlockSpec(shape, lambda s: (0,) * len(shape), pipeline_mode=pl.Buffered(1))


def weight_spec(groups, ff, dim):
    return pl.BlockSpec((GROUP, ff, dim), lambda s: (lax.axis_index('c') * groups + lax.rem(s, groups), 0, 0))


def dma_sems(*shape):
    return pltpu.SemaphoreType.DMA(shape)


def sums_scratch(own, n_tok, dim):
    return [pltpu.VMEM((own, n_tok, dim), F32), pltpu.VMEM((3, n_tok, dim), F32)]


def layer_forward(mine, grad, routes, dense, w_gate, w_up, w_down):
    n_tok, dim = mine.shape
    n_all, ff, _ = w_gate.shape
    n_exp = n_all // CORES
    n_src = 8
    own = n_src // CHIPS
    groups = n_exp // GROUP
    tall = weight_spec(groups, ff, dim)
    table = fixed(n_src, n_exp, n_tok)
    block = jax.ShapeDtypeStruct((n_tok, dim), BF16)
    every = jax.ShapeDtypeStruct((n_src, n_tok, dim), BF16)
    ranks = jax.ShapeDtypeStruct((n_src, n_exp, n_tok), jnp.int32)
    gates = jax.ShapeDtypeStruct((n_src, n_exp, n_tok), F32)
    anywhere = pl.BlockSpec(memory_space=pl.ANY)
    rows = CORES * CAP
    return pl.pallas_call(
        forward_kernel,
        out_shape=(block, block, every, every, ranks, gates, ranks, gates),
        grid_spec=pltpu.PrefetchScalarGridSpec(
            num_scalar_prefetch=0, grid=(2 * groups,),
            in_specs=[fixed(n_tok, dim), fixed(n_tok, dim), fixed(*routes.shape), fixed(dim, dim), tall, tall, tall],
            out_specs=(fixed(n_tok, dim), fixed(n_tok, dim), anywhere, anywhere, table, table, table, table),
            scratch_shapes=[pltpu.VMEM((n_src, n_tok, dim), BF16), pltpu.VMEM((n_src, n_tok, dim), BF16),
                            pltpu.VMEM((n_src,) + routes.shape, F32), pltpu.VMEM((n_tok, n_tok), BF16),
                            pltpu.VMEM((CORES, GROUP * CAP, n_tok), BF16), pltpu.VMEM((GROUP, rows, 128), F32),
                            pltpu.VMEM((GROUP, rows, dim), BF16), pltpu.VMEM((CORES, 3, GROUP * CAP, dim), BF16)]
            + sums_scratch(own, n_tok, dim)
            + [dma_sems(7)] * 6 + [dma_sems(3)] * 2 + [dma_sems(2)]),
        compiler_params=pltpu.CompilerParams(dimension_semantics=('arbitrary',), vmem_limit_bytes=62 << 20,
                                             collective_id=0, has_side_effects=True),
    )(mine, grad, routes, dense, w_gate, w_up, w_down)


def layer_backward(whole, mine, rank, gate, x_own, grad_own, dense, w_gate, w_up, w_down, other=None):
    n_src, n_tok, dim = whole.shape
    n_all, ff, _ = w_gate.shape
    n_exp = rank.shape[1]
    own = n_src // CHIPS
    piece = dim // (CHIPS * CORES)
    groups = n_exp // GROUP
    kept = own * CAP
    last_layer = other is not None
    tall = weight_spec(groups, ff, dim)
    table = fixed(n_src, n_exp, n_tok)
    block = fixed(n_tok, dim)
    square = fixed(dim, dim)
    slab = fixed(dim // 8, dim)
    grad_shape = jax.ShapeDtypeStruct((n_all, ff, piece), BF16)
    part_shape = jax.ShapeDtypeStruct((dim, dim), BF16)
    slab_shape = jax.ShapeDtypeStruct((dim // 8, dim), BF16)
    extra_shapes = (slab_shape, slab_shape) if last_layer else (part_shape,)
    extra_specs = (slab, slab) if last_layer else (square,)
    scratch = [pltpu.VMEM((n_src, n_tok, dim), BF16), pltpu.VMEM((n_exp, kept, dim), BF16),
               pltpu.VMEM((n_exp, kept, dim), BF16), pltpu.VMEM((n_exp, kept, ff), BF16),
               pltpu.VMEM((n_exp, kept, ff), BF16), pltpu.VMEM((n_exp, kept, ff), BF16),
               pltpu.VMEM((CORES, GROUP * CAP, n_tok), BF16), pltpu.VMEM((CORES, GROUP * CAP, dim), BF16)]
    scratch += sums_scratch(own, n_tok, dim)
    scratch += [pltpu.VMEM((GROUP, kept, dim), BF16), pltpu.VMEM((GROUP, kept, dim), BF16),
                pltpu.VMEM((2, CORES, 3, GROUP, ff, piece), BF16),
                dma_sems(7), dma_sems(7), dma_sems(3), dma_sems(3), dma_sems(2, 3), dma_sems(2, 3), dma_sems(groups, 3)]
    if last_layer:
        scratch += [pltpu.VMEM((dim, dim), BF16), pltpu.VMEM((2, 8, dim // 8, dim), BF16), dma_sems(2, 8), dma_sems(2, 8)]
    operands = (whole, mine, rank, gate, x_own, grad_own, dense, w_gate, w_up, w_down) + ((other,) if last_layer else ())
    return pl.pallas_call(
        functools.partial(layer_kernel, last_layer),
        out_shape=(jax.ShapeDtypeStruct((n_tok, dim), BF16),) + extra_shapes + (grad_shape,) * 3,
        grid_spec=pltpu.PrefetchScalarGridSpec(
            num_scalar_prefetch=0, grid=(3 * groups,),
            in_specs=[fixed(n_src, n_tok, dim), block, table, table, block, block, square, tall, tall, tall]
            + ([square] if last_layer else []),
            out_specs=(block,) + extra_specs + (pl.BlockSpec(memory_space=pl.ANY),) * 3,
            scratch_shapes=scratch),
        compiler_params=pltpu.CompilerParams(dimension_semantics=('arbitrary',), vmem_limit_bytes=67043328,
                                             collective_id=1 + int(last_layer), has_side_effects=True),
    )(*operands)


def mix(x, weight):
    return (x.astype(F32) + jnp.dot(x, weight, preferred_element_type=F32)).astype(BF16)


def solution(mesh):
    fine = Mesh(mesh.devices.reshape(2, CHIPS, CORES), ('y', 'x', 'c'))
    tok_spec = P(ALL, None)
    exp_spec = P('y', None, None)
    layer_specs = (P(None, None), tok_spec, tok_spec, exp_spec, exp_spec, exp_spec)
    grad_specs = (P(ALL, None), P('y', ('x', 'c'), None), P('y', ('x', 'c'), None), P('y', None, ('x', 'c')))

    def local_step(tokens, dy_out, dense_w1, route_idx1, route_gate1, w_gate1, w_up1, w_down1, dense_w2, route_idx2, route_gate2, w_gate2, w_up2, w_down2):
        w_gate1, w_up1, w_gate2, w_up2 = (jnp.swapaxes(w, 1, 2) for w in (w_gate1, w_up1, w_gate2, w_up2))
        routes = jnp.concatenate([route_idx1.astype(F32).T, route_idx2.astype(F32).T, route_gate1.T, route_gate2.T], axis=0)
        u_one = mix(tokens, dense_w1)
        y_one, u_two, u_all, dy_all, rank1, gate1, rank2, gate2 = layer_forward(
            u_one, dy_out, routes, dense_w2, w_gate1, w_up1, w_down1)
        grad_mid, part_two, gg, gu, gd = layer_backward(
            dy_all, u_two, rank2, gate2, y_one, dy_out, dense_w2, w_gate2, w_up2, w_down2)
        gate_two, up_two, down_two = jnp.swapaxes(gg, 1, 2), jnp.swapaxes(gu, 1, 2), gd
        grad_tok, dense_one, dense_two, gg, gu, gd = layer_backward(
            u_all, grad_mid, rank1, gate1, tokens, grad_mid, dense_w1, w_gate1, w_up1, w_down1, part_two)
        gate_one, up_one, down_one = jnp.swapaxes(gg, 1, 2), jnp.swapaxes(gu, 1, 2), gd
        return (grad_tok, dense_one, gate_one, up_one, down_one, dense_two, gate_two, up_two, down_two)

    return jax.shard_map(local_step, mesh=fine, in_specs=(tok_spec, tok_spec) + layer_specs + layer_specs,
                         out_specs=(tok_spec,) + grad_specs + grad_specs, check_vma=False)
```

```python
import functools

import jax
import jax.numpy as jnp
from jax import lax
from jax.experimental import pallas as pl
from jax.experimental.pallas import tpu as pltpu
from jax.sharding import Mesh, PartitionSpec as P

F32 = jnp.float32
BF16 = jnp.bfloat16
CAP = 64
GROUP = 4
CORES = 2
CHIPS = 2
ALL = ('x', 'c', 'y')
MESH = pl.DeviceIdType.MESH
FLIPS = ((0, 0), (0, 0), (0, 1), (0, 0), (0, 1), (1, 0), (1, 1))
ROUTE = 'yxxcccc'


def matmul(lhs, rhs, lhs_dim=1, rhs_dim=0):
    return lax.dot_general(lhs, rhs, (((lhs_dim,), (rhs_dim,)), ((), ())), preferred_element_type=F32)


def position():
    return tuple(lax.axis_index(name) for name in ALL)


def send(src, dst, sems, at, axis):
    return pltpu.make_async_remote_copy(src, dst, sems[0].at[at], sems[1].at[at],
                                        device_id={axis: 1 - lax.axis_index(axis)}, device_id_type=MESH)


def spreader(mine_ref, peer_ref, sems):
    ix, ic, iy = position()

    def copy(at):
        flip_x, flip_y = FLIPS[at]
        x = 1 - ix if flip_x else ix
        y = 1 - iy if flip_y else iy
        block = peer_ref.at[(x * CORES + ic) * 2 + y]
        return send(block if flip_x or flip_y else mine_ref, block, sems, at, ROUTE[at])

    return copy


def adder(p_ref, rs_ref, sems):
    ix, ic, iy = position()

    def copy(at):
        part = ((1 - ic) * 2 + 1 - iy, (1 - ic) * 2 + iy, ic * 2 + 1 - iy)[at]
        return send(p_ref.at[part], rs_ref.at[at], sems, at, 'ccy'[at])

    return copy


def greet(everyone):
    barrier = pltpu.get_barrier_semaphore()
    if everyone:
        others = [target(hop) for hop in range(1, 8)]
    else:
        others = [{axis: 1 - lax.axis_index(axis)} for axis in ALL]
    for other in others:
        pl.semaphore_signal(barrier, inc=1, device_id=other, device_id_type=MESH)
    pl.semaphore_wait(barrier, len(others))


def rank_of(x, c, y):
    return (x * CORES + c) * 2 + y


def target(hop):
    goal = lax.rem(rank_of(*position()) + hop, 8)
    return {'x': lax.div(goal, 4), 'c': lax.rem(lax.div(goal, 2), 2), 'y': lax.rem(goal, 2)}


def at_step(number):
    return pl.when(pl.program_id(0) == number)


def gate_hidden(x_rows, w_gate, w_up):
    a_pre = matmul(x_rows, w_gate, 1, 1)
    b_pre = matmul(x_rows, w_up, 1, 1)
    return a_pre, b_pre, jax.nn.sigmoid(a_pre)


def select_rows(rank_ref, gate_ref, group, src):
    n_tok = rank_ref.shape[-1]
    slot = lax.broadcasted_iota(jnp.int32, (CAP, n_tok), 0)
    picks, gates = [], []
    for exp in range(GROUP):
        row = pl.ds(group * GROUP + exp, 1)
        hit = slot == rank_ref[src, row, :]
        picks.append(jnp.where(hit, 1.0, 0.0).astype(BF16))
        gates.append(jnp.sum(jnp.where(hit, gate_ref[src, row, :], 0.0), axis=1, keepdims=True))
    return jnp.concatenate(picks, axis=0), jnp.concatenate(gates, axis=0)


def route_table(route_ref, before_ref, src, layer, rank_ref, gate_ref, n_exp):
    _, ic, iy = position()
    n_tok = route_ref.shape[-1]
    experts = ((iy * CORES + ic) * n_exp + lax.broadcasted_iota(jnp.int32, (n_exp, n_tok), 0)).astype(F32)
    member = jnp.zeros((n_exp, n_tok), F32)
    gates = jnp.zeros((n_exp, n_tok), F32)
    for top in range(8):
        hit = experts == route_ref[src, layer * 8 + top:layer * 8 + top + 1, :]
        member = jnp.where(hit, 1.0, member)
        gates = jnp.where(hit, route_ref[src, 16 + layer * 8 + top:17 + layer * 8 + top, :], gates)
    count = matmul(member.astype(BF16), before_ref[...])
    rank_ref[src] = jnp.where(member > 0.0, count, -1.0).astype(jnp.int32)
    gate_ref[src] = gates


def forward_kernel(mine_ref, grad_ref, routes_ref, dense_ref, wg_ref, wu_ref, wd_ref,
                   y_ref, u_ref, uall_ref, dall_ref, rank1_ref, gate1_ref, rank2_ref, gate2_ref,
                   us_ref, ds_ref, route_ref, before_ref, pick_ref, row_ref, x_ref, part_ref, p_ref, rs_ref,
                   u_send, u_recv, d_send, d_recv, t_send, t_recv, rs_send, rs_recv, out_sem):
    n_exp, n_tok = rank1_ref.shape[1:]
    n_group = n_exp // GROUP
    step = pl.program_id(0)
    ix, ic, iy = position()
    me = rank_of(ix, ic, iy)
    spread_u = spreader(mine_ref, us_ref, (u_send, u_recv))
    spread_d = spreader(grad_ref, ds_ref, (d_send, d_recv))
    spread_t = spreader(routes_ref, route_ref, (t_send, t_recv))
    add_up = adder(p_ref, rs_ref, (rs_send, rs_recv))
    stores = ((us_ref, uall_ref), (ds_ref, dall_ref))

    def pass_on(copy, arrived, onward):
        copy(arrived).wait_recv()
        for at in onward:
            copy(at).start()

    @at_step(0)
    def _():
        greet(False)
        for copy in (spread_t, spread_u):
            for at in (0, 3, 1):
                copy(at).start()
        us_ref[me] = mine_ref[...]
        ds_ref[me] = grad_ref[...]
        route_ref[me] = routes_ref[...]
        p_ref[...] = jnp.zeros_like(p_ref)
        before_ref[...] = jnp.where(lax.broadcasted_iota(jnp.int32, (n_tok, n_tok), 0)
                                    < lax.broadcasted_iota(jnp.int32, (n_tok, n_tok), 1), 1.0, 0.0).astype(BF16)
        pass_on(spread_t, 0, (4, 2))
        spread_t(3).wait_recv()
        spread_t(4).wait_recv()

        @pl.loop(0, 4)
        def _(src):
            route_table(route_ref, before_ref, ix * 4 + src, 0, rank1_ref, gate1_ref, n_exp)

        pass_on(spread_u, 0, (4, 2))
        for at in (0, 3, 1):
            spread_d(at).start()
        spread_u(3).wait_recv()
        spread_u(4).wait_recv()

    @at_step(n_group // 4)
    def _():
        pass_on(spread_t, 1, (5,))
        pass_on(spread_u, 1, (5,))

    @at_step(n_group // 2)
    def _():
        pass_on(spread_t, 2, (6,))
        pass_on(spread_u, 2, (6,))
        pass_on(spread_d, 0, (4, 2))

    @at_step(n_group - 1)
    def _():
        spread_t(5).wait_recv()
        spread_t(6).wait_recv()

        @pl.loop(0, 4)
        def _(src):
            route_table(route_ref, before_ref, (1 - ix) * 4 + src, 0, rank1_ref, gate1_ref, n_exp)

        @pl.loop(0, 8)
        def _(src):
            route_table(route_ref, before_ref, src, 1, rank2_ref, gate2_ref, n_exp)

    @at_step(n_group)
    def _():
        add_up(0).start()

    @at_step(n_group + 1)
    def _():
        add_up(2).start()

    @at_step(n_group + n_group // 2)
    def _():
        pass_on(spread_d, 1, (5,))

    @at_step(2 * n_group - 1)
    def _():
        pass_on(spread_d, 2, (6,))
        spread_u(5).wait_recv()
        spread_u(6).wait_recv()
        pltpu.make_async_copy(us_ref, uall_ref, out_sem.at[0]).start()

    group = lax.rem(step, n_group)
    far = 1 - lax.div(step, n_group)
    y_now = jnp.where(far == 1, 1 - iy, iy)

    for core in range(CORES):
        src = rank_of(ix, core, y_now)
        pick, gate = select_rows(rank1_ref, gate1_ref, group, src)
        pick_ref[core] = pick
        rows = matmul(pick, us_ref[src]).astype(BF16)
        at = slice(core * CAP, (core + 1) * CAP)
        for exp in range(GROUP):
            x_ref[exp, at, :] = rows[exp * CAP:(exp + 1) * CAP]
            row_ref[exp, at, :] = jnp.broadcast_to(gate[exp * CAP:(exp + 1) * CAP], (CAP, 128))

    for exp in range(GROUP):
        a_pre, b_pre, sigma = gate_hidden(x_ref[exp], wg_ref[exp], wu_ref[exp])
        hidden = (a_pre * sigma * b_pre).astype(BF16)
        out = matmul(hidden, wd_ref[exp]).astype(BF16).astype(F32) * row_ref[exp][:, :1]
        high = out.astype(BF16)
        rest = out - high.astype(F32)
        mid = rest.astype(BF16)
        low = (rest - mid.astype(F32)).astype(BF16)
        at = slice(exp * CAP, (exp + 1) * CAP)
        for core in range(CORES):
            here = slice(core * CAP, (core + 1) * CAP)
            part_ref[core, 0, at, :] = high[here]
            part_ref[core, 1, at, :] = mid[here]
            part_ref[core, 2, at, :] = low[here]

    for core in range(CORES):
        pick = pick_ref[core]
        total = matmul(pick, part_ref[core, 0], 0, 0)
        total += matmul(pick, part_ref[core, 1], 0, 0) + matmul(pick, part_ref[core, 2], 0, 0)
        p_ref[core * 2 + y_now] += total

    @at_step(n_group)
    def _():
        add_up(0).wait_recv()
        p_ref[ic * 2 + 1 - iy] += rs_ref[0]

    @at_step(2 * n_group - 1)
    def _():
        for at in (3, 4, 5, 6):
            spread_d(at).wait_recv()
        pltpu.make_async_copy(ds_ref, dall_ref, out_sem.at[1]).start()
        add_up(1).start()
        add_up(1).wait_recv()
        add_up(2).wait_recv()
        y_own = (mine_ref[...].astype(F32) + (p_ref[ic * 2 + iy] + rs_ref[1] + rs_ref[2])).astype(BF16)
        y_ref[...] = y_own
        u_ref[...] = (y_own.astype(F32) + matmul(y_own, dense_ref[...])).astype(BF16)
        for copy in (spread_u, spread_d, spread_t):
            for at in range(7):
                copy(at).wait_send()
        for at in range(3):
            add_up(at).wait_send()
        for at in range(2):
            pltpu.make_async_copy(*stores[at], out_sem.at[at]).wait()


def layer_kernel(last_layer, *refs):
    refs = list(refs)
    whole_ref, mine_ref, rank_ref, gate_ref, x_own_ref, grad_own_ref, dense_ref, wg_ref, wu_ref, wd_ref = refs[:10]
    del refs[:10]
    if last_layer:
        other_ref = refs.pop(0)
        one_ref, two_ref = refs[1:3]
        del refs[1:3]
    else:
        part_ref = refs.pop(1)
    gx_out_ref, gg_ref, gu_ref, gd_ref = refs[:4]
    (peer_ref, xo_ref, do_ref, h_ref, ga_ref, gb_ref, pick_ref, gx_ref, p_ref, rs_ref, x_ref, d_ref, stage_ref,
     ag_send, ag_recv, rs_send, rs_recv, keep_sem, give_send, give_recv) = refs[4:24]
    if last_layer:
        part_ref, land_ref, land_send, land_recv = refs[24:]
    n_src, _, dim = whole_ref.shape
    own = n_src // CHIPS
    n_group = xo_ref.shape[0] // GROUP
    n_first = 2 * n_group
    n_step = 3 * n_group
    half = dim // CHIPS
    piece = half // CORES
    step = pl.program_id(0)
    ix, ic, iy = position()
    cols = pl.ds(pl.multiple_of(ix * half, half), half)
    u_ref, dy_ref = (whole_ref, peer_ref) if last_layer else (peer_ref, whole_ref)
    outs = (gg_ref, gu_ref, gd_ref)
    spread = spreader(mine_ref, peer_ref, (ag_send, ag_recv))
    add_up = adder(p_ref, rs_ref, (rs_send, rs_recv))

    def land_copy(layer, hop):
        goal = target(hop)
        rows = dim // 8
        src = (part_ref, other_ref)[layer]
        at = pl.ds(pl.multiple_of(rank_of(goal['x'], goal['c'], goal['y']) * rows, rows), rows)
        return pltpu.make_async_remote_copy(src.at[at, :], land_ref.at[layer, hop], land_send.at[layer, hop],
                                            land_recv.at[layer, hop], device_id=goal, device_id_type=MESH)

    def land_sum(layer, out_ref):
        rows = dim // 8
        at = pl.ds(pl.multiple_of(rank_of(ix, ic, iy) * rows, rows), rows)
        total = (part_ref, other_ref)[layer][at, :].astype(F32)
        for hop in range(1, 8):
            land_copy(layer, hop).wait_recv()
            total += land_ref[layer, hop].astype(F32)
        out_ref[...] = total.astype(BF16)

    def store_copies(group, moved):
        buf = lax.rem(group, 2)
        rows = pl.ds(ic * n_group * GROUP + group * GROUP, GROUP)
        for kind in range(3):
            dst = outs[kind].at[rows]
            if moved:
                yield pltpu.make_async_remote_copy(
                    stage_ref.at[buf, 1 - ic, kind], dst, give_send.at[buf, kind], give_recv.at[group, kind],
                    device_id={'c': 1 - ic}, device_id_type=MESH)
            else:
                yield pltpu.make_async_copy(stage_ref.at[buf, ic, kind], dst, keep_sem.at[buf, kind])

    def store_start(group):
        for moved in (True, False):
            for copy in store_copies(group, moved):
                copy.start()

    def store_wait(group):
        for copy in store_copies(group, True):
            copy.wait_send()
        for copy in store_copies(group, False):
            copy.wait()

    def pull(src, group, x_dst, d_dst, base, at, keep):
        pick, gate = select_rows(rank_ref, gate_ref, group, src)
        if keep is not None:
            pick_ref[keep] = pick
        x_rows = matmul(pick, u_ref[src]).astype(BF16)
        d_rows = (matmul(pick, dy_ref[src]) * gate).astype(BF16)
        rows = pl.ds(pl.multiple_of(at * CAP, CAP), CAP)
        for exp in range(GROUP):
            x_dst[base + exp, rows, :] = x_rows[exp * CAP:(exp + 1) * CAP]
            d_dst[base + exp, rows, :] = d_rows[exp * CAP:(exp + 1) * CAP]

    def hidden_grads(x_rows, d_rows, exp):
        a_pre, b_pre, sigma = gate_hidden(x_rows, wg_ref[exp], wu_ref[exp])
        silu = a_pre * sigma
        grad_hidden = matmul(d_rows, wd_ref[exp], 1, 1).astype(BF16).astype(F32)
        grad_a = (grad_hidden * b_pre * sigma * (1.0 + a_pre * (1.0 - sigma))).astype(BF16)
        return (silu * b_pre).astype(BF16), grad_a, (grad_hidden * silu).astype(BF16)

    @at_step(0)
    def _():
        greet(last_layer)
        for at in (0, 3, 1):
            spread(at).start()
        if last_layer:
            for hop in range(1, 8):
                land_copy(1, hop).start()
        peer_ref[rank_of(ix, ic, iy)] = mine_ref[...]
        p_ref[...] = jnp.zeros_like(p_ref)
        spread(3).wait_recv()

    @at_step(n_group // 2)
    def _():
        spread(0).wait_recv()
        spread(4).start()
        spread(2).start()

    @at_step(n_group)
    def _():
        spread(4).wait_recv()

    @at_step(n_group + n_group // 2)
    def _():
        spread(1).wait_recv()
        spread(5).start()

    @at_step(n_first - 1)
    def _():
        spread(2).wait_recv()
        spread(6).start()

    @pl.when(step < n_first)
    def _():
        group = lax.rem(step, n_group)
        late = lax.div(step, n_group)
        y_now = jnp.where(late == 1, 1 - iy, iy)
        base = group * GROUP
        rows = pl.ds(pl.multiple_of(late * CORES * CAP, CORES * CAP), CORES * CAP)

        for core in range(CORES):
            pull(rank_of(ix, core, y_now), group, xo_ref, do_ref, base, late * CORES + core, core)

        for exp in range(GROUP):
            hidden, grad_a, grad_b = hidden_grads(xo_ref[base + exp, rows, :], do_ref[base + exp, rows, :], exp)
            h_ref[base + exp, rows, :] = hidden
            ga_ref[base + exp, rows, :] = grad_a
            gb_ref[base + exp, rows, :] = grad_b
            grad_x = (matmul(grad_a, wg_ref[exp]) + matmul(grad_b, wu_ref[exp])).astype(BF16)
            at = slice(exp * CAP, (exp + 1) * CAP)
            for core in range(CORES):
                gx_ref[core, at, :] = grad_x[core * CAP:(core + 1) * CAP]

        for core in range(CORES):
            p_ref[core * 2 + y_now] += matmul(pick_ref[core], gx_ref[core], 0, 0)

    @at_step(n_first)
    def _():
        add_up(0).start()
        add_up(1).start()
        spread(5).wait_recv()
        spread(6).wait_recv()

    @at_step(n_first + 1)
    def _():
        add_up(2).start()

    @at_step(n_step - 1)
    def _():
        add_up(1).wait_recv()
        add_up(2).wait_recv()
        total = p_ref[ic * 2 + iy] + rs_ref[1] + rs_ref[2]
        grad = (grad_own_ref[...].astype(F32) + total).astype(BF16)
        part_ref[...] = matmul(x_own_ref[...], grad, 0, 0).astype(BF16)
        gx_out_ref[...] = (grad.astype(F32) + matmul(grad, dense_ref[...], 1, 1)).astype(BF16)
        if last_layer:
            for hop in range(1, 8):
                land_copy(0, hop).start()

    @pl.when(step >= n_first)
    def _():
        group = step - n_first

        @pl.when(group >= 1)
        def _():
            store_start(group - 1)

        for src in range(own):
            pull((1 - ix) * own + src, group, x_ref, d_ref, 0, src, None)

        @pl.when(group >= 2)
        def _():
            store_wait(group - 2)

        buf = lax.rem(group, 2)

        for exp in range(GROUP):
            base = group * GROUP + exp
            hidden, grad_a, grad_b = hidden_grads(x_ref[exp], d_ref[exp], exp)
            x_own, x_far = xo_ref[base, :, cols], x_ref[exp, :, cols]
            d_own, d_far = do_ref[base, :, cols], d_ref[exp, :, cols]
            grads = (matmul(ga_ref[base], x_own, 0, 0) + matmul(grad_a, x_far, 0, 0),
                     matmul(gb_ref[base], x_own, 0, 0) + matmul(grad_b, x_far, 0, 0),
                     matmul(h_ref[base], d_own, 0, 0) + matmul(hidden, d_far, 0, 0))
            for kind in range(3):
                for core in range(CORES):
                    stage_ref[buf, core, kind, exp] = grads[kind][:, core * piece:(core + 1) * piece].astype(BF16)

    @at_step(n_first)
    def _():
        add_up(0).wait_recv()
        p_ref[ic * 2 + 1 - iy] += rs_ref[0]

    @at_step(n_step - 1)
    def _():
        last = n_group - 1
        store_wait(last - 1)
        store_start(last)
        if last_layer:
            land_sum(1, two_ref)
            land_sum(0, one_ref)
            for layer in range(2):
                for hop in range(1, 8):
                    land_copy(layer, hop).wait_send()
        for at in range(7):
            spread(at).wait_send()
        for at in range(3):
            add_up(at).wait_send()
        store_wait(last)
        for group in range(n_group):
            for copy in store_copies(group, True):
                copy.wait_recv()


def fixed(*shape):
    return pl.BlockSpec(shape, lambda s: (0,) * len(shape), pipeline_mode=pl.Buffered(1))


def weight_spec(groups, ff, dim):
    return pl.BlockSpec((GROUP, ff, dim), lambda s: (lax.axis_index('c') * groups + lax.rem(s, groups), 0, 0))


def dma_sems(*shape):
    return pltpu.SemaphoreType.DMA(shape)


def sums_scratch(own, n_tok, dim):
    return [pltpu.VMEM((own, n_tok, dim), F32), pltpu.VMEM((3, n_tok, dim), F32)]


def layer_forward(mine, grad, routes, dense, w_gate, w_up, w_down):
    n_tok, dim = mine.shape
    n_all, ff, _ = w_gate.shape
    n_exp = n_all // CORES
    n_src = 8
    own = n_src // CHIPS
    groups = n_exp // GROUP
    tall = weight_spec(groups, ff, dim)
    table = fixed(n_src, n_exp, n_tok)
    block = jax.ShapeDtypeStruct((n_tok, dim), BF16)
    every = jax.ShapeDtypeStruct((n_src, n_tok, dim), BF16)
    ranks = jax.ShapeDtypeStruct((n_src, n_exp, n_tok), jnp.int32)
    gates = jax.ShapeDtypeStruct((n_src, n_exp, n_tok), F32)
    anywhere = pl.BlockSpec(memory_space=pl.ANY)
    rows = CORES * CAP
    return pl.pallas_call(
        forward_kernel,
        out_shape=(block, block, every, every, ranks, gates, ranks, gates),
        grid_spec=pltpu.PrefetchScalarGridSpec(
            num_scalar_prefetch=0, grid=(2 * groups,),
            in_specs=[fixed(n_tok, dim), fixed(n_tok, dim), fixed(*routes.shape), fixed(dim, dim), tall, tall, tall],
            out_specs=(fixed(n_tok, dim), fixed(n_tok, dim), anywhere, anywhere, table, table, table, table),
            scratch_shapes=[pltpu.VMEM((n_src, n_tok, dim), BF16), pltpu.VMEM((n_src, n_tok, dim), BF16),
                            pltpu.VMEM((n_src,) + routes.shape, F32), pltpu.VMEM((n_tok, n_tok), BF16),
                            pltpu.VMEM((CORES, GROUP * CAP, n_tok), BF16), pltpu.VMEM((GROUP, rows, 128), F32),
                            pltpu.VMEM((GROUP, rows, dim), BF16), pltpu.VMEM((CORES, 3, GROUP * CAP, dim), BF16)]
            + sums_scratch(own, n_tok, dim)
            + [dma_sems(7)] * 6 + [dma_sems(3)] * 2 + [dma_sems(2)]),
        compiler_params=pltpu.CompilerParams(dimension_semantics=('arbitrary',), vmem_limit_bytes=62 << 20,
                                             collective_id=0, has_side_effects=True),
    )(mine, grad, routes, dense, w_gate, w_up, w_down)


def layer_backward(whole, mine, rank, gate, x_own, grad_own, dense, w_gate, w_up, w_down, other=None):
    n_src, n_tok, dim = whole.shape
    n_all, ff, _ = w_gate.shape
    n_exp = rank.shape[1]
    own = n_src // CHIPS
    piece = dim // (CHIPS * CORES)
    groups = n_exp // GROUP
    kept = own * CAP
    last_layer = other is not None
    tall = weight_spec(groups, ff, dim)
    table = fixed(n_src, n_exp, n_tok)
    block = fixed(n_tok, dim)
    square = fixed(dim, dim)
    slab = fixed(dim // 8, dim)
    grad_shape = jax.ShapeDtypeStruct((n_all, ff, piece), BF16)
    part_shape = jax.ShapeDtypeStruct((dim, dim), BF16)
    slab_shape = jax.ShapeDtypeStruct((dim // 8, dim), BF16)
    extra_shapes = (slab_shape, slab_shape) if last_layer else (part_shape,)
    extra_specs = (slab, slab) if last_layer else (square,)
    scratch = [pltpu.VMEM((n_src, n_tok, dim), BF16), pltpu.VMEM((n_exp, kept, dim), BF16),
               pltpu.VMEM((n_exp, kept, dim), BF16), pltpu.VMEM((n_exp, kept, ff), BF16),
               pltpu.VMEM((n_exp, kept, ff), BF16), pltpu.VMEM((n_exp, kept, ff), BF16),
               pltpu.VMEM((CORES, GROUP * CAP, n_tok), BF16), pltpu.VMEM((CORES, GROUP * CAP, dim), BF16)]
    scratch += sums_scratch(own, n_tok, dim)
    scratch += [pltpu.VMEM((GROUP, kept, dim), BF16), pltpu.VMEM((GROUP, kept, dim), BF16),
                pltpu.VMEM((2, CORES, 3, GROUP, ff, piece), BF16),
                dma_sems(7), dma_sems(7), dma_sems(3), dma_sems(3), dma_sems(2, 3), dma_sems(2, 3), dma_sems(groups, 3)]
    if last_layer:
        scratch += [pltpu.VMEM((dim, dim), BF16), pltpu.VMEM((2, 8, dim // 8, dim), BF16), dma_sems(2, 8), dma_sems(2, 8)]
    operands = (whole, mine, rank, gate, x_own, grad_own, dense, w_gate, w_up, w_down) + ((other,) if last_layer else ())
    return pl.pallas_call(
        functools.partial(layer_kernel, last_layer),
        out_shape=(jax.ShapeDtypeStruct((n_tok, dim), BF16),) + extra_shapes + (grad_shape,) * 3,
        grid_spec=pltpu.PrefetchScalarGridSpec(
            num_scalar_prefetch=0, grid=(3 * groups,),
            in_specs=[fixed(n_src, n_tok, dim), block, table, table, block, block, square, tall, tall, tall]
            + ([square] if last_layer else []),
            out_specs=(block,) + extra_specs + (pl.BlockSpec(memory_space=pl.ANY),) * 3,
            scratch_shapes=scratch),
        compiler_params=pltpu.CompilerParams(dimension_semantics=('arbitrary',), vmem_limit_bytes=67043328,
                                             collective_id=1 + int(last_layer), has_side_effects=True),
    )(*operands)


def mix(x, weight):
    return (x.astype(F32) + jnp.dot(x, weight, preferred_element_type=F32)).astype(BF16)


def solution(mesh):
    fine = Mesh(mesh.devices.reshape(2, CHIPS, CORES), ('y', 'x', 'c'))
    tok_spec = P(ALL, None)
    exp_spec = P('y', None, None)
    layer_specs = (P(None, None), tok_spec, tok_spec, exp_spec, exp_spec, exp_spec)
    grad_specs = (P(ALL, None), P('y', ('x', 'c'), None), P('y', ('x', 'c'), None), P('y', None, ('x', 'c')))

    def local_step(tokens, dy_out, dense_w1, route_idx1, route_gate1, w_gate1, w_up1, w_down1, dense_w2, route_idx2, route_gate2, w_gate2, w_up2, w_down2):
        w_gate1, w_up1, w_gate2, w_up2 = (jnp.swapaxes(w, 1, 2) for w in (w_gate1, w_up1, w_gate2, w_up2))
        routes = jnp.concatenate([route_idx1.astype(F32).T, route_idx2.astype(F32).T, route_gate1.T, route_gate2.T], axis=0)
        u_one = mix(tokens, dense_w1)
        y_one, u_two, u_all, dy_all, rank1, gate1, rank2, gate2 = layer_forward(
            u_one, dy_out, routes, dense_w2, w_gate1, w_up1, w_down1)
        grad_mid, part_two, gg, gu, gd = layer_backward(
            dy_all, u_two, rank2, gate2, y_one, dy_out, dense_w2, w_gate2, w_up2, w_down2)
        gate_two, up_two, down_two = jnp.swapaxes(gg, 1, 2), jnp.swapaxes(gu, 1, 2), gd
        grad_tok, dense_one, dense_two, gg, gu, gd = layer_backward(
            u_all, grad_mid, rank1, gate1, tokens, grad_mid, dense_w1, w_gate1, w_up1, w_down1, part_two)
        gate_one, up_one, down_one = jnp.swapaxes(gg, 1, 2), jnp.swapaxes(gu, 1, 2), gd
        return (grad_tok, dense_one, gate_one, up_one, down_one, dense_two, gate_two, up_two, down_two)

    return jax.shard_map(local_step, mesh=fine, in_specs=(tok_spec, tok_spec) + layer_specs + layer_specs,
                         out_specs=(tok_spec,) + grad_specs + grad_specs, check_vma=False)
```

```python
import functools

import jax
import jax.numpy as jnp
from jax import lax
from jax.experimental import pallas as pl
from jax.experimental.pallas import tpu as pltpu
from jax.sharding import Mesh, PartitionSpec as P

F32 = jnp.float32
BF16 = jnp.bfloat16
CAP = 64
GROUP = 4
LANES = 256
CORES = 2
CHIPS = 2
ALL = ('x', 'c', 'y')
MESH = pl.DeviceIdType.MESH
FLIPS = ((0, 0), (0, 0), (0, 1), (0, 0), (0, 1), (1, 0), (1, 1))
ROUTE = 'yxxcccc'


def matmul(lhs, rhs, lhs_dim=1, rhs_dim=0):
    return lax.dot_general(lhs, rhs, (((lhs_dim,), (rhs_dim,)), ((), ())), preferred_element_type=F32)


def position():
    return tuple(lax.axis_index(name) for name in ALL)


def send(src, dst, sems, at, axis):
    return pltpu.make_async_remote_copy(src, dst, sems[0].at[at], sems[1].at[at],
                                        device_id={axis: 1 - lax.axis_index(axis)}, device_id_type=MESH)


def spreader(mine_ref, peer_ref, sems):
    ix, ic, iy = position()

    def copy(at):
        flip_x, flip_y = FLIPS[at]
        x = 1 - ix if flip_x else ix
        y = 1 - iy if flip_y else iy
        block = peer_ref.at[(x * CORES + ic) * 2 + y]
        return send(block if flip_x or flip_y else mine_ref, block, sems, at, ROUTE[at])

    return copy


def adder(p_ref, rs_ref, sems):
    ix, ic, iy = position()

    def copy(at):
        part = ((1 - ic) * 2 + 1 - iy, (1 - ic) * 2 + iy, ic * 2 + 1 - iy)[at]
        return send(p_ref.at[part], rs_ref.at[at], sems, at, 'ccy'[at])

    return copy


def greet(everyone):
    barrier = pltpu.get_barrier_semaphore()
    if everyone:
        others = [target(hop) for hop in range(1, 8)]
    else:
        others = [{axis: 1 - lax.axis_index(axis)} for axis in ALL]
    for other in others:
        pl.semaphore_signal(barrier, inc=1, device_id=other, device_id_type=MESH)
    pl.semaphore_wait(barrier, len(others))


def rank_of(x, c, y):
    return (x * CORES + c) * 2 + y


def target(hop):
    goal = lax.rem(rank_of(*position()) + hop, 8)
    return {'x': lax.div(goal, 4), 'c': lax.rem(lax.div(goal, 2), 2), 'y': lax.rem(goal, 2)}


def at_step(number):
    return pl.when(pl.program_id(0) == number)


def side_by_side(first, second):
    pad = jnp.zeros((LANES - first.shape[0], first.shape[1]), first.dtype)
    return jnp.concatenate([first, pad, second, pad], axis=0)


def select_rows(rank_ref, gate_ref, group, src):
    n_tok = rank_ref.shape[-1]
    slot = lax.broadcasted_iota(jnp.int32, (CAP, n_tok), 0)
    picks, gates = [], []
    for exp in range(GROUP):
        row = pl.ds(group * GROUP + exp, 1)
        hit = slot == rank_ref[src, row, :]
        picks.append(jnp.where(hit, 1.0, 0.0).astype(BF16))
        gates.append(jnp.sum(jnp.where(hit, gate_ref[src, row, :], 0.0), axis=1, keepdims=True))
    return jnp.concatenate(picks, axis=0), jnp.concatenate(gates, axis=0)


def route_table(route_ref, before_ref, src, layer, rank_ref, gate_ref, n_exp):
    _, ic, iy = position()
    n_tok = route_ref.shape[-1]
    experts = ((iy * CORES + ic) * n_exp + lax.broadcasted_iota(jnp.int32, (n_exp, n_tok), 0)).astype(F32)
    member = jnp.zeros((n_exp, n_tok), F32)
    gates = jnp.zeros((n_exp, n_tok), F32)
    for top in range(8):
        hit = experts == route_ref[src, layer * 8 + top:layer * 8 + top + 1, :]
        member = jnp.where(hit, 1.0, member)
        gates = jnp.where(hit, route_ref[src, 16 + layer * 8 + top:17 + layer * 8 + top, :], gates)
    count = matmul(member.astype(BF16), before_ref[...])
    rank_ref[src] = jnp.where(member > 0.0, count, -1.0).astype(jnp.int32)
    gate_ref[src] = gates


def forward_kernel(mine_ref, grad_ref, routes_ref, dense_ref, wg_ref, wu_ref, wd_ref,
                   y_ref, u_ref, uall_ref, dall_ref, rank1_ref, gate1_ref, rank2_ref, gate2_ref,
                   us_ref, ds_ref, route_ref, before_ref, pick_ref, row_ref, x_ref, part_ref, p_ref, rs_ref,
                   u_send, u_recv, d_send, d_recv, t_send, t_recv, rs_send, rs_recv, out_sem):
    n_exp, n_tok = rank1_ref.shape[1:]
    n_group = n_exp // GROUP
    step = pl.program_id(0)
    ix, ic, iy = position()
    me = rank_of(ix, ic, iy)
    spread_u = spreader(mine_ref, us_ref, (u_send, u_recv))
    spread_d = spreader(grad_ref, ds_ref, (d_send, d_recv))
    spread_t = spreader(routes_ref, route_ref, (t_send, t_recv))
    add_up = adder(p_ref, rs_ref, (rs_send, rs_recv))
    stores = ((us_ref, uall_ref), (ds_ref, dall_ref))

    def pass_on(copy, arrived, onward):
        copy(arrived).wait_recv()
        for at in onward:
            copy(at).start()

    @at_step(0)
    def _():
        greet(False)
        for copy in (spread_t, spread_u):
            for at in (0, 3, 1):
                copy(at).start()
        us_ref[me] = mine_ref[...]
        ds_ref[me] = grad_ref[...]
        route_ref[me] = routes_ref[...]
        p_ref[...] = jnp.zeros_like(p_ref)
        before_ref[...] = jnp.where(lax.broadcasted_iota(jnp.int32, (n_tok, n_tok), 0)
                                    < lax.broadcasted_iota(jnp.int32, (n_tok, n_tok), 1), 1.0, 0.0).astype(BF16)
        pass_on(spread_t, 0, (4, 2))
        spread_t(3).wait_recv()
        spread_t(4).wait_recv()

        @pl.loop(0, 4)
        def _(src):
            route_table(route_ref, before_ref, ix * 4 + src, 0, rank1_ref, gate1_ref, n_exp)

        pass_on(spread_u, 0, (4, 2))
        for at in (0, 3, 1):
            spread_d(at).start()
        spread_u(3).wait_recv()
        spread_u(4).wait_recv()

    @at_step(n_group // 4)
    def _():
        pass_on(spread_t, 1, (5,))
        pass_on(spread_u, 1, (5,))

    @at_step(n_group // 2)
    def _():
        pass_on(spread_t, 2, (6,))
        pass_on(spread_u, 2, (6,))
        pass_on(spread_d, 0, (4, 2))

    @at_step(n_group - 1)
    def _():
        spread_t(5).wait_recv()
        spread_t(6).wait_recv()

        @pl.loop(0, 4)
        def _(src):
            route_table(route_ref, before_ref, (1 - ix) * 4 + src, 0, rank1_ref, gate1_ref, n_exp)

        @pl.loop(0, 8)
        def _(src):
            route_table(route_ref, before_ref, src, 1, rank2_ref, gate2_ref, n_exp)

    @at_step(n_group)
    def _():
        add_up(0).start()

    @at_step(n_group + 1)
    def _():
        add_up(2).start()

    @at_step(n_group + n_group // 2)
    def _():
        pass_on(spread_d, 1, (5,))

    @at_step(2 * n_group - 1)
    def _():
        pass_on(spread_d, 2, (6,))
        spread_u(5).wait_recv()
        spread_u(6).wait_recv()
        pltpu.make_async_copy(us_ref, uall_ref, out_sem.at[0]).start()

    group = lax.rem(step, n_group)
    far = 1 - lax.div(step, n_group)
    y_now = jnp.where(far == 1, 1 - iy, iy)

    for core in range(CORES):
        src = rank_of(ix, core, y_now)
        pick, gate = select_rows(rank1_ref, gate1_ref, group, src)
        pick_ref[core] = pick
        rows = matmul(pick, us_ref[src]).astype(BF16)
        at = slice(core * CAP, (core + 1) * CAP)
        for exp in range(GROUP):
            x_ref[exp, at, :] = rows[exp * CAP:(exp + 1) * CAP]
            row_ref[exp, at, :] = jnp.broadcast_to(gate[exp * CAP:(exp + 1) * CAP], (CAP, 128))

    ff = wg_ref.shape[1]
    pre = {}
    for tick in range(GROUP + 2):
        if tick < GROUP:
            pre[tick] = matmul(x_ref[tick], side_by_side(wg_ref[tick], wu_ref[tick]), 1, 1)
        if 0 < tick <= GROUP:
            both = pre.pop(tick - 1)
            a_pre, b_pre = both[:, :ff], both[:, LANES:LANES + ff]
            pre[tick - 1, 1] = (a_pre * jax.nn.sigmoid(a_pre) * b_pre).astype(BF16)
        if tick > 1:
            exp = tick - 2
            out = matmul(pre.pop((exp, 1)), wd_ref[exp]).astype(BF16).astype(F32) * row_ref[exp][:, :1]
            high = out.astype(BF16)
            rest = out - high.astype(F32)
            mid = rest.astype(BF16)
            low = (rest - mid.astype(F32)).astype(BF16)
            at = slice(exp * CAP, (exp + 1) * CAP)
            for core in range(CORES):
                here = slice(core * CAP, (core + 1) * CAP)
                part_ref[core, 0, at, :] = high[here]
                part_ref[core, 1, at, :] = mid[here]
                part_ref[core, 2, at, :] = low[here]

    for core in range(CORES):
        pick = pick_ref[core]
        total = matmul(pick, part_ref[core, 0], 0, 0)
        total += matmul(pick, part_ref[core, 1], 0, 0) + matmul(pick, part_ref[core, 2], 0, 0)
        p_ref[core * 2 + y_now] += total

    @at_step(n_group)
    def _():
        add_up(0).wait_recv()
        p_ref[ic * 2 + 1 - iy] += rs_ref[0]

    @at_step(2 * n_group - 1)
    def _():
        for at in (3, 4, 5, 6):
            spread_d(at).wait_recv()
        pltpu.make_async_copy(ds_ref, dall_ref, out_sem.at[1]).start()
        add_up(1).start()
        add_up(1).wait_recv()
        add_up(2).wait_recv()
        y_own = (mine_ref[...].astype(F32) + (p_ref[ic * 2 + iy] + rs_ref[1] + rs_ref[2])).astype(BF16)
        y_ref[...] = y_own
        u_ref[...] = (y_own.astype(F32) + matmul(y_own, dense_ref[...])).astype(BF16)
        for copy in (spread_u, spread_d, spread_t):
            for at in range(7):
                copy(at).wait_send()
        for at in range(3):
            add_up(at).wait_send()
        for at in range(2):
            pltpu.make_async_copy(*stores[at], out_sem.at[at]).wait()


def layer_kernel(last_layer, *refs):
    refs = list(refs)
    whole_ref, mine_ref, rank_ref, gate_ref, x_own_ref, grad_own_ref, dense_ref, wg_ref, wu_ref, wd_ref = refs[:10]
    del refs[:10]
    if last_layer:
        other_ref = refs.pop(0)
        one_ref, two_ref = refs[1:3]
        del refs[1:3]
    else:
        part_ref = refs.pop(1)
    gx_out_ref, gg_ref, gu_ref, gd_ref = refs[:4]
    (peer_ref, xo_ref, do_ref, h_ref, ga_ref, gb_ref, pick_ref, gx_ref, p_ref, rs_ref, x_ref, d_ref, stage_ref,
     ag_send, ag_recv, rs_send, rs_recv, keep_sem, give_send, give_recv) = refs[4:24]
    if last_layer:
        part_ref, land_ref, land_send, land_recv = refs[24:]
    n_src, _, dim = whole_ref.shape
    own = n_src // CHIPS
    n_group = xo_ref.shape[0] // GROUP
    n_first = 2 * n_group
    n_step = 3 * n_group
    half = dim // CHIPS
    piece = half // CORES
    step = pl.program_id(0)
    ix, ic, iy = position()
    cols = pl.ds(pl.multiple_of(ix * half, half), half)
    u_ref, dy_ref = (whole_ref, peer_ref) if last_layer else (peer_ref, whole_ref)
    outs = (gg_ref, gu_ref, gd_ref)
    spread = spreader(mine_ref, peer_ref, (ag_send, ag_recv))
    add_up = adder(p_ref, rs_ref, (rs_send, rs_recv))

    def land_copy(layer, hop):
        goal = target(hop)
        rows = dim // 8
        src = (part_ref, other_ref)[layer]
        at = pl.ds(pl.multiple_of(rank_of(goal['x'], goal['c'], goal['y']) * rows, rows), rows)
        return pltpu.make_async_remote_copy(src.at[at, :], land_ref.at[layer, hop], land_send.at[layer, hop],
                                            land_recv.at[layer, hop], device_id=goal, device_id_type=MESH)

    def land_sum(layer, out_ref):
        rows = dim // 8
        at = pl.ds(pl.multiple_of(rank_of(ix, ic, iy) * rows, rows), rows)
        total = (part_ref, other_ref)[layer][at, :].astype(F32)
        for hop in range(1, 8):
            land_copy(layer, hop).wait_recv()
            total += land_ref[layer, hop].astype(F32)
        out_ref[...] = total.astype(BF16)

    def store_copies(group, moved):
        buf = lax.rem(group, 2)
        rows = pl.ds(ic * n_group * GROUP + group * GROUP, GROUP)
        for kind in range(3):
            dst = outs[kind].at[rows]
            if moved:
                yield pltpu.make_async_remote_copy(
                    stage_ref.at[buf, 1 - ic, kind], dst, give_send.at[buf, kind], give_recv.at[group, kind],
                    device_id={'c': 1 - ic}, device_id_type=MESH)
            else:
                yield pltpu.make_async_copy(stage_ref.at[buf, ic, kind], dst, keep_sem.at[buf, kind])

    def store_start(group):
        for moved in (True, False):
            for copy in store_copies(group, moved):
                copy.start()

    def store_wait(group):
        for copy in store_copies(group, True):
            copy.wait_send()
        for copy in store_copies(group, False):
            copy.wait()

    def pull(src, group, at, keep):
        pick, gate = select_rows(rank_ref, gate_ref, group, src)
        if keep:
            pick_ref[at] = pick
        x_rows = matmul(pick, u_ref[src]).astype(BF16)
        d_rows = (matmul(pick, dy_ref[src]) * gate).astype(BF16)
        for exp in range(GROUP):
            x_ref[exp, at * CAP:(at + 1) * CAP, :] = x_rows[exp * CAP:(exp + 1) * CAP]
            d_ref[exp, at * CAP:(at + 1) * CAP, :] = d_rows[exp * CAP:(exp + 1) * CAP]

    def hidden_pre(x_rows, d_rows, exp):
        ff = wg_ref.shape[1]
        both = matmul(x_rows, side_by_side(wg_ref[exp], wu_ref[exp]), 1, 1)
        return both[:, :ff], both[:, LANES:LANES + ff], matmul(d_rows, wd_ref[exp], 1, 1)

    def hidden_grads(a_pre, b_pre, back):
        sigma = jax.nn.sigmoid(a_pre)
        silu = a_pre * sigma
        grad_hidden = back.astype(BF16).astype(F32)
        grad_a = (grad_hidden * b_pre * sigma * (1.0 + a_pre * (1.0 - sigma))).astype(BF16)
        return (silu * b_pre).astype(BF16), grad_a, (grad_hidden * silu).astype(BF16)

    @at_step(0)
    def _():
        greet(last_layer)
        for at in (0, 3, 1):
            spread(at).start()
        if last_layer:
            for hop in range(1, 8):
                land_copy(1, hop).start()
        peer_ref[rank_of(ix, ic, iy)] = mine_ref[...]
        p_ref[...] = jnp.zeros_like(p_ref)
        spread(3).wait_recv()

    @at_step(n_group // 2)
    def _():
        spread(0).wait_recv()
        spread(4).start()
        spread(2).start()

    @at_step(n_group)
    def _():
        spread(4).wait_recv()

    @at_step(n_group + n_group // 2)
    def _():
        spread(1).wait_recv()
        spread(5).start()

    @at_step(n_first - 1)
    def _():
        spread(2).wait_recv()
        spread(6).start()

    @pl.when(step < n_first)
    def _():
        group = lax.rem(step, n_group)
        late = lax.div(step, n_group)
        y_now = jnp.where(late == 1, 1 - iy, iy)
        base = group * GROUP
        rows = pl.ds(pl.multiple_of(late * CORES * CAP, CORES * CAP), CORES * CAP)

        for core in range(CORES):
            pull(rank_of(ix, core, y_now), group, core, True)

        near = CORES * CAP
        pre = {}
        for tick in range(GROUP + 2):
            if tick < GROUP:
                pre[tick] = hidden_pre(x_ref[tick, :near, :], d_ref[tick, :near, :], tick)
            if 0 < tick <= GROUP:
                exp = tick - 1
                hidden, grad_a, grad_b = hidden_grads(*pre.pop(exp))
                xo_ref[base + exp, rows, :] = x_ref[exp, :near, cols]
                do_ref[base + exp, rows, :] = d_ref[exp, :near, cols]
                h_ref[base + exp, rows, :] = hidden
                ga_ref[base + exp, rows, :] = grad_a
                gb_ref[base + exp, rows, :] = grad_b
                pre[exp, 1] = None
            if tick > 1:
                exp = tick - 2
                grad_x = (matmul(ga_ref[base + exp, rows, :], wg_ref[exp]) + matmul(gb_ref[base + exp, rows, :], wu_ref[exp])).astype(BF16)
                at = slice(exp * CAP, (exp + 1) * CAP)
                for core in range(CORES):
                    gx_ref[core, at, :] = grad_x[core * CAP:(core + 1) * CAP]

        for core in range(CORES):
            p_ref[core * 2 + y_now] += matmul(pick_ref[core], gx_ref[core], 0, 0)

    @at_step(n_first)
    def _():
        add_up(0).start()
        add_up(1).start()
        spread(5).wait_recv()
        spread(6).wait_recv()
        add_up(0).wait_recv()
        p_ref[ic * 2 + 1 - iy] += rs_ref[0]
        add_up(2).start()

    @at_step(n_step - 1)
    def _():
        add_up(1).wait_recv()
        add_up(2).wait_recv()
        total = p_ref[ic * 2 + iy] + rs_ref[1] + rs_ref[2]
        grad = (grad_own_ref[...].astype(F32) + total).astype(BF16)
        part_ref[...] = matmul(x_own_ref[...], grad, 0, 0).astype(BF16)
        gx_out_ref[...] = (grad.astype(F32) + matmul(grad, dense_ref[...], 1, 1)).astype(BF16)
        if last_layer:
            for hop in range(1, 8):
                land_copy(0, hop).start()

    @pl.when(step >= n_first)
    def _():
        group = step - n_first

        @pl.when(group >= 2)
        def _():
            store_wait(group - 2)

        @pl.when(group >= 1)
        def _():
            store_start(group - 1)

        for src in range(own):
            pull((1 - ix) * own + src, group, src, False)

        buf = lax.rem(group, 2)

        pre = {}
        for tick in range(GROUP + 2):
            if tick < GROUP:
                pre[tick] = hidden_pre(x_ref[tick], d_ref[tick], tick)
            if 0 < tick <= GROUP:
                exp = tick - 1
                pre[exp, 1] = hidden_grads(*pre.pop(exp))
            if tick > 1:
                exp = tick - 2
                base = group * GROUP + exp
                hidden, grad_a, grad_b = pre.pop((exp, 1))
                x_own, x_far = xo_ref[base], x_ref[exp, :, cols]
                d_own, d_far = do_ref[base], d_ref[exp, :, cols]
                grads = (matmul(ga_ref[base], x_own, 0, 0) + matmul(grad_a, x_far, 0, 0),
                         matmul(gb_ref[base], x_own, 0, 0) + matmul(grad_b, x_far, 0, 0),
                         matmul(h_ref[base], d_own, 0, 0) + matmul(hidden, d_far, 0, 0))
                for kind in range(3):
                    for core in range(CORES):
                        stage_ref[buf, core, kind, exp] = grads[kind][:, core * piece:(core + 1) * piece].astype(BF16)

    @at_step(n_step - 1)
    def _():
        last = n_group - 1
        store_wait(last - 1)
        store_start(last)
        if last_layer:
            land_sum(1, two_ref)
            land_sum(0, one_ref)
            for layer in range(2):
                for hop in range(1, 8):
                    land_copy(layer, hop).wait_send()
        for at in range(7):
            spread(at).wait_send()
        for at in range(3):
            add_up(at).wait_send()
        store_wait(last)
        for group in range(n_group):
            for copy in store_copies(group, True):
                copy.wait_recv()


def fixed(*shape):
    return pl.BlockSpec(shape, lambda s: (0,) * len(shape), pipeline_mode=pl.Buffered(1))


def weight_spec(groups, ff, dim):
    return pl.BlockSpec((GROUP, ff, dim), lambda s: (lax.axis_index('c') * groups + lax.rem(s, groups), 0, 0))


def dma_sems(*shape):
    return pltpu.SemaphoreType.DMA(shape)


def sums_scratch(own, n_tok, dim):
    return [pltpu.VMEM((own, n_tok, dim), F32), pltpu.VMEM((3, n_tok, dim), F32)]


def layer_forward(mine, grad, routes, dense, w_gate, w_up, w_down):
    n_tok, dim = mine.shape
    n_all, ff, _ = w_gate.shape
    n_exp = n_all // CORES
    n_src = 8
    own = n_src // CHIPS
    groups = n_exp // GROUP
    tall = weight_spec(groups, ff, dim)
    table = fixed(n_src, n_exp, n_tok)
    block = jax.ShapeDtypeStruct((n_tok, dim), BF16)
    every = jax.ShapeDtypeStruct((n_src, n_tok, dim), BF16)
    ranks = jax.ShapeDtypeStruct((n_src, n_exp, n_tok), jnp.int32)
    gates = jax.ShapeDtypeStruct((n_src, n_exp, n_tok), F32)
    anywhere = pl.BlockSpec(memory_space=pl.ANY)
    rows = CORES * CAP
    return pl.pallas_call(
        forward_kernel,
        out_shape=(block, block, every, every, ranks, gates, ranks, gates),
        grid_spec=pltpu.PrefetchScalarGridSpec(
            num_scalar_prefetch=0, grid=(2 * groups,),
            in_specs=[fixed(n_tok, dim), fixed(n_tok, dim), fixed(*routes.shape), fixed(dim, dim), tall, tall, tall],
            out_specs=(fixed(n_tok, dim), fixed(n_tok, dim), anywhere, anywhere, table, table, table, table),
            scratch_shapes=[pltpu.VMEM((n_src, n_tok, dim), BF16), pltpu.VMEM((n_src, n_tok, dim), BF16),
                            pltpu.VMEM((n_src,) + routes.shape, F32), pltpu.VMEM((n_tok, n_tok), BF16),
                            pltpu.VMEM((CORES, GROUP * CAP, n_tok), BF16), pltpu.VMEM((GROUP, rows, 128), F32),
                            pltpu.VMEM((GROUP, rows, dim), BF16), pltpu.VMEM((CORES, 3, GROUP * CAP, dim), BF16)]
            + sums_scratch(own, n_tok, dim)
            + [dma_sems(7)] * 6 + [dma_sems(3)] * 2 + [dma_sems(2)]),
        compiler_params=pltpu.CompilerParams(dimension_semantics=('arbitrary',), vmem_limit_bytes=62 << 20,
                                             collective_id=0, has_side_effects=True),
    )(mine, grad, routes, dense, w_gate, w_up, w_down)


def layer_backward(whole, mine, rank, gate, x_own, grad_own, dense, w_gate, w_up, w_down, other=None):
    n_src, n_tok, dim = whole.shape
    n_all, ff, _ = w_gate.shape
    n_exp = rank.shape[1]
    own = n_src // CHIPS
    piece = dim // (CHIPS * CORES)
    groups = n_exp // GROUP
    kept = own * CAP
    last_layer = other is not None
    tall = weight_spec(groups, ff, dim)
    table = fixed(n_src, n_exp, n_tok)
    block = fixed(n_tok, dim)
    square = fixed(dim, dim)
    slab = fixed(dim // 8, dim)
    grad_shape = jax.ShapeDtypeStruct((n_all, ff, piece), BF16)
    part_shape = jax.ShapeDtypeStruct((dim, dim), BF16)
    slab_shape = jax.ShapeDtypeStruct((dim // 8, dim), BF16)
    extra_shapes = (slab_shape, slab_shape) if last_layer else (part_shape,)
    extra_specs = (slab, slab) if last_layer else (square,)
    half = dim // CHIPS
    scratch = [pltpu.VMEM((n_src, n_tok, dim), BF16), pltpu.VMEM((n_exp, kept, half), BF16),
               pltpu.VMEM((n_exp, kept, half), BF16), pltpu.VMEM((n_exp, kept, ff), BF16),
               pltpu.VMEM((n_exp, kept, ff), BF16), pltpu.VMEM((n_exp, kept, ff), BF16),
               pltpu.VMEM((CORES, GROUP * CAP, n_tok), BF16), pltpu.VMEM((CORES, GROUP * CAP, dim), BF16)]
    scratch += sums_scratch(own, n_tok, dim)
    scratch += [pltpu.VMEM((GROUP, kept, dim), BF16), pltpu.VMEM((GROUP, kept, dim), BF16),
                pltpu.VMEM((2, CORES, 3, GROUP, ff, piece), BF16),
                dma_sems(7), dma_sems(7), dma_sems(3), dma_sems(3), dma_sems(2, 3), dma_sems(2, 3), dma_sems(groups, 3)]
    if last_layer:
        scratch += [pltpu.VMEM((dim, dim), BF16), pltpu.VMEM((2, 8, dim // 8, dim), BF16), dma_sems(2, 8), dma_sems(2, 8)]
    operands = (whole, mine, rank, gate, x_own, grad_own, dense, w_gate, w_up, w_down) + ((other,) if last_layer else ())
    return pl.pallas_call(
        functools.partial(layer_kernel, last_layer),
        out_shape=(jax.ShapeDtypeStruct((n_tok, dim), BF16),) + extra_shapes + (grad_shape,) * 3,
        grid_spec=pltpu.PrefetchScalarGridSpec(
            num_scalar_prefetch=0, grid=(3 * groups,),
            in_specs=[fixed(n_src, n_tok, dim), block, table, table, block, block, square, tall, tall, tall]
            + ([square] if last_layer else []),
            out_specs=(block,) + extra_specs + (pl.BlockSpec(memory_space=pl.ANY),) * 3,
            scratch_shapes=scratch),
        compiler_params=pltpu.CompilerParams(dimension_semantics=('arbitrary',), vmem_limit_bytes=67043328,
                                             collective_id=1 + int(last_layer), has_side_effects=True),
    )(*operands)


def mix(x, weight):
    return (x.astype(F32) + jnp.dot(x, weight, preferred_element_type=F32)).astype(BF16)


def solution(mesh):
    fine = Mesh(mesh.devices.reshape(2, CHIPS, CORES), ('y', 'x', 'c'))
    tok_spec = P(ALL, None)
    exp_spec = P('y', None, None)
    layer_specs = (P(None, None), tok_spec, tok_spec, exp_spec, exp_spec, exp_spec)
    grad_specs = (P(ALL, None), P('y', ('x', 'c'), None), P('y', ('x', 'c'), None), P('y', None, ('x', 'c')))

    def local_step(tokens, dy_out, dense_w1, route_idx1, route_gate1, w_gate1, w_up1, w_down1, dense_w2, route_idx2, route_gate2, w_gate2, w_up2, w_down2):
        w_gate1, w_up1, w_gate2, w_up2 = (jnp.swapaxes(w, 1, 2) for w in (w_gate1, w_up1, w_gate2, w_up2))
        routes = jnp.concatenate([route_idx1.astype(F32).T, route_idx2.astype(F32).T, route_gate1.T, route_gate2.T], axis=0)
        u_one = mix(tokens, dense_w1)
        y_one, u_two, u_all, dy_all, rank1, gate1, rank2, gate2 = layer_forward(
            u_one, dy_out, routes, dense_w2, w_gate1, w_up1, w_down1)
        grad_mid, part_two, gg, gu, gd = layer_backward(
            dy_all, u_two, rank2, gate2, y_one, dy_out, dense_w2, w_gate2, w_up2, w_down2)
        gate_two, up_two, down_two = jnp.swapaxes(gg, 1, 2), jnp.swapaxes(gu, 1, 2), gd
        grad_tok, dense_one, dense_two, gg, gu, gd = layer_backward(
            u_all, grad_mid, rank1, gate1, tokens, grad_mid, dense_w1, w_gate1, w_up1, w_down1, part_two)
        gate_one, up_one, down_one = jnp.swapaxes(gg, 1, 2), jnp.swapaxes(gu, 1, 2), gd
        return (grad_tok, dense_one, gate_one, up_one, down_one, dense_two, gate_two, up_two, down_two)

    return jax.shard_map(local_step, mesh=fine, in_specs=(tok_spec, tok_spec) + layer_specs + layer_specs,
                         out_specs=(tok_spec,) + grad_specs + grad_specs, check_vma=False)
```

```python
import functools

import jax
import jax.numpy as jnp
from jax import lax
from jax.experimental import pallas as pl
from jax.experimental.pallas import tpu as pltpu
from jax.sharding import Mesh, PartitionSpec as P

F32 = jnp.float32
BF16 = jnp.bfloat16
CAP = 64
GROUP = 4
LANES = 256
CORES = 2
CHIPS = 2
ALL = ('x', 'c', 'y')
MESH = pl.DeviceIdType.MESH
FLIPS = ((0, 0), (0, 0), (0, 1), (0, 0), (0, 1), (1, 0), (1, 1))
ROUTE = 'yxxcccc'


def matmul(lhs, rhs, lhs_dim=1, rhs_dim=0):
    return lax.dot_general(lhs, rhs, (((lhs_dim,), (rhs_dim,)), ((), ())), preferred_element_type=F32)


def position():
    return tuple(lax.axis_index(name) for name in ALL)


def send(src, dst, sems, at, axis):
    return pltpu.make_async_remote_copy(src, dst, sems[0].at[at], sems[1].at[at],
                                        device_id={axis: 1 - lax.axis_index(axis)}, device_id_type=MESH)


def spreader(mine_ref, peer_ref, sems):
    ix, ic, iy = position()

    def copy(at):
        flip_x, flip_y = FLIPS[at]
        x = 1 - ix if flip_x else ix
        y = 1 - iy if flip_y else iy
        block = peer_ref.at[(x * CORES + ic) * 2 + y]
        return send(block if flip_x or flip_y else mine_ref, block, sems, at, ROUTE[at])

    return copy


def adder(p_ref, rs_ref, sems):
    ix, ic, iy = position()

    def copy(at):
        part = ((1 - ic) * 2 + 1 - iy, (1 - ic) * 2 + iy, ic * 2 + 1 - iy)[at]
        return send(p_ref.at[part], rs_ref.at[at], sems, at, 'ccy'[at])

    return copy


def greet(everyone):
    barrier = pltpu.get_barrier_semaphore()
    if everyone:
        others = [target(hop) for hop in range(1, 8)]
    else:
        others = [{axis: 1 - lax.axis_index(axis)} for axis in ALL]
    for other in others:
        pl.semaphore_signal(barrier, inc=1, device_id=other, device_id_type=MESH)
    pl.semaphore_wait(barrier, len(others))


def rank_of(x, c, y):
    return (x * CORES + c) * 2 + y


def target(hop):
    goal = lax.rem(rank_of(*position()) + hop, 8)
    return {'x': lax.div(goal, 4), 'c': lax.rem(lax.div(goal, 2), 2), 'y': lax.rem(goal, 2)}


def at_step(number):
    return pl.when(pl.program_id(0) == number)


def side_by_side(first, second):
    pad = jnp.zeros((LANES - first.shape[0], first.shape[1]), first.dtype)
    return jnp.concatenate([first, pad, second, pad], axis=0)


def select_rows(rank_ref, gate_ref, group, src):
    n_tok = rank_ref.shape[-1]
    slot = lax.broadcasted_iota(jnp.int32, (CAP, n_tok), 0)
    picks, gates = [], []
    for exp in range(GROUP):
        row = pl.ds(group * GROUP + exp, 1)
        hit = slot == rank_ref[src, row, :]
        picks.append(jnp.where(hit, 1.0, 0.0).astype(BF16))
        gates.append(jnp.sum(jnp.where(hit, gate_ref[src, row, :], 0.0), axis=1, keepdims=True))
    return jnp.concatenate(picks, axis=0), jnp.concatenate(gates, axis=0)


def route_table(route_ref, before_ref, src, layer, rank_ref, gate_ref, n_exp):
    _, ic, iy = position()
    n_tok = route_ref.shape[-1]
    experts = ((iy * CORES + ic) * n_exp + lax.broadcasted_iota(jnp.int32, (n_exp, n_tok), 0)).astype(F32)
    member = jnp.zeros((n_exp, n_tok), F32)
    gates = jnp.zeros((n_exp, n_tok), F32)
    for top in range(8):
        hit = experts == route_ref[src, layer * 8 + top:layer * 8 + top + 1, :]
        member = jnp.where(hit, 1.0, member)
        gates = jnp.where(hit, route_ref[src, 16 + layer * 8 + top:17 + layer * 8 + top, :], gates)
    count = matmul(member.astype(BF16), before_ref[...])
    rank_ref[src] = jnp.where(member > 0.0, count, -1.0).astype(jnp.int32)
    gate_ref[src] = gates


def forward_kernel(tok_ref, grad_ref, idx1_ref, idx2_ref, top1_ref, top2_ref, mix_ref, dense_ref, wg_ref, wu_ref, wd_ref,
                   y_ref, u_ref, uall_ref, dall_ref, rank1_ref, gate1_ref, rank2_ref, gate2_ref,
                   raw_ref, us_ref, ds_ref, routes_ref, route_ref, before_ref, pick_ref, row_ref, x_ref, part_ref, p_ref, rs_ref,
                   u_send, u_recv, d_send, d_recv, t_send, t_recv, rs_send, rs_recv, out_sem):
    n_exp, n_tok = rank1_ref.shape[1:]
    n_group = n_exp // GROUP
    step = pl.program_id(0)
    ix, ic, iy = position()
    me = rank_of(ix, ic, iy)
    spread_u = spreader(tok_ref, raw_ref, (u_send, u_recv))
    spread_d = spreader(grad_ref, ds_ref, (d_send, d_recv))
    spread_t = spreader(routes_ref, route_ref, (t_send, t_recv))
    add_up = adder(p_ref, rs_ref, (rs_send, rs_recv))
    stores = ((us_ref, uall_ref), (ds_ref, dall_ref))

    def mixed(x):
        return (x.astype(F32) + matmul(x, mix_ref[...])).astype(BF16)

    def pass_on(copy, arrived, onward):
        copy(arrived).wait_recv()
        for at in onward:
            copy(at).start()

    @at_step(0)
    def _():
        for at, part_in in enumerate((idx1_ref, idx2_ref, top1_ref, top2_ref)):
            routes_ref[at * 8:at * 8 + 8, :] = part_in[...].astype(F32)
        greet(False)
        for copy in (spread_t, spread_u):
            for at in (0, 3, 1):
                copy(at).start()
        us_ref[me] = mixed(tok_ref[...])
        ds_ref[me] = grad_ref[...]
        route_ref[me] = routes_ref[...]
        p_ref[...] = jnp.zeros_like(p_ref)
        before_ref[...] = jnp.where(lax.broadcasted_iota(jnp.int32, (n_tok, n_tok), 0)
                                    < lax.broadcasted_iota(jnp.int32, (n_tok, n_tok), 1), 1.0, 0.0).astype(BF16)
        pass_on(spread_t, 0, (4, 2))
        spread_u(3).wait_recv()
        us_ref[rank_of(ix, 1 - ic, iy)] = mixed(raw_ref[rank_of(ix, 1 - ic, iy)])
        spread_t(3).wait_recv()
        spread_t(4).wait_recv()

        @pl.loop(0, 4)
        def _(src):
            route_table(route_ref, before_ref, ix * 4 + src, 0, rank1_ref, gate1_ref, n_exp)

        pass_on(spread_u, 0, (4, 2))
        for at in (0, 3, 1):
            spread_d(at).start()
        us_ref[rank_of(ix, ic, 1 - iy)] = mixed(raw_ref[rank_of(ix, ic, 1 - iy)])
        spread_u(4).wait_recv()
        us_ref[rank_of(ix, 1 - ic, 1 - iy)] = mixed(raw_ref[rank_of(ix, 1 - ic, 1 - iy)])

    @at_step(n_group // 4)
    def _():
        pass_on(spread_t, 1, (5,))
        pass_on(spread_u, 1, (5,))

    @at_step(n_group // 2)
    def _():
        pass_on(spread_t, 2, (6,))
        pass_on(spread_u, 2, (6,))
        pass_on(spread_d, 0, (4, 2))

    @at_step(n_group - 1)
    def _():
        for copy in (spread_t, spread_u):
            copy(5).wait_recv()
            copy(6).wait_recv()

        @pl.loop(0, 4)
        def _(src):
            us_ref[(1 - ix) * 4 + src] = mixed(raw_ref[(1 - ix) * 4 + src])
            route_table(route_ref, before_ref, (1 - ix) * 4 + src, 0, rank1_ref, gate1_ref, n_exp)

        @pl.loop(0, 8)
        def _(src):
            route_table(route_ref, before_ref, src, 1, rank2_ref, gate2_ref, n_exp)

    @at_step(n_group)
    def _():
        add_up(0).start()
        pltpu.make_async_copy(us_ref, uall_ref, out_sem.at[0]).start()

    @at_step(n_group + 1)
    def _():
        add_up(2).start()

    @at_step(n_group + n_group // 2)
    def _():
        pass_on(spread_d, 1, (5,))

    @at_step(2 * n_group - 2)
    def _():
        pass_on(spread_d, 2, (6,))

    @at_step(2 * n_group - 1)
    def _():
        for at in (3, 4, 5, 6):
            spread_d(at).wait_recv()
        pltpu.make_async_copy(ds_ref, dall_ref, out_sem.at[1]).start()

    group = lax.rem(step, n_group)
    far = 1 - lax.div(step, n_group)
    y_now = jnp.where(far == 1, 1 - iy, iy)

    for core in range(CORES):
        src = rank_of(ix, core, y_now)
        pick, gate = select_rows(rank1_ref, gate1_ref, group, src)
        pick_ref[core] = pick
        rows = matmul(pick, us_ref[src]).astype(BF16)
        at = slice(core * CAP, (core + 1) * CAP)
        for exp in range(GROUP):
            x_ref[exp, at, :] = rows[exp * CAP:(exp + 1) * CAP]
            row_ref[exp, at, :] = jnp.broadcast_to(gate[exp * CAP:(exp + 1) * CAP], (CAP, 128))

    ff = wg_ref.shape[1]
    pre = {}
    for tick in range(GROUP + 2):
        if tick < GROUP:
            pre[tick] = matmul(x_ref[tick], side_by_side(wg_ref[tick], wu_ref[tick]), 1, 1)
        if 0 < tick <= GROUP:
            both = pre.pop(tick - 1)
            a_pre, b_pre = both[:, :ff], both[:, LANES:LANES + ff]
            pre[tick - 1, 1] = (a_pre * jax.nn.sigmoid(a_pre) * b_pre).astype(BF16)
        if tick > 1:
            exp = tick - 2
            out = matmul(pre.pop((exp, 1)), wd_ref[exp]).astype(BF16).astype(F32) * row_ref[exp][:, :1]
            high = out.astype(BF16)
            rest = out - high.astype(F32)
            mid = rest.astype(BF16)
            low = (rest - mid.astype(F32)).astype(BF16)
            at = slice(exp * CAP, (exp + 1) * CAP)
            for core in range(CORES):
                here = slice(core * CAP, (core + 1) * CAP)
                part_ref[core, 0, at, :] = high[here]
                part_ref[core, 1, at, :] = mid[here]
                part_ref[core, 2, at, :] = low[here]

    for core in range(CORES):
        pick = pick_ref[core]
        total = matmul(pick, part_ref[core, 0], 0, 0)
        total += matmul(pick, part_ref[core, 1], 0, 0) + matmul(pick, part_ref[core, 2], 0, 0)
        p_ref[core * 2 + y_now] += total

    @at_step(n_group)
    def _():
        add_up(0).wait_recv()
        p_ref[ic * 2 + 1 - iy] += rs_ref[0]

    @at_step(2 * n_group - 1)
    def _():
        add_up(1).start()
        add_up(1).wait_recv()
        add_up(2).wait_recv()
        y_own = (us_ref[me].astype(F32) + (p_ref[ic * 2 + iy] + rs_ref[1] + rs_ref[2])).astype(BF16)
        y_ref[...] = y_own
        u_ref[...] = (y_own.astype(F32) + matmul(y_own, dense_ref[...])).astype(BF16)
        for copy in (spread_u, spread_d, spread_t):
            for at in range(7):
                copy(at).wait_send()
        for at in range(3):
            add_up(at).wait_send()
        for at in range(2):
            pltpu.make_async_copy(*stores[at], out_sem.at[at]).wait()


def layer_kernel(last_layer, *refs):
    refs = list(refs)
    whole_ref, mine_ref, rank_ref, gate_ref, x_own_ref, grad_own_ref, dense_ref, wg_ref, wu_ref, wd_ref = refs[:10]
    del refs[:10]
    if last_layer:
        other_ref = refs.pop(0)
        one_ref, two_ref = refs[1:3]
        del refs[1:3]
    else:
        part_ref = refs.pop(1)
    gx_out_ref, gg_ref, gu_ref, gd_ref = refs[:4]
    (peer_ref, xo_ref, do_ref, h_ref, ga_ref, gb_ref, pick_ref, gx_ref, p_ref, rs_ref, x_ref, d_ref, stage_ref,
     ag_send, ag_recv, rs_send, rs_recv, keep_sem, give_send, give_recv) = refs[4:24]
    if last_layer:
        part_ref, land_ref, land_send, land_recv = refs[24:]
    n_src, _, dim = whole_ref.shape
    own = n_src // CHIPS
    n_group = xo_ref.shape[0] // GROUP
    n_first = 2 * n_group
    n_step = 3 * n_group
    half = dim // CHIPS
    piece = half // CORES
    step = pl.program_id(0)
    ix, ic, iy = position()
    cols = pl.ds(pl.multiple_of(ix * half, half), half)
    u_ref, dy_ref = (whole_ref, peer_ref) if last_layer else (peer_ref, whole_ref)
    outs = (gg_ref, gu_ref, gd_ref)
    spread = spreader(mine_ref, peer_ref, (ag_send, ag_recv))
    add_up = adder(p_ref, rs_ref, (rs_send, rs_recv))

    def land_copy(layer, hop):
        goal = target(hop)
        rows = dim // 8
        src = (part_ref, other_ref)[layer]
        at = pl.ds(pl.multiple_of(rank_of(goal['x'], goal['c'], goal['y']) * rows, rows), rows)
        return pltpu.make_async_remote_copy(src.at[at, :], land_ref.at[layer, hop], land_send.at[layer, hop],
                                            land_recv.at[layer, hop], device_id=goal, device_id_type=MESH)

    def land_sum(layer, out_ref):
        rows = dim // 8
        at = pl.ds(pl.multiple_of(rank_of(ix, ic, iy) * rows, rows), rows)
        total = (part_ref, other_ref)[layer][at, :].astype(F32)
        for hop in range(1, 8):
            land_copy(layer, hop).wait_recv()
            total += land_ref[layer, hop].astype(F32)
        out_ref[...] = total.astype(BF16)

    def store_copies(group, moved):
        buf = lax.rem(group, 2)
        rows = pl.ds(ic * n_group * GROUP + group * GROUP, GROUP)
        for kind in range(3):
            dst = outs[kind].at[rows]
            if moved:
                yield pltpu.make_async_remote_copy(
                    stage_ref.at[buf, 1 - ic, kind], dst, give_send.at[buf, kind], give_recv.at[group, kind],
                    device_id={'c': 1 - ic}, device_id_type=MESH)
            else:
                yield pltpu.make_async_copy(stage_ref.at[buf, ic, kind], dst, keep_sem.at[buf, kind])

    def store_start(group):
        for moved in (True, False):
            for copy in store_copies(group, moved):
                copy.start()

    def store_wait(group):
        for copy in store_copies(group, True):
            copy.wait_send()
        for copy in store_copies(group, False):
            copy.wait()

    def pull(src, group, at, keep):
        pick, gate = select_rows(rank_ref, gate_ref, group, src)
        if keep:
            pick_ref[at] = pick
        x_rows = matmul(pick, u_ref[src]).astype(BF16)
        d_rows = (matmul(pick, dy_ref[src]) * gate).astype(BF16)
        for exp in range(GROUP):
            x_ref[exp, at * CAP:(at + 1) * CAP, :] = x_rows[exp * CAP:(exp + 1) * CAP]
            d_ref[exp, at * CAP:(at + 1) * CAP, :] = d_rows[exp * CAP:(exp + 1) * CAP]

    def hidden_pre(x_rows, d_rows, exp):
        ff = wg_ref.shape[1]
        both = matmul(x_rows, side_by_side(wg_ref[exp], wu_ref[exp]), 1, 1)
        return both[:, :ff], both[:, LANES:LANES + ff], matmul(d_rows, wd_ref[exp], 1, 1)

    def hidden_grads(a_pre, b_pre, back):
        sigma = jax.nn.sigmoid(a_pre)
        silu = a_pre * sigma
        grad_hidden = back.astype(BF16).astype(F32)
        grad_a = (grad_hidden * b_pre * sigma * (1.0 + a_pre * (1.0 - sigma))).astype(BF16)
        return (silu * b_pre).astype(BF16), grad_a, (grad_hidden * silu).astype(BF16)

    @at_step(0)
    def _():
        greet(last_layer)
        for at in (0, 3, 1):
            spread(at).start()
        if last_layer:
            for hop in range(1, 8):
                land_copy(1, hop).start()
        peer_ref[rank_of(ix, ic, iy)] = mine_ref[...]
        p_ref[...] = jnp.zeros_like(p_ref)
        spread(3).wait_recv()

    @at_step(n_group // 2)
    def _():
        spread(0).wait_recv()
        spread(4).start()
        spread(2).start()

    @at_step(n_group)
    def _():
        spread(4).wait_recv()

    @at_step(n_group + n_group // 2)
    def _():
        spread(1).wait_recv()
        spread(5).start()

    @at_step(n_first - 1)
    def _():
        spread(2).wait_recv()
        spread(6).start()

    @pl.when(step < n_first)
    def _():
        group = lax.rem(step, n_group)
        late = lax.div(step, n_group)
        y_now = jnp.where(late == 1, 1 - iy, iy)
        base = group * GROUP
        rows = pl.ds(pl.multiple_of(late * CORES * CAP, CORES * CAP), CORES * CAP)

        for core in range(CORES):
            pull(rank_of(ix, core, y_now), group, core, True)

        near = CORES * CAP
        pre = {}
        for tick in range(GROUP + 2):
            if tick < GROUP:
                pre[tick] = hidden_pre(x_ref[tick, :near, :], d_ref[tick, :near, :], tick)
            if 0 < tick <= GROUP:
                exp = tick - 1
                hidden, grad_a, grad_b = hidden_grads(*pre.pop(exp))
                xo_ref[base + exp, rows, :] = x_ref[exp, :near, cols]
                do_ref[base + exp, rows, :] = d_ref[exp, :near, cols]
                h_ref[base + exp, rows, :] = hidden
                ga_ref[base + exp, rows, :] = grad_a
                gb_ref[base + exp, rows, :] = grad_b
                pre[exp, 1] = None
            if tick > 1:
                exp = tick - 2
                grad_x = (matmul(ga_ref[base + exp, rows, :], wg_ref[exp]) + matmul(gb_ref[base + exp, rows, :], wu_ref[exp])).astype(BF16)
                at = slice(exp * CAP, (exp + 1) * CAP)
                for core in range(CORES):
                    gx_ref[core, at, :] = grad_x[core * CAP:(core + 1) * CAP]

        for core in range(CORES):
            p_ref[core * 2 + y_now] += matmul(pick_ref[core], gx_ref[core], 0, 0)

    @at_step(n_first)
    def _():
        add_up(0).start()
        add_up(1).start()
        spread(5).wait_recv()
        spread(6).wait_recv()

    @at_step(n_first + 1)
    def _():
        add_up(2).start()

    @at_step(n_step - 1)
    def _():
        add_up(1).wait_recv()
        add_up(2).wait_recv()
        total = p_ref[ic * 2 + iy] + rs_ref[1] + rs_ref[2]
        grad = (grad_own_ref[...].astype(F32) + total).astype(BF16)
        part_ref[...] = matmul(x_own_ref[...], grad, 0, 0).astype(BF16)
        gx_out_ref[...] = (grad.astype(F32) + matmul(grad, dense_ref[...], 1, 1)).astype(BF16)
        if last_layer:
            for hop in range(1, 8):
                land_copy(0, hop).start()

    @pl.when(step >= n_first)
    def _():
        group = step - n_first

        @pl.when(group >= 2)
        def _():
            store_wait(group - 2)

        @pl.when(group >= 1)
        def _():
            store_start(group - 1)

        for src in range(own):
            pull((1 - ix) * own + src, group, src, False)

        buf = lax.rem(group, 2)

        pre = {}
        for tick in range(GROUP + 2):
            if tick < GROUP:
                pre[tick] = hidden_pre(x_ref[tick], d_ref[tick], tick)
            if 0 < tick <= GROUP:
                exp = tick - 1
                pre[exp, 1] = hidden_grads(*pre.pop(exp))
            if tick > 1:
                exp = tick - 2
                base = group * GROUP + exp
                hidden, grad_a, grad_b = pre.pop((exp, 1))
                x_own, x_far = xo_ref[base], x_ref[exp, :, cols]
                d_own, d_far = do_ref[base], d_ref[exp, :, cols]
                grads = (matmul(ga_ref[base], x_own, 0, 0) + matmul(grad_a, x_far, 0, 0),
                         matmul(gb_ref[base], x_own, 0, 0) + matmul(grad_b, x_far, 0, 0),
                         matmul(h_ref[base], d_own, 0, 0) + matmul(hidden, d_far, 0, 0))
                for kind in range(3):
                    for core in range(CORES):
                        stage_ref[buf, core, kind, exp] = grads[kind][:, core * piece:(core + 1) * piece].astype(BF16)

    @at_step(n_first)
    def _():
        add_up(0).wait_recv()
        p_ref[ic * 2 + 1 - iy] += rs_ref[0]

    @at_step(n_step - 1)
    def _():
        last = n_group - 1
        store_wait(last - 1)
        store_start(last)
        if last_layer:
            land_sum(1, two_ref)
            land_sum(0, one_ref)
            for layer in range(2):
                for hop in range(1, 8):
                    land_copy(layer, hop).wait_send()
        for at in range(7):
            spread(at).wait_send()
        for at in range(3):
            add_up(at).wait_send()
        store_wait(last)
        for group in range(n_group):
            for copy in store_copies(group, True):
                copy.wait_recv()


def fixed(*shape):
    return pl.BlockSpec(shape, lambda s: (0,) * len(shape), pipeline_mode=pl.Buffered(1))


def weight_spec(groups, ff, dim):
    return pl.BlockSpec((GROUP, ff, dim), lambda s: (lax.axis_index('c') * groups + lax.rem(s, groups), 0, 0))


def dma_sems(*shape):
    return pltpu.SemaphoreType.DMA(shape)


def sums_scratch(own, n_tok, dim):
    return [pltpu.VMEM((own, n_tok, dim), F32), pltpu.VMEM((3, n_tok, dim), F32)]


def layer_forward(tokens, grad, idx1, idx2, top1, top2, dense1, dense2, w_gate, w_up, w_down):
    n_tok, dim = tokens.shape
    top = idx1.shape[0]
    n_all, ff, _ = w_gate.shape
    n_exp = n_all // CORES
    n_src = 8
    own = n_src // CHIPS
    groups = n_exp // GROUP
    tall = weight_spec(groups, ff, dim)
    table = fixed(n_src, n_exp, n_tok)
    block = jax.ShapeDtypeStruct((n_tok, dim), BF16)
    every = jax.ShapeDtypeStruct((n_src, n_tok, dim), BF16)
    ranks = jax.ShapeDtypeStruct((n_src, n_exp, n_tok), jnp.int32)
    gates = jax.ShapeDtypeStruct((n_src, n_exp, n_tok), F32)
    anywhere = pl.BlockSpec(memory_space=pl.ANY)
    rows = CORES * CAP
    return pl.pallas_call(
        forward_kernel,
        out_shape=(block, block, every, every, ranks, gates, ranks, gates),
        grid_spec=pltpu.PrefetchScalarGridSpec(
            num_scalar_prefetch=0, grid=(2 * groups,),
            in_specs=[fixed(n_tok, dim)] * 2 + [fixed(top, n_tok)] * 4 + [fixed(dim, dim)] * 2 + [tall] * 3,
            out_specs=(fixed(n_tok, dim), fixed(n_tok, dim), anywhere, anywhere, table, table, table, table),
            scratch_shapes=[pltpu.VMEM((n_src, n_tok, dim), BF16)] * 3
            + [pltpu.VMEM((4 * top, n_tok), F32), pltpu.VMEM((n_src, 4 * top, n_tok), F32), pltpu.VMEM((n_tok, n_tok), BF16),
                            pltpu.VMEM((CORES, GROUP * CAP, n_tok), BF16), pltpu.VMEM((GROUP, rows, 128), F32),
                            pltpu.VMEM((GROUP, rows, dim), BF16), pltpu.VMEM((CORES, 3, GROUP * CAP, dim), BF16)]
            + sums_scratch(own, n_tok, dim)
            + [dma_sems(7)] * 6 + [dma_sems(3)] * 2 + [dma_sems(2)]),
        compiler_params=pltpu.CompilerParams(dimension_semantics=('arbitrary',), vmem_limit_bytes=62 << 20,
                                             collective_id=0, has_side_effects=True),
    )(tokens, grad, idx1, idx2, top1, top2, dense1, dense2, w_gate, w_up, w_down)


def layer_backward(whole, mine, rank, gate, x_own, grad_own, dense, w_gate, w_up, w_down, other=None):
    n_src, n_tok, dim = whole.shape
    n_all, ff, _ = w_gate.shape
    n_exp = rank.shape[1]
    own = n_src // CHIPS
    piece = dim // (CHIPS * CORES)
    groups = n_exp // GROUP
    kept = own * CAP
    last_layer = other is not None
    tall = weight_spec(groups, ff, dim)
    table = fixed(n_src, n_exp, n_tok)
    block = fixed(n_tok, dim)
    square = fixed(dim, dim)
    slab = fixed(dim // 8, dim)
    grad_shape = jax.ShapeDtypeStruct((n_all, ff, piece), BF16)
    part_shape = jax.ShapeDtypeStruct((dim, dim), BF16)
    slab_shape = jax.ShapeDtypeStruct((dim // 8, dim), BF16)
    extra_shapes = (slab_shape, slab_shape) if last_layer else (part_shape,)
    extra_specs = (slab, slab) if last_layer else (square,)
    half = dim // CHIPS
    scratch = [pltpu.VMEM((n_src, n_tok, dim), BF16), pltpu.VMEM((n_exp, kept, half), BF16),
               pltpu.VMEM((n_exp, kept, half), BF16), pltpu.VMEM((n_exp, kept, ff), BF16),
               pltpu.VMEM((n_exp, kept, ff), BF16), pltpu.VMEM((n_exp, kept, ff), BF16),
               pltpu.VMEM((CORES, GROUP * CAP, n_tok), BF16), pltpu.VMEM((CORES, GROUP * CAP, dim), BF16)]
    scratch += sums_scratch(own, n_tok, dim)
    scratch += [pltpu.VMEM((GROUP, kept, dim), BF16), pltpu.VMEM((GROUP, kept, dim), BF16),
                pltpu.VMEM((2, CORES, 3, GROUP, ff, piece), BF16),
                dma_sems(7), dma_sems(7), dma_sems(3), dma_sems(3), dma_sems(2, 3), dma_sems(2, 3), dma_sems(groups, 3)]
    if last_layer:
        scratch += [pltpu.VMEM((dim, dim), BF16), pltpu.VMEM((2, 8, dim // 8, dim), BF16), dma_sems(2, 8), dma_sems(2, 8)]
    operands = (whole, mine, rank, gate, x_own, grad_own, dense, w_gate, w_up, w_down) + ((other,) if last_layer else ())
    return pl.pallas_call(
        functools.partial(layer_kernel, last_layer),
        out_shape=(jax.ShapeDtypeStruct((n_tok, dim), BF16),) + extra_shapes + (grad_shape,) * 3,
        grid_spec=pltpu.PrefetchScalarGridSpec(
            num_scalar_prefetch=0, grid=(3 * groups,),
            in_specs=[fixed(n_src, n_tok, dim), block, table, table, block, block, square, tall, tall, tall]
            + ([square] if last_layer else []),
            out_specs=(block,) + extra_specs + (pl.BlockSpec(memory_space=pl.ANY),) * 3,
            scratch_shapes=scratch),
        compiler_params=pltpu.CompilerParams(dimension_semantics=('arbitrary',), vmem_limit_bytes=67043328,
                                             collective_id=1 + int(last_layer), has_side_effects=True),
    )(*operands)


def settle_kernel(chunks, *refs):
    n = len(chunks)
    sources, outs, bufs = refs[:n], refs[n:2 * n], refs[2 * n:3 * n]
    in_sem, out_sem = refs[3 * n:]
    loads, stores = [], []
    for src, out, buf, count in zip(sources, outs, bufs, chunks):
        rows = src.shape[0] // count
        for at in range(count):
            here = pl.ds(at * rows, rows)
            loads.append(pltpu.make_async_copy(src.at[here], buf.at[here], in_sem.at[len(loads)]))
            stores.append(pltpu.make_async_copy(buf.at[here], out.at[here], out_sem.at[len(stores)]))
    for load in loads:
        load.start()
    for load, store in zip(loads, stores):
        load.wait()
        store.start()
    for store in stores:
        store.wait()


def settle(*arrays):
    chunks = tuple(8 if array.ndim == 3 else 1 for array in arrays)
    anywhere = pl.BlockSpec(memory_space=pl.ANY)
    return pl.pallas_call(
        functools.partial(settle_kernel, chunks),
        out_shape=tuple(jax.ShapeDtypeStruct(array.shape, array.dtype) for array in arrays),
        in_specs=[anywhere] * len(arrays), out_specs=(anywhere,) * len(arrays),
        scratch_shapes=[pltpu.VMEM(array.shape, array.dtype) for array in arrays] + [dma_sems(sum(chunks))] * 2,
        compiler_params=pltpu.CompilerParams(vmem_limit_bytes=40 << 20),
    )(*arrays)


def solution(mesh):
    fine = Mesh(mesh.devices.reshape(2, CHIPS, CORES), ('y', 'x', 'c'))
    tok_spec = P(ALL, None)
    exp_spec = P('y', None, None)
    layer_specs = (P(None, None), tok_spec, tok_spec, exp_spec, exp_spec, exp_spec)
    grad_specs = (P(ALL, None), P('y', ('x', 'c'), None), P('y', ('x', 'c'), None), P('y', None, ('x', 'c')))

    def local_step(tokens, dy_out, dense_w1, route_idx1, route_gate1, w_gate1, w_up1, w_down1, dense_w2, route_idx2, route_gate2, w_gate2, w_up2, w_down2):
        w_gate1, w_up1, w_gate2, w_up2 = (jnp.swapaxes(w, 1, 2) for w in (w_gate1, w_up1, w_gate2, w_up2))
        y_one, u_two, u_all, dy_all, rank1, gate1, rank2, gate2 = layer_forward(
            tokens, dy_out, route_idx1.T, route_idx2.T, route_gate1.T, route_gate2.T, dense_w1, dense_w2, w_gate1, w_up1, w_down1)
        grad_mid, part_two, *grads_two = layer_backward(
            dy_all, u_two, rank2, gate2, y_one, dy_out, dense_w2, w_gate2, w_up2, w_down2)
        grad_tok, dense_one, dense_two, *grads_one = layer_backward(
            u_all, grad_mid, rank1, gate1, tokens, grad_mid, dense_w1, w_gate1, w_up1, w_down1, part_two)
        (grad_tok, dense_one, gate_one, up_one, down_one, dense_two, gate_two, up_two, down_two) = settle(
            grad_tok, dense_one, *grads_one, dense_two, *grads_two)
        gate_one, up_one, gate_two, up_two = (jnp.swapaxes(g, 1, 2) for g in (gate_one, up_one, gate_two, up_two))
        return (grad_tok, dense_one, gate_one, up_one, down_one, dense_two, gate_two, up_two, down_two)

    return jax.shard_map(local_step, mesh=fine, in_specs=(tok_spec, tok_spec) + layer_specs + layer_specs,
                         out_specs=(tok_spec,) + grad_specs + grad_specs, check_vma=False)
```

```python
import functools

import jax
import jax.numpy as jnp
from jax import lax
from jax.experimental import pallas as pl
from jax.experimental.pallas import tpu as pltpu
from jax.sharding import Mesh, PartitionSpec as P

F32 = jnp.float32
BF16 = jnp.bfloat16
CAP = 64
GROUP = 4
LANES = 256
CORES = 2
CHIPS = 2
ALL = ('x', 'c', 'y')
MESH = pl.DeviceIdType.MESH
FLIPS = ((0, 0), (0, 0), (0, 1), (0, 0), (0, 1), (1, 0), (1, 1))
ROUTE = 'yxxcccc'


def matmul(lhs, rhs, lhs_dim=1, rhs_dim=0):
    return lax.dot_general(lhs, rhs, (((lhs_dim,), (rhs_dim,)), ((), ())), preferred_element_type=F32)


def position():
    return tuple(lax.axis_index(name) for name in ALL)


def send(src, dst, sems, at, axis):
    return pltpu.make_async_remote_copy(src, dst, sems[0].at[at], sems[1].at[at],
                                        device_id={axis: 1 - lax.axis_index(axis)}, device_id_type=MESH)


def spreader(mine_ref, peer_ref, sems):
    ix, ic, iy = position()

    def copy(at):
        flip_x, flip_y = FLIPS[at]
        x = 1 - ix if flip_x else ix
        y = 1 - iy if flip_y else iy
        block = peer_ref.at[(x * CORES + ic) * 2 + y]
        return send(block if flip_x or flip_y else mine_ref, block, sems, at, ROUTE[at])

    return copy


def adder(p_ref, rs_ref, sems):
    ix, ic, iy = position()

    def copy(at):
        part = ((1 - ic) * 2 + 1 - iy, (1 - ic) * 2 + iy, ic * 2 + 1 - iy)[at]
        return send(p_ref.at[part], rs_ref.at[at], sems, at, 'ccy'[at])

    return copy


def greet(everyone):
    barrier = pltpu.get_barrier_semaphore()
    if everyone:
        others = [target(hop) for hop in range(1, 8)]
    else:
        others = [{axis: 1 - lax.axis_index(axis)} for axis in ALL]
    for other in others:
        pl.semaphore_signal(barrier, inc=1, device_id=other, device_id_type=MESH)
    pl.semaphore_wait(barrier, len(others))


def rank_of(x, c, y):
    return (x * CORES + c) * 2 + y


def target(hop):
    goal = lax.rem(rank_of(*position()) + hop, 8)
    return {'x': lax.div(goal, 4), 'c': lax.rem(lax.div(goal, 2), 2), 'y': lax.rem(goal, 2)}


def at_step(number):
    return pl.when(pl.program_id(0) == number)


def side_by_side(first, second):
    pad = jnp.zeros((LANES - first.shape[0], first.shape[1]), first.dtype)
    return jnp.concatenate([first, pad, second, pad], axis=0)


def select_rows(rank_ref, gate_ref, group, src):
    n_tok = rank_ref.shape[-1]
    slot = lax.broadcasted_iota(jnp.int32, (CAP, n_tok), 0)
    picks, gates = [], []
    for exp in range(GROUP):
        row = pl.ds(group * GROUP + exp, 1)
        hit = slot == rank_ref[src, row, :]
        picks.append(jnp.where(hit, 1.0, 0.0).astype(BF16))
        gates.append(jnp.sum(jnp.where(hit, gate_ref[src, row, :], 0.0), axis=1, keepdims=True))
    return jnp.concatenate(picks, axis=0), jnp.concatenate(gates, axis=0)


def route_table(route_ref, before_ref, src, layer, rank_ref, gate_ref, n_exp):
    _, ic, iy = position()
    n_tok = route_ref.shape[-1]
    experts = ((iy * CORES + ic) * n_exp + lax.broadcasted_iota(jnp.int32, (n_exp, n_tok), 0)).astype(F32)
    member = jnp.zeros((n_exp, n_tok), F32)
    gates = jnp.zeros((n_exp, n_tok), F32)
    for top in range(8):
        hit = experts == route_ref[src, layer * 8 + top:layer * 8 + top + 1, :]
        member = jnp.where(hit, 1.0, member)
        gates = jnp.where(hit, route_ref[src, 16 + layer * 8 + top:17 + layer * 8 + top, :], gates)
    count = matmul(member.astype(BF16), before_ref[...])
    rank_ref[src] = jnp.where(member > 0.0, count, -1.0).astype(jnp.int32)
    gate_ref[src] = gates


def forward_kernel(tok_ref, grad_ref, idx1_ref, idx2_ref, top1_ref, top2_ref, mix_ref, dense_ref, wg_ref, wu_ref, wd_ref,
                   y_ref, u_ref, uall_ref, dall_ref, rank1_ref, gate1_ref, rank2_ref, gate2_ref,
                   raw_ref, us_ref, ds_ref, routes_ref, route_ref, before_ref, pick_ref, row_ref, x_ref, part_ref, p_ref, rs_ref,
                   u_send, u_recv, d_send, d_recv, t_send, t_recv, rs_send, rs_recv, out_sem):
    n_exp, n_tok = rank1_ref.shape[1:]
    n_group = n_exp // GROUP
    step = pl.program_id(0)
    ix, ic, iy = position()
    me = rank_of(ix, ic, iy)
    spread_u = spreader(tok_ref, raw_ref, (u_send, u_recv))
    spread_d = spreader(grad_ref, ds_ref, (d_send, d_recv))
    spread_t = spreader(routes_ref, route_ref, (t_send, t_recv))
    add_up = adder(p_ref, rs_ref, (rs_send, rs_recv))
    stores = ((us_ref, uall_ref), (ds_ref, dall_ref))

    def mixed(x):
        return (x.astype(F32) + matmul(x, mix_ref[...])).astype(BF16)

    def pass_on(copy, arrived, onward):
        copy(arrived).wait_recv()
        for at in onward:
            copy(at).start()

    @at_step(0)
    def _():
        for at, part_in in enumerate((idx1_ref, idx2_ref, top1_ref, top2_ref)):
            routes_ref[at * 8:at * 8 + 8, :] = part_in[...].astype(F32)
        greet(False)
        for copy in (spread_t, spread_u):
            for at in (0, 3, 1):
                copy(at).start()
        us_ref[me] = mixed(tok_ref[...])
        ds_ref[me] = grad_ref[...]
        route_ref[me] = routes_ref[...]
        p_ref[...] = jnp.zeros_like(p_ref)
        before_ref[...] = jnp.where(lax.broadcasted_iota(jnp.int32, (n_tok, n_tok), 0)
                                    < lax.broadcasted_iota(jnp.int32, (n_tok, n_tok), 1), 1.0, 0.0).astype(BF16)
        pass_on(spread_t, 0, (4, 2))
        spread_u(3).wait_recv()
        us_ref[rank_of(ix, 1 - ic, iy)] = mixed(raw_ref[rank_of(ix, 1 - ic, iy)])
        spread_t(3).wait_recv()
        spread_t(4).wait_recv()

        @pl.loop(0, 4)
        def _(src):
            route_table(route_ref, before_ref, ix * 4 + src, 0, rank1_ref, gate1_ref, n_exp)

        pass_on(spread_u, 0, (4, 2))
        for at in (0, 3, 1):
            spread_d(at).start()
        us_ref[rank_of(ix, ic, 1 - iy)] = mixed(raw_ref[rank_of(ix, ic, 1 - iy)])
        spread_u(4).wait_recv()
        us_ref[rank_of(ix, 1 - ic, 1 - iy)] = mixed(raw_ref[rank_of(ix, 1 - ic, 1 - iy)])

    @at_step(n_group // 4)
    def _():
        pass_on(spread_t, 1, (5,))
        pass_on(spread_u, 1, (5,))

    @at_step(n_group // 2)
    def _():
        pass_on(spread_t, 2, (6,))
        pass_on(spread_u, 2, (6,))
        pass_on(spread_d, 0, (4, 2))

    @at_step(n_group - 1)
    def _():
        for copy in (spread_t, spread_u):
            copy(5).wait_recv()
            copy(6).wait_recv()

        @pl.loop(0, 4)
        def _(src):
            us_ref[(1 - ix) * 4 + src] = mixed(raw_ref[(1 - ix) * 4 + src])
            route_table(route_ref, before_ref, (1 - ix) * 4 + src, 0, rank1_ref, gate1_ref, n_exp)

        @pl.loop(0, 8)
        def _(src):
            route_table(route_ref, before_ref, src, 1, rank2_ref, gate2_ref, n_exp)

    @at_step(n_group)
    def _():
        add_up(0).start()
        pltpu.make_async_copy(us_ref, uall_ref, out_sem.at[0]).start()

    @at_step(n_group + 1)
    def _():
        add_up(2).start()

    @at_step(n_group + n_group // 2)
    def _():
        pass_on(spread_d, 1, (5,))

    @at_step(2 * n_group - 2)
    def _():
        pass_on(spread_d, 2, (6,))

    @at_step(2 * n_group - 1)
    def _():
        for at in (3, 4, 5, 6):
            spread_d(at).wait_recv()
        pltpu.make_async_copy(ds_ref, dall_ref, out_sem.at[1]).start()

    group = lax.rem(step, n_group)
    far = 1 - lax.div(step, n_group)
    y_now = jnp.where(far == 1, 1 - iy, iy)

    for core in range(CORES):
        src = rank_of(ix, core, y_now)
        pick, gate = select_rows(rank1_ref, gate1_ref, group, src)
        pick_ref[core] = pick
        rows = matmul(pick, us_ref[src]).astype(BF16)
        at = slice(core * CAP, (core + 1) * CAP)
        for exp in range(GROUP):
            x_ref[exp, at, :] = rows[exp * CAP:(exp + 1) * CAP]
            row_ref[exp, at, :] = jnp.broadcast_to(gate[exp * CAP:(exp + 1) * CAP], (CAP, 128))

    ff = wg_ref.shape[1]
    pre = {}
    for tick in range(GROUP + 2):
        if tick < GROUP:
            pre[tick] = matmul(x_ref[tick], side_by_side(wg_ref[tick], wu_ref[tick]), 1, 1)
        if 0 < tick <= GROUP:
            both = pre.pop(tick - 1)
            a_pre, b_pre = both[:, :ff], both[:, LANES:LANES + ff]
            pre[tick - 1, 1] = (a_pre * jax.nn.sigmoid(a_pre) * b_pre).astype(BF16)
        if tick > 1:
            exp = tick - 2
            out = matmul(pre.pop((exp, 1)), wd_ref[exp]).astype(BF16).astype(F32) * row_ref[exp][:, :1]
            high = out.astype(BF16)
            rest = out - high.astype(F32)
            mid = rest.astype(BF16)
            low = (rest - mid.astype(F32)).astype(BF16)
            at = slice(exp * CAP, (exp + 1) * CAP)
            for core in range(CORES):
                here = slice(core * CAP, (core + 1) * CAP)
                part_ref[core, 0, at, :] = high[here]
                part_ref[core, 1, at, :] = mid[here]
                part_ref[core, 2, at, :] = low[here]

    for core in range(CORES):
        pick = pick_ref[core]
        total = matmul(pick, part_ref[core, 0], 0, 0)
        total += matmul(pick, part_ref[core, 1], 0, 0) + matmul(pick, part_ref[core, 2], 0, 0)
        p_ref[core * 2 + y_now] += total

    @at_step(n_group)
    def _():
        add_up(0).wait_recv()
        p_ref[ic * 2 + 1 - iy] += rs_ref[0]

    @at_step(2 * n_group - 1)
    def _():
        add_up(1).start()
        add_up(1).wait_recv()
        add_up(2).wait_recv()
        y_own = (us_ref[me].astype(F32) + (p_ref[ic * 2 + iy] + rs_ref[1] + rs_ref[2])).astype(BF16)
        y_ref[...] = y_own
        u_ref[...] = (y_own.astype(F32) + matmul(y_own, dense_ref[...])).astype(BF16)
        for copy in (spread_u, spread_d, spread_t):
            for at in range(7):
                copy(at).wait_send()
        for at in range(3):
            add_up(at).wait_send()
        for at in range(2):
            pltpu.make_async_copy(*stores[at], out_sem.at[at]).wait()


def layer_kernel(last_layer, *refs):
    refs = list(refs)
    whole_ref, mine_ref, rank_ref, gate_ref, x_own_ref, grad_own_ref, dense_ref, wg_ref, wu_ref, wd_ref = refs[:10]
    del refs[:10]
    if last_layer:
        other_ref = refs.pop(0)
        one_ref, two_ref = refs[1:3]
        del refs[1:3]
    else:
        part_ref = refs.pop(1)
    gx_out_ref, gg_ref, gu_ref, gd_ref = refs[:4]
    (peer_ref, xo_ref, do_ref, h_ref, ga_ref, gb_ref, pick_ref, gx_ref, p_ref, rs_ref, x_ref, d_ref, stage_ref,
     ag_send, ag_recv, rs_send, rs_recv, keep_sem, give_send, give_recv) = refs[4:24]
    if last_layer:
        part_ref, land_ref, land_send, land_recv = refs[24:]
    n_src, _, dim = whole_ref.shape
    own = n_src // CHIPS
    n_group = xo_ref.shape[0] // GROUP
    n_first = 2 * n_group
    n_step = 3 * n_group
    half = dim // CHIPS
    piece = half // CORES
    step = pl.program_id(0)
    ix, ic, iy = position()
    cols = pl.ds(pl.multiple_of(ix * half, half), half)
    u_ref, dy_ref = (whole_ref, peer_ref) if last_layer else (peer_ref, whole_ref)
    outs = (gg_ref, gu_ref, gd_ref)
    spread = spreader(mine_ref, peer_ref, (ag_send, ag_recv))
    add_up = adder(p_ref, rs_ref, (rs_send, rs_recv))

    def land_copy(layer, hop):
        goal = target(hop)
        rows = dim // 8
        src = (part_ref, other_ref)[layer]
        at = pl.ds(pl.multiple_of(rank_of(goal['x'], goal['c'], goal['y']) * rows, rows), rows)
        return pltpu.make_async_remote_copy(src.at[at, :], land_ref.at[layer, hop], land_send.at[layer, hop],
                                            land_recv.at[layer, hop], device_id=goal, device_id_type=MESH)

    def land_sum(layer, out_ref):
        rows = dim // 8
        at = pl.ds(pl.multiple_of(rank_of(ix, ic, iy) * rows, rows), rows)
        total = (part_ref, other_ref)[layer][at, :].astype(F32)
        for hop in range(1, 8):
            land_copy(layer, hop).wait_recv()
            total += land_ref[layer, hop].astype(F32)
        out_ref[...] = total.astype(BF16)

    def store_copies(group, moved):
        buf = lax.rem(group, 2)
        rows = pl.ds(ic * n_group * GROUP + group * GROUP, GROUP)
        for kind in range(3):
            dst = outs[kind].at[rows]
            if moved:
                yield pltpu.make_async_remote_copy(
                    stage_ref.at[buf, 1 - ic, kind], dst, give_send.at[buf, kind], give_recv.at[group, kind],
                    device_id={'c': 1 - ic}, device_id_type=MESH)
            else:
                yield pltpu.make_async_copy(stage_ref.at[buf, ic, kind], dst, keep_sem.at[buf, kind])

    def store_start(group):
        for moved in (True, False):
            for copy in store_copies(group, moved):
                copy.start()

    def store_wait(group):
        for copy in store_copies(group, True):
            copy.wait_send()
        for copy in store_copies(group, False):
            copy.wait()

    def pull(src, group, at, keep):
        pick, gate = select_rows(rank_ref, gate_ref, group, src)
        if keep:
            pick_ref[at] = pick
        x_rows = matmul(pick, u_ref[src]).astype(BF16)
        d_rows = (matmul(pick, dy_ref[src]) * gate).astype(BF16)
        for exp in range(GROUP):
            x_ref[exp, at * CAP:(at + 1) * CAP, :] = x_rows[exp * CAP:(exp + 1) * CAP]
            d_ref[exp, at * CAP:(at + 1) * CAP, :] = d_rows[exp * CAP:(exp + 1) * CAP]

    def hidden_pre(x_rows, d_rows, exp):
        ff = wg_ref.shape[1]
        both = matmul(x_rows, side_by_side(wg_ref[exp], wu_ref[exp]), 1, 1)
        return both[:, :ff], both[:, LANES:LANES + ff], matmul(d_rows, wd_ref[exp], 1, 1)

    def hidden_grads(a_pre, b_pre, back):
        sigma = jax.nn.sigmoid(a_pre)
        silu = a_pre * sigma
        grad_hidden = back.astype(BF16).astype(F32)
        grad_a = (grad_hidden * b_pre * sigma * (1.0 + a_pre * (1.0 - sigma))).astype(BF16)
        return (silu * b_pre).astype(BF16), grad_a, (grad_hidden * silu).astype(BF16)

    @at_step(0)
    def _():
        greet(last_layer)
        for at in (0, 3, 1):
            spread(at).start()
        if last_layer:
            for hop in range(1, 8):
                land_copy(1, hop).start()
        peer_ref[rank_of(ix, ic, iy)] = mine_ref[...]
        p_ref[...] = jnp.zeros_like(p_ref)
        spread(3).wait_recv()

    @at_step(n_group - 2)
    def _():
        spread(0).wait_recv()
        spread(4).start()
        spread(2).start()

    @at_step(n_group)
    def _():
        spread(4).wait_recv()

    @at_step(n_group + n_group // 2)
    def _():
        spread(1).wait_recv()
        spread(5).start()

    @at_step(n_first - 1)
    def _():
        spread(2).wait_recv()
        spread(6).start()

    @pl.when(step < n_first)
    def _():
        group = lax.rem(step, n_group)
        late = lax.div(step, n_group)
        y_now = jnp.where(late == 1, 1 - iy, iy)
        base = group * GROUP
        rows = pl.ds(pl.multiple_of(late * CORES * CAP, CORES * CAP), CORES * CAP)

        for core in range(CORES):
            pull(rank_of(ix, core, y_now), group, core, True)

        near = CORES * CAP
        pre = {}
        for tick in range(GROUP + 2):
            if tick < GROUP:
                pre[tick] = hidden_pre(x_ref[tick, :near, :], d_ref[tick, :near, :], tick)
            if 0 < tick <= GROUP:
                exp = tick - 1
                hidden, grad_a, grad_b = hidden_grads(*pre.pop(exp))
                xo_ref[base + exp, rows, :] = x_ref[exp, :near, cols]
                do_ref[base + exp, rows, :] = d_ref[exp, :near, cols]
                h_ref[base + exp, rows, :] = hidden
                ga_ref[base + exp, rows, :] = grad_a
                gb_ref[base + exp, rows, :] = grad_b
                pre[exp, 1] = None
            if tick > 1:
                exp = tick - 2
                grad_x = (matmul(ga_ref[base + exp, rows, :], wg_ref[exp]) + matmul(gb_ref[base + exp, rows, :], wu_ref[exp])).astype(BF16)
                at = slice(exp * CAP, (exp + 1) * CAP)
                for core in range(CORES):
                    gx_ref[core, at, :] = grad_x[core * CAP:(core + 1) * CAP]

        for core in range(CORES):
            p_ref[core * 2 + y_now] += matmul(pick_ref[core], gx_ref[core], 0, 0)

    @at_step(n_first)
    def _():
        add_up(0).start()
        add_up(1).start()
        spread(5).wait_recv()
        spread(6).wait_recv()
        add_up(0).wait_recv()
        p_ref[ic * 2 + 1 - iy] += rs_ref[0]
        add_up(2).start()

    @at_step(n_step - 1)
    def _():
        add_up(1).wait_recv()
        add_up(2).wait_recv()
        total = p_ref[ic * 2 + iy] + rs_ref[1] + rs_ref[2]
        grad = (grad_own_ref[...].astype(F32) + total).astype(BF16)
        part_ref[...] = matmul(x_own_ref[...], grad, 0, 0).astype(BF16)
        gx_out_ref[...] = (grad.astype(F32) + matmul(grad, dense_ref[...], 1, 1)).astype(BF16)
        if last_layer:
            for hop in range(1, 8):
                land_copy(0, hop).start()

    @pl.when(step >= n_first)
    def _():
        group = step - n_first

        @pl.when(group >= 2)
        def _():
            store_wait(group - 2)

        @pl.when(group >= 1)
        def _():
            store_start(group - 1)

        for src in range(own):
            pull((1 - ix) * own + src, group, src, False)

        buf = lax.rem(group, 2)

        pre = {}
        for tick in range(GROUP + 2):
            if tick < GROUP:
                pre[tick] = hidden_pre(x_ref[tick], d_ref[tick], tick)
            if 0 < tick <= GROUP:
                exp = tick - 1
                pre[exp, 1] = hidden_grads(*pre.pop(exp))
            if tick > 1:
                exp = tick - 2
                base = group * GROUP + exp
                hidden, grad_a, grad_b = pre.pop((exp, 1))
                x_own, x_far = xo_ref[base], x_ref[exp, :, cols]
                d_own, d_far = do_ref[base], d_ref[exp, :, cols]
                grads = (matmul(ga_ref[base], x_own, 0, 0) + matmul(grad_a, x_far, 0, 0),
                         matmul(gb_ref[base], x_own, 0, 0) + matmul(grad_b, x_far, 0, 0),
                         matmul(h_ref[base], d_own, 0, 0) + matmul(hidden, d_far, 0, 0))
                for kind in range(3):
                    for core in range(CORES):
                        stage_ref[buf, core, kind, exp] = grads[kind][:, core * piece:(core + 1) * piece].astype(BF16)

    @at_step(n_step - 1)
    def _():
        last = n_group - 1
        store_wait(last - 1)
        store_start(last)
        if last_layer:
            land_sum(1, two_ref)
            land_sum(0, one_ref)
            for layer in range(2):
                for hop in range(1, 8):
                    land_copy(layer, hop).wait_send()
        for at in range(7):
            spread(at).wait_send()
        for at in range(3):
            add_up(at).wait_send()
        store_wait(last)
        for group in range(n_group):
            for copy in store_copies(group, True):
                copy.wait_recv()


def fixed(*shape):
    return pl.BlockSpec(shape, lambda s: (0,) * len(shape), pipeline_mode=pl.Buffered(1))


def weight_spec(groups, ff, dim):
    return pl.BlockSpec((GROUP, ff, dim), lambda s: (lax.axis_index('c') * groups + lax.rem(s, groups), 0, 0))


def dma_sems(*shape):
    return pltpu.SemaphoreType.DMA(shape)


def sums_scratch(own, n_tok, dim):
    return [pltpu.VMEM((own, n_tok, dim), F32), pltpu.VMEM((3, n_tok, dim), F32)]


def layer_forward(tokens, grad, idx1, idx2, top1, top2, dense1, dense2, w_gate, w_up, w_down):
    n_tok, dim = tokens.shape
    top = idx1.shape[0]
    n_all, ff, _ = w_gate.shape
    n_exp = n_all // CORES
    n_src = 8
    own = n_src // CHIPS
    groups = n_exp // GROUP
    tall = weight_spec(groups, ff, dim)
    table = fixed(n_src, n_exp, n_tok)
    block = jax.ShapeDtypeStruct((n_tok, dim), BF16)
    every = jax.ShapeDtypeStruct((n_src, n_tok, dim), BF16)
    ranks = jax.ShapeDtypeStruct((n_src, n_exp, n_tok), jnp.int32)
    gates = jax.ShapeDtypeStruct((n_src, n_exp, n_tok), F32)
    anywhere = pl.BlockSpec(memory_space=pl.ANY)
    rows = CORES * CAP
    return pl.pallas_call(
        forward_kernel,
        out_shape=(block, block, every, every, ranks, gates, ranks, gates),
        grid_spec=pltpu.PrefetchScalarGridSpec(
            num_scalar_prefetch=0, grid=(2 * groups,),
            in_specs=[fixed(n_tok, dim)] * 2 + [fixed(top, n_tok)] * 4 + [fixed(dim, dim)] * 2 + [tall] * 3,
            out_specs=(fixed(n_tok, dim), fixed(n_tok, dim), anywhere, anywhere, table, table, table, table),
            scratch_shapes=[pltpu.VMEM((n_src, n_tok, dim), BF16)] * 3
            + [pltpu.VMEM((4 * top, n_tok), F32), pltpu.VMEM((n_src, 4 * top, n_tok), F32), pltpu.VMEM((n_tok, n_tok), BF16),
                            pltpu.VMEM((CORES, GROUP * CAP, n_tok), BF16), pltpu.VMEM((GROUP, rows, 128), F32),
                            pltpu.VMEM((GROUP, rows, dim), BF16), pltpu.VMEM((CORES, 3, GROUP * CAP, dim), BF16)]
            + sums_scratch(own, n_tok, dim)
            + [dma_sems(7)] * 6 + [dma_sems(3)] * 2 + [dma_sems(2)]),
        compiler_params=pltpu.CompilerParams(dimension_semantics=('arbitrary',), vmem_limit_bytes=62 << 20,
                                             collective_id=0, has_side_effects=True),
    )(tokens, grad, idx1, idx2, top1, top2, dense1, dense2, w_gate, w_up, w_down)


def layer_backward(whole, mine, rank, gate, x_own, grad_own, dense, w_gate, w_up, w_down, other=None):
    n_src, n_tok, dim = whole.shape
    n_all, ff, _ = w_gate.shape
    n_exp = rank.shape[1]
    own = n_src // CHIPS
    piece = dim // (CHIPS * CORES)
    groups = n_exp // GROUP
    kept = own * CAP
    last_layer = other is not None
    tall = weight_spec(groups, ff, dim)
    table = fixed(n_src, n_exp, n_tok)
    block = fixed(n_tok, dim)
    square = fixed(dim, dim)
    slab = fixed(dim // 8, dim)
    grad_shape = jax.ShapeDtypeStruct((n_all, ff, piece), BF16)
    part_shape = jax.ShapeDtypeStruct((dim, dim), BF16)
    slab_shape = jax.ShapeDtypeStruct((dim // 8, dim), BF16)
    extra_shapes = (slab_shape, slab_shape) if last_layer else (part_shape,)
    extra_specs = (slab, slab) if last_layer else (square,)
    half = dim // CHIPS
    scratch = [pltpu.VMEM((n_src, n_tok, dim), BF16), pltpu.VMEM((n_exp, kept, half), BF16),
               pltpu.VMEM((n_exp, kept, half), BF16), pltpu.VMEM((n_exp, kept, ff), BF16),
               pltpu.VMEM((n_exp, kept, ff), BF16), pltpu.VMEM((n_exp, kept, ff), BF16),
               pltpu.VMEM((CORES, GROUP * CAP, n_tok), BF16), pltpu.VMEM((CORES, GROUP * CAP, dim), BF16)]
    scratch += sums_scratch(own, n_tok, dim)
    scratch += [pltpu.VMEM((GROUP, kept, dim), BF16), pltpu.VMEM((GROUP, kept, dim), BF16),
                pltpu.VMEM((2, CORES, 3, GROUP, ff, piece), BF16),
                dma_sems(7), dma_sems(7), dma_sems(3), dma_sems(3), dma_sems(2, 3), dma_sems(2, 3), dma_sems(groups, 3)]
    if last_layer:
        scratch += [pltpu.VMEM((dim, dim), BF16), pltpu.VMEM((2, 8, dim // 8, dim), BF16), dma_sems(2, 8), dma_sems(2, 8)]
    operands = (whole, mine, rank, gate, x_own, grad_own, dense, w_gate, w_up, w_down) + ((other,) if last_layer else ())
    return pl.pallas_call(
        functools.partial(layer_kernel, last_layer),
        out_shape=(jax.ShapeDtypeStruct((n_tok, dim), BF16),) + extra_shapes + (grad_shape,) * 3,
        grid_spec=pltpu.PrefetchScalarGridSpec(
            num_scalar_prefetch=0, grid=(3 * groups,),
            in_specs=[fixed(n_src, n_tok, dim), block, table, table, block, block, square, tall, tall, tall]
            + ([square] if last_layer else []),
            out_specs=(block,) + extra_specs + (pl.BlockSpec(memory_space=pl.ANY),) * 3,
            scratch_shapes=scratch),
        compiler_params=pltpu.CompilerParams(dimension_semantics=('arbitrary',), vmem_limit_bytes=67043328,
                                             collective_id=1 + int(last_layer), has_side_effects=True),
    )(*operands)


def settle_kernel(chunks, *refs):
    n = len(chunks)
    sources, outs, bufs = refs[:n], refs[n:2 * n], refs[2 * n:3 * n]
    in_sem, out_sem = refs[3 * n:]
    loads, stores = [], []
    for src, out, buf, count in zip(sources, outs, bufs, chunks):
        rows = src.shape[0] // count
        for at in range(count):
            here = pl.ds(at * rows, rows)
            loads.append(pltpu.make_async_copy(src.at[here], buf.at[here], in_sem.at[len(loads)]))
            stores.append(pltpu.make_async_copy(buf.at[here], out.at[here], out_sem.at[len(stores)]))
    for load in loads:
        load.start()
    for load, store in zip(loads, stores):
        load.wait()
        store.start()
    for store in stores:
        store.wait()


def settle(*arrays):
    chunks = tuple(8 if array.ndim == 3 else 1 for array in arrays)
    anywhere = pl.BlockSpec(memory_space=pl.ANY)
    return pl.pallas_call(
        functools.partial(settle_kernel, chunks),
        out_shape=tuple(jax.ShapeDtypeStruct(array.shape, array.dtype) for array in arrays),
        in_specs=[anywhere] * len(arrays), out_specs=(anywhere,) * len(arrays),
        scratch_shapes=[pltpu.VMEM(array.shape, array.dtype) for array in arrays] + [dma_sems(sum(chunks))] * 2,
        compiler_params=pltpu.CompilerParams(vmem_limit_bytes=67043328),
    )(*arrays)


def solution(mesh):
    fine = Mesh(mesh.devices.reshape(2, CHIPS, CORES), ('y', 'x', 'c'))
    tok_spec = P(ALL, None)
    exp_spec = P('y', None, None)
    layer_specs = (P(None, None), tok_spec, tok_spec, exp_spec, exp_spec, exp_spec)
    grad_specs = (P(ALL, None), P('y', ('x', 'c'), None), P('y', ('x', 'c'), None), P('y', None, ('x', 'c')))

    def local_step(tokens, dy_out, dense_w1, route_idx1, route_gate1, w_gate1, w_up1, w_down1, dense_w2, route_idx2, route_gate2, w_gate2, w_up2, w_down2):
        w_gate1, w_up1, w_gate2, w_up2 = (jnp.swapaxes(w, 1, 2) for w in (w_gate1, w_up1, w_gate2, w_up2))
        y_one, u_two, u_all, dy_all, rank1, gate1, rank2, gate2 = layer_forward(
            tokens, dy_out, route_idx1.T, route_idx2.T, route_gate1.T, route_gate2.T, dense_w1, dense_w2, w_gate1, w_up1, w_down1)
        grad_mid, part_two, *grads_two = layer_backward(
            dy_all, u_two, rank2, gate2, y_one, dy_out, dense_w2, w_gate2, w_up2, w_down2)
        grad_tok, dense_one, dense_two, *grads_one = layer_backward(
            u_all, grad_mid, rank1, gate1, tokens, grad_mid, dense_w1, w_gate1, w_up1, w_down1, part_two)
        (grad_tok, dense_one, gate_one, up_one, down_one, dense_two, gate_two, up_two, down_two) = settle(
            grad_tok, dense_one, *grads_one, dense_two, *grads_two)
        gate_one, up_one, gate_two, up_two = (jnp.swapaxes(g, 1, 2) for g in (gate_one, up_one, gate_two, up_two))
        return (grad_tok, dense_one, gate_one, up_one, down_one, dense_two, gate_two, up_two, down_two)

    return jax.shard_map(local_step, mesh=fine, in_specs=(tok_spec, tok_spec) + layer_specs + layer_specs,
                         out_specs=(tok_spec,) + grad_specs + grad_specs, check_vma=False)
```

```python
import functools

import jax
import jax.numpy as jnp
from jax import lax
from jax.experimental import pallas as pl
from jax.experimental.pallas import tpu as pltpu
from jax.sharding import Mesh, PartitionSpec as P

F32 = jnp.float32
BF16 = jnp.bfloat16
CAP = 64
GROUP = 8
LANES = 256
CORES = 2
CHIPS = 2
ALL = ('x', 'c', 'y')
MESH = pl.DeviceIdType.MESH
FLIPS = ((0, 0), (0, 0), (0, 1), (0, 0), (0, 1), (1, 0), (1, 1))
ROUTE = 'yxxcccc'


def matmul(lhs, rhs, lhs_dim=1, rhs_dim=0):
    return lax.dot_general(lhs, rhs, (((lhs_dim,), (rhs_dim,)), ((), ())), preferred_element_type=F32)


def position():
    return tuple(lax.axis_index(name) for name in ALL)


def send(src, dst, sems, at, axis):
    return pltpu.make_async_remote_copy(src, dst, sems[0].at[at], sems[1].at[at],
                                        device_id={axis: 1 - lax.axis_index(axis)}, device_id_type=MESH)


def spreader(mine_ref, peer_ref, sems):
    ix, ic, iy = position()

    def copy(at):
        flip_x, flip_y = FLIPS[at]
        x = 1 - ix if flip_x else ix
        y = 1 - iy if flip_y else iy
        block = peer_ref.at[(x * CORES + ic) * 2 + y]
        return send(block if flip_x or flip_y else mine_ref, block, sems, at, ROUTE[at])

    return copy


def adder(p_ref, rs_ref, sems):
    ix, ic, iy = position()

    def copy(at):
        part = ((1 - ic) * 2 + 1 - iy, (1 - ic) * 2 + iy, ic * 2 + 1 - iy)[at]
        return send(p_ref.at[part], rs_ref.at[at], sems, at, 'ccy'[at])

    return copy


def greet(everyone):
    barrier = pltpu.get_barrier_semaphore()
    if everyone:
        others = [target(hop) for hop in range(1, 8)]
    else:
        others = [{axis: 1 - lax.axis_index(axis)} for axis in ALL]
    for other in others:
        pl.semaphore_signal(barrier, inc=1, device_id=other, device_id_type=MESH)
    pl.semaphore_wait(barrier, len(others))


def rank_of(x, c, y):
    return (x * CORES + c) * 2 + y


def target(hop):
    goal = lax.rem(rank_of(*position()) + hop, 8)
    return {'x': lax.div(goal, 4), 'c': lax.rem(lax.div(goal, 2), 2), 'y': lax.rem(goal, 2)}


def at_step(number):
    return pl.when(pl.program_id(0) == number)


def side_by_side(first, second):
    pad = jnp.zeros((LANES - first.shape[0], first.shape[1]), first.dtype)
    return jnp.concatenate([first, pad, second, pad], axis=0)


def select_rows(rank_ref, gate_ref, group, src):
    n_tok = rank_ref.shape[-1]
    slot = lax.broadcasted_iota(jnp.int32, (CAP, n_tok), 0)
    picks, gates = [], []
    for exp in range(GROUP):
        row = pl.ds(group * GROUP + exp, 1)
        hit = slot == rank_ref[src, row, :]
        picks.append(jnp.where(hit, 1.0, 0.0).astype(BF16))
        gates.append(jnp.sum(jnp.where(hit, gate_ref[src, row, :], 0.0), axis=1, keepdims=True))
    return jnp.concatenate(picks, axis=0), jnp.concatenate(gates, axis=0)


def route_table(route_ref, before_ref, src, layer, rank_ref, gate_ref, n_exp):
    _, ic, iy = position()
    n_tok = route_ref.shape[-1]
    experts = ((iy * CORES + ic) * n_exp + lax.broadcasted_iota(jnp.int32, (n_exp, n_tok), 0)).astype(F32)
    member = jnp.zeros((n_exp, n_tok), F32)
    gates = jnp.zeros((n_exp, n_tok), F32)
    for top in range(8):
        hit = experts == route_ref[src, layer * 8 + top:layer * 8 + top + 1, :]
        member = jnp.where(hit, 1.0, member)
        gates = jnp.where(hit, route_ref[src, 16 + layer * 8 + top:17 + layer * 8 + top, :], gates)
    count = matmul(member.astype(BF16), before_ref[...])
    rank_ref[src] = jnp.where(member > 0.0, count, -1.0).astype(jnp.int32)
    gate_ref[src] = gates


def forward_kernel(tok_ref, grad_ref, idx1_ref, idx2_ref, top1_ref, top2_ref, mix_ref, dense_ref, wg_ref, wu_ref, wd_ref,
                   y_ref, u_ref, uall_ref, dall_ref, rank1_ref, gate1_ref, rank2_ref, gate2_ref,
                   raw_ref, us_ref, ds_ref, routes_ref, route_ref, before_ref, pick_ref, row_ref, x_ref, part_ref, p_ref, rs_ref,
                   u_send, u_recv, d_send, d_recv, t_send, t_recv, rs_send, rs_recv, out_sem):
    n_exp, n_tok = rank1_ref.shape[1:]
    n_group = n_exp // GROUP
    step = pl.program_id(0)
    ix, ic, iy = position()
    me = rank_of(ix, ic, iy)
    spread_u = spreader(tok_ref, raw_ref, (u_send, u_recv))
    spread_d = spreader(grad_ref, ds_ref, (d_send, d_recv))
    spread_t = spreader(routes_ref, route_ref, (t_send, t_recv))
    add_up = adder(p_ref, rs_ref, (rs_send, rs_recv))
    stores = ((us_ref, uall_ref), (ds_ref, dall_ref))

    def mixed(x):
        return (x.astype(F32) + matmul(x, mix_ref[...])).astype(BF16)

    def pass_on(copy, arrived, onward):
        copy(arrived).wait_recv()
        for at in onward:
            copy(at).start()

    @at_step(0)
    def _():
        for at, part_in in enumerate((idx1_ref, idx2_ref, top1_ref, top2_ref)):
            routes_ref[at * 8:at * 8 + 8, :] = part_in[...].astype(F32)
        greet(False)
        for copy in (spread_t, spread_u):
            for at in (0, 3, 1):
                copy(at).start()
        us_ref[me] = mixed(tok_ref[...])
        ds_ref[me] = grad_ref[...]
        route_ref[me] = routes_ref[...]
        p_ref[...] = jnp.zeros_like(p_ref)
        before_ref[...] = jnp.where(lax.broadcasted_iota(jnp.int32, (n_tok, n_tok), 0)
                                    < lax.broadcasted_iota(jnp.int32, (n_tok, n_tok), 1), 1.0, 0.0).astype(BF16)
        pass_on(spread_t, 0, (4, 2))
        spread_u(3).wait_recv()
        us_ref[rank_of(ix, 1 - ic, iy)] = mixed(raw_ref[rank_of(ix, 1 - ic, iy)])
        spread_t(3).wait_recv()
        spread_t(4).wait_recv()

        @pl.loop(0, 4)
        def _(src):
            route_table(route_ref, before_ref, ix * 4 + src, 0, rank1_ref, gate1_ref, n_exp)

        pass_on(spread_u, 0, (4, 2))
        for at in (0, 3, 1):
            spread_d(at).start()
        us_ref[rank_of(ix, ic, 1 - iy)] = mixed(raw_ref[rank_of(ix, ic, 1 - iy)])
        spread_u(4).wait_recv()
        us_ref[rank_of(ix, 1 - ic, 1 - iy)] = mixed(raw_ref[rank_of(ix, 1 - ic, 1 - iy)])

    @at_step(n_group // 4)
    def _():
        pass_on(spread_t, 1, (5,))
        pass_on(spread_u, 1, (5,))

    @at_step(n_group // 2)
    def _():
        pass_on(spread_t, 2, (6,))
        pass_on(spread_u, 2, (6,))
        pass_on(spread_d, 0, (4, 2))

    @at_step(n_group - 1)
    def _():
        for copy in (spread_t, spread_u):
            copy(5).wait_recv()
            copy(6).wait_recv()

        @pl.loop(0, 4)
        def _(src):
            us_ref[(1 - ix) * 4 + src] = mixed(raw_ref[(1 - ix) * 4 + src])
            route_table(route_ref, before_ref, (1 - ix) * 4 + src, 0, rank1_ref, gate1_ref, n_exp)

        @pl.loop(0, 8)
        def _(src):
            route_table(route_ref, before_ref, src, 1, rank2_ref, gate2_ref, n_exp)

    @at_step(n_group)
    def _():
        add_up(0).start()
        pltpu.make_async_copy(us_ref, uall_ref, out_sem.at[0]).start()

    @at_step(n_group + n_group // 2)
    def _():
        pass_on(spread_d, 1, (5,))

    @at_step(2 * n_group - 2)
    def _():
        pass_on(spread_d, 2, (6,))

    @at_step(2 * n_group - 1)
    def _():
        for at in (3, 4, 5, 6):
            spread_d(at).wait_recv()
        pltpu.make_async_copy(ds_ref, dall_ref, out_sem.at[1]).start()

    group = lax.rem(step, n_group)
    far = 1 - lax.div(step, n_group)
    y_now = jnp.where(far == 1, 1 - iy, iy)

    for core in range(CORES):
        src = rank_of(ix, core, y_now)
        pick, gate = select_rows(rank1_ref, gate1_ref, group, src)
        pick_ref[core] = pick
        rows = matmul(pick, us_ref[src]).astype(BF16)
        at = slice(core * CAP, (core + 1) * CAP)
        for exp in range(GROUP):
            x_ref[exp, at, :] = rows[exp * CAP:(exp + 1) * CAP]
            row_ref[exp, at, :] = jnp.broadcast_to(gate[exp * CAP:(exp + 1) * CAP], (CAP, 128))

    @at_step(n_group)
    def _():
        add_up(0).wait_recv()
        p_ref[ic * 2 + 1 - iy] += rs_ref[0]
        add_up(2).start()

    ff = wg_ref.shape[1]
    pre = {}
    for tick in range(GROUP + 2):
        if tick < GROUP:
            pre[tick] = matmul(x_ref[tick], side_by_side(wg_ref[tick], wu_ref[tick]), 1, 1)
        if 0 < tick <= GROUP:
            both = pre.pop(tick - 1)
            a_pre, b_pre = both[:, :ff], both[:, LANES:LANES + ff]
            pre[tick - 1, 1] = (a_pre * jax.nn.sigmoid(a_pre) * b_pre).astype(BF16)
        if tick > 1:
            exp = tick - 2
            out = matmul(pre.pop((exp, 1)), wd_ref[exp]).astype(BF16).astype(F32) * row_ref[exp][:, :1]
            high = out.astype(BF16)
            rest = out - high.astype(F32)
            mid = rest.astype(BF16)
            low = (rest - mid.astype(F32)).astype(BF16)
            at = slice(exp * CAP, (exp + 1) * CAP)
            for core in range(CORES):
                here = slice(core * CAP, (core + 1) * CAP)
                part_ref[core, 0, at, :] = high[here]
                part_ref[core, 1, at, :] = mid[here]
                part_ref[core, 2, at, :] = low[here]

    for core in range(CORES):
        pick = pick_ref[core]
        total = matmul(pick, part_ref[core, 0], 0, 0)
        total += matmul(pick, part_ref[core, 1], 0, 0) + matmul(pick, part_ref[core, 2], 0, 0)
        p_ref[core * 2 + y_now] += total

    @at_step(2 * n_group - 1)
    def _():
        add_up(1).start()
        add_up(1).wait_recv()
        add_up(2).wait_recv()
        y_own = (us_ref[me].astype(F32) + (p_ref[ic * 2 + iy] + rs_ref[1] + rs_ref[2])).astype(BF16)
        y_ref[...] = y_own
        u_ref[...] = (y_own.astype(F32) + matmul(y_own, dense_ref[...])).astype(BF16)
        for copy in (spread_u, spread_d, spread_t):
            for at in range(7):
                copy(at).wait_send()
        for at in range(3):
            add_up(at).wait_send()
        for at in range(2):
            pltpu.make_async_copy(*stores[at], out_sem.at[at]).wait()


def layer_kernel(last_layer, *refs):
    refs = list(refs)
    whole_ref, mine_ref, rank_ref, gate_ref, x_own_ref, dense_ref, wg_ref, wu_ref, wd_ref, other_ref = refs[:10]
    del refs[:10]
    grad_own_ref = mine_ref if last_layer else other_ref
    if last_layer:
        one_ref, two_ref = refs[1:3]
        del refs[1:3]
    else:
        part_ref = refs.pop(1)
    gx_out_ref, gg_ref, gu_ref, gd_ref = refs[:4]
    (peer_ref, xo_ref, do_ref, h_ref, ga_ref, gb_ref, pick_ref, gx_ref, p_ref, rs_ref, x_ref, d_ref, stage_ref,
     ag_send, ag_recv, rs_send, rs_recv, keep_sem, give_send, give_recv, late_sem) = refs[4:25]
    late_copies = [pltpu.make_async_copy(src, pick_ref.at[at], late_sem.at[at]) for at, src in enumerate((x_own_ref, dense_ref))]
    if last_layer:
        part_ref = gx_ref.at[0]
        land_ref, land_send, land_recv = refs[25:]
    n_src, _, dim = whole_ref.shape
    own = n_src // CHIPS
    n_group = xo_ref.shape[0] // GROUP
    n_first = 2 * n_group
    n_step = 3 * n_group
    half = dim // CHIPS
    piece = half // CORES
    step = pl.program_id(0)
    ix, ic, iy = position()
    cols = pl.ds(pl.multiple_of(ix * half, half), half)
    u_ref, dy_ref = (whole_ref, peer_ref) if last_layer else (peer_ref, whole_ref)
    outs = (gg_ref, gu_ref, gd_ref)
    spread = spreader(mine_ref, peer_ref, (ag_send, ag_recv))
    add_up = adder(p_ref, rs_ref, (rs_send, rs_recv))

    def land_copy(layer, hop):
        goal = target(hop)
        rows = dim // 8
        src = (part_ref, other_ref)[layer]
        at = pl.ds(pl.multiple_of(rank_of(goal['x'], goal['c'], goal['y']) * rows, rows), rows)
        return pltpu.make_async_remote_copy(src.at[at, :], land_ref.at[layer, hop], land_send.at[layer, hop],
                                            land_recv.at[layer, hop], device_id=goal, device_id_type=MESH)

    def land_sum(layer, out_ref):
        rows = dim // 8
        at = pl.ds(pl.multiple_of(rank_of(ix, ic, iy) * rows, rows), rows)
        total = (part_ref, other_ref)[layer][at, :].astype(F32)
        for hop in range(1, 8):
            land_copy(layer, hop).wait_recv()
            total += land_ref[layer, hop].astype(F32)
        out_ref[...] = total.astype(BF16)

    def store_copies(group, moved):
        buf = lax.rem(group, 2)
        rows = pl.ds(ic * n_group * GROUP + group * GROUP, GROUP)
        for kind in range(3):
            dst = outs[kind].at[rows]
            if moved:
                yield pltpu.make_async_remote_copy(
                    stage_ref.at[buf, 1 - ic, kind], dst, give_send.at[buf, kind], give_recv.at[group, kind],
                    device_id={'c': 1 - ic}, device_id_type=MESH)
            else:
                yield pltpu.make_async_copy(stage_ref.at[buf, ic, kind], dst, keep_sem.at[buf, kind])

    def store_start(group):
        for moved in (True, False):
            for copy in store_copies(group, moved):
                copy.start()

    def store_wait(group):
        for copy in store_copies(group, True):
            copy.wait_send()
        for copy in store_copies(group, False):
            copy.wait()

    def pull(src, group, at, keep):
        pick, gate = select_rows(rank_ref, gate_ref, group, src)
        if keep:
            pick_ref[at] = pick
        x_rows = matmul(pick, u_ref[src]).astype(BF16)
        d_rows = (matmul(pick, dy_ref[src]) * gate).astype(BF16)
        for exp in range(GROUP):
            x_ref[exp, at * CAP:(at + 1) * CAP, :] = x_rows[exp * CAP:(exp + 1) * CAP]
            d_ref[exp, at * CAP:(at + 1) * CAP, :] = d_rows[exp * CAP:(exp + 1) * CAP]

    def hidden_pre(x_rows, d_rows, exp):
        ff = wg_ref.shape[1]
        both = matmul(x_rows, side_by_side(wg_ref[exp], wu_ref[exp]), 1, 1)
        return both[:, :ff], both[:, LANES:LANES + ff], matmul(d_rows, wd_ref[exp], 1, 1)

    def hidden_grads(a_pre, b_pre, back):
        sigma = jax.nn.sigmoid(a_pre)
        silu = a_pre * sigma
        grad_hidden = back.astype(BF16).astype(F32)
        grad_a = (grad_hidden * b_pre * sigma * (1.0 + a_pre * (1.0 - sigma))).astype(BF16)
        return (silu * b_pre).astype(BF16), grad_a, (grad_hidden * silu).astype(BF16)

    @at_step(0)
    def _():
        greet(last_layer)
        for at in (0, 3, 1):
            spread(at).start()
        if last_layer:
            for hop in range(1, 8):
                land_copy(1, hop).start()
        peer_ref[rank_of(ix, ic, iy)] = mine_ref[...]
        p_ref[...] = jnp.zeros_like(p_ref)
        spread(3).wait_recv()

    @at_step(n_group - 1)
    def _():
        spread(0).wait_recv()
        spread(4).start()
        spread(2).start()

    @at_step(n_group)
    def _():
        spread(4).wait_recv()

    @at_step(n_group + n_group // 2)
    def _():
        spread(1).wait_recv()
        spread(5).start()

    @at_step(n_first - 1)
    def _():
        spread(2).wait_recv()
        spread(6).start()

    @pl.when(step < n_first)
    def _():
        group = lax.rem(step, n_group)
        late = lax.div(step, n_group)
        y_now = jnp.where(late == 1, 1 - iy, iy)
        base = group * GROUP
        rows = pl.ds(pl.multiple_of(late * CORES * CAP, CORES * CAP), CORES * CAP)

        for core in range(CORES):
            pull(rank_of(ix, core, y_now), group, core, True)

        near = CORES * CAP
        pre = {}
        for tick in range(GROUP + 2):
            if tick < GROUP:
                pre[tick] = hidden_pre(x_ref[tick, :near, :], d_ref[tick, :near, :], tick)
            if 0 < tick <= GROUP:
                exp = tick - 1
                hidden, grad_a, grad_b = hidden_grads(*pre.pop(exp))
                xo_ref[base + exp, rows, :] = x_ref[exp, :near, cols]
                do_ref[base + exp, rows, :] = d_ref[exp, :near, cols]
                h_ref[base + exp, rows, :] = hidden
                ga_ref[base + exp, rows, :] = grad_a
                gb_ref[base + exp, rows, :] = grad_b
                pre[exp, 1] = None
            if tick > 1:
                exp = tick - 2
                grad_x = (matmul(ga_ref[base + exp, rows, :], wg_ref[exp]) + matmul(gb_ref[base + exp, rows, :], wu_ref[exp])).astype(BF16)
                at = slice(exp * CAP, (exp + 1) * CAP)
                for core in range(CORES):
                    gx_ref[core, at, :] = grad_x[core * CAP:(core + 1) * CAP]

        for core in range(CORES):
            p_ref[core * 2 + y_now] += matmul(pick_ref[core], gx_ref[core], 0, 0)

    @at_step(n_first)
    def _():
        add_up(0).start()
        add_up(1).start()
        spread(5).wait_recv()
        spread(6).wait_recv()
        for copy in late_copies:
            copy.start()

    @pl.when(step >= n_first)
    def _():
        group = step - n_first

        @pl.when(group >= 2)
        def _():
            store_wait(group - 2)

        @pl.when(group >= 1)
        def _():
            store_start(group - 1)

        for src in range(own):
            pull((1 - ix) * own + src, group, src, False)

        @at_step(n_first)
        def _():
            add_up(0).wait_recv()
            p_ref[ic * 2 + 1 - iy] += rs_ref[0]
            add_up(2).start()

        @at_step(n_step - 1)
        def _():
            for copy in late_copies:
                copy.wait()
            add_up(1).wait_recv()
            add_up(2).wait_recv()
            total = p_ref[ic * 2 + iy] + rs_ref[1] + rs_ref[2]
            grad = (grad_own_ref[...].astype(F32) + total).astype(BF16)
            part_ref[...] = matmul(pick_ref[0], grad, 0, 0).astype(BF16)
            gx_out_ref[...] = (grad.astype(F32) + matmul(grad, pick_ref[1], 1, 1)).astype(BF16)
            if last_layer:
                for hop in range(1, 8):
                    land_copy(0, hop).start()

        buf = lax.rem(group, 2)

        pre = {}
        for tick in range(GROUP + 2):
            if tick < GROUP:
                pre[tick] = hidden_pre(x_ref[tick], d_ref[tick], tick)
            if 0 < tick <= GROUP:
                exp = tick - 1
                pre[exp, 1] = hidden_grads(*pre.pop(exp))
            if tick > 1:
                exp = tick - 2
                base = group * GROUP + exp
                hidden, grad_a, grad_b = pre.pop((exp, 1))
                x_own, x_far = xo_ref[base], x_ref[exp, :, cols]
                d_own, d_far = do_ref[base], d_ref[exp, :, cols]
                grads = (matmul(ga_ref[base], x_own, 0, 0) + matmul(grad_a, x_far, 0, 0),
                         matmul(gb_ref[base], x_own, 0, 0) + matmul(grad_b, x_far, 0, 0),
                         matmul(h_ref[base], d_own, 0, 0) + matmul(hidden, d_far, 0, 0))
                for kind in range(3):
                    for core in range(CORES):
                        stage_ref[buf, core, kind, exp] = grads[kind][:, core * piece:(core + 1) * piece].astype(BF16)

    @at_step(n_step - 1)
    def _():
        last = n_group - 1
        store_wait(last - 1)
        store_start(last)
        if last_layer:
            land_sum(1, two_ref)
            land_sum(0, one_ref)
            for layer in range(2):
                for hop in range(1, 8):
                    land_copy(layer, hop).wait_send()
        for at in range(7):
            spread(at).wait_send()
        for at in range(3):
            add_up(at).wait_send()
        store_wait(last)
        for group in range(n_group):
            for copy in store_copies(group, True):
                copy.wait_recv()


def fixed(*shape):
    return pl.BlockSpec(shape, lambda s: (0,) * len(shape), pipeline_mode=pl.Buffered(1))


def weight_spec(groups, ff, dim):
    return pl.BlockSpec((GROUP, ff, dim), lambda s: (lax.axis_index('c') * groups + lax.rem(s, groups), 0, 0))


def dma_sems(*shape):
    return pltpu.SemaphoreType.DMA(shape)


def sums_scratch(own, n_tok, dim):
    return [pltpu.VMEM((own, n_tok, dim), F32), pltpu.VMEM((3, n_tok, dim), F32)]


def layer_forward(tokens, grad, idx1, idx2, top1, top2, dense1, dense2, w_gate, w_up, w_down):
    n_tok, dim = tokens.shape
    top = idx1.shape[0]
    n_all, ff, _ = w_gate.shape
    n_exp = n_all // CORES
    n_src = 8
    own = n_src // CHIPS
    groups = n_exp // GROUP
    tall = weight_spec(groups, ff, dim)
    table = fixed(n_src, n_exp, n_tok)
    block = jax.ShapeDtypeStruct((n_tok, dim), BF16)
    every = jax.ShapeDtypeStruct((n_src, n_tok, dim), BF16)
    ranks = jax.ShapeDtypeStruct((n_src, n_exp, n_tok), jnp.int32)
    gates = jax.ShapeDtypeStruct((n_src, n_exp, n_tok), F32)
    anywhere = pl.BlockSpec(memory_space=pl.ANY)
    rows = CORES * CAP
    return pl.pallas_call(
        forward_kernel,
        out_shape=(block, block, every, every, ranks, gates, ranks, gates),
        grid_spec=pltpu.PrefetchScalarGridSpec(
            num_scalar_prefetch=0, grid=(2 * groups,),
            in_specs=[fixed(n_tok, dim)] * 2 + [fixed(top, n_tok)] * 4 + [fixed(dim, dim)] * 2 + [tall] * 3,
            out_specs=(fixed(n_tok, dim), fixed(n_tok, dim), anywhere, anywhere, table, table, table, table),
            scratch_shapes=[pltpu.VMEM((n_src, n_tok, dim), BF16)] * 3
            + [pltpu.VMEM((4 * top, n_tok), F32), pltpu.VMEM((n_src, 4 * top, n_tok), F32), pltpu.VMEM((n_tok, n_tok), BF16),
                            pltpu.VMEM((CORES, GROUP * CAP, n_tok), BF16), pltpu.VMEM((GROUP, rows, 128), F32),
                            pltpu.VMEM((GROUP, rows, dim), BF16), pltpu.VMEM((CORES, 3, GROUP * CAP, dim), BF16)]
            + sums_scratch(own, n_tok, dim)
            + [dma_sems(7)] * 6 + [dma_sems(3)] * 2 + [dma_sems(2)]),
        compiler_params=pltpu.CompilerParams(dimension_semantics=('arbitrary',), vmem_limit_bytes=62 << 20,
                                             collective_id=0, has_side_effects=True),
    )(tokens, grad, idx1, idx2, top1, top2, dense1, dense2, w_gate, w_up, w_down)


def layer_backward(last_layer, whole, mine, rank, gate, x_own, dense, w_gate, w_up, w_down, other):
    n_src, n_tok, dim = whole.shape
    n_all, ff, _ = w_gate.shape
    n_exp = rank.shape[1]
    own = n_src // CHIPS
    piece = dim // (CHIPS * CORES)
    groups = n_exp // GROUP
    kept = own * CAP
    tall = weight_spec(groups, ff, dim)
    table = fixed(n_src, n_exp, n_tok)
    block = fixed(n_tok, dim)
    square = fixed(dim, dim)
    slab = fixed(dim // 8, dim)
    grad_shape = jax.ShapeDtypeStruct((n_all, ff, piece), BF16)
    part_shape = jax.ShapeDtypeStruct((dim, dim), BF16)
    slab_shape = jax.ShapeDtypeStruct((dim // 8, dim), BF16)
    extra_shapes = (slab_shape, slab_shape) if last_layer else (part_shape,)
    extra_specs = (slab, slab) if last_layer else (square,)
    half = dim // CHIPS
    scratch = [pltpu.VMEM((n_src, n_tok, dim), BF16), pltpu.VMEM((n_exp, kept, half), BF16),
               pltpu.VMEM((n_exp, kept, half), BF16), pltpu.VMEM((n_exp, kept, ff), BF16),
               pltpu.VMEM((n_exp, kept, ff), BF16), pltpu.VMEM((n_exp, kept, ff), BF16),
               pltpu.VMEM((CORES, GROUP * CAP, n_tok), BF16), pltpu.VMEM((CORES, GROUP * CAP, dim), BF16)]
    scratch += sums_scratch(own, n_tok, dim)
    scratch += [pltpu.VMEM((GROUP, kept, dim), BF16), pltpu.VMEM((GROUP, kept, dim), BF16),
                pltpu.VMEM((2, CORES, 3, GROUP, ff, piece), BF16),
                dma_sems(7), dma_sems(7), dma_sems(3), dma_sems(3), dma_sems(2, 3), dma_sems(2, 3), dma_sems(groups, 3), dma_sems(2)]
    if last_layer:
        scratch += [pltpu.VMEM((2, 8, dim // 8, dim), BF16), dma_sems(2, 8), dma_sems(2, 8)]
    anywhere = pl.BlockSpec(memory_space=pl.ANY)
    return pl.pallas_call(
        functools.partial(layer_kernel, last_layer),
        out_shape=(jax.ShapeDtypeStruct((n_tok, dim), BF16),) + extra_shapes + (grad_shape,) * 3,
        grid_spec=pltpu.PrefetchScalarGridSpec(
            num_scalar_prefetch=0, grid=(3 * groups,),
            in_specs=[fixed(n_src, n_tok, dim), block, table, table, anywhere, anywhere, tall, tall, tall, square],
            out_specs=(block,) + extra_specs + (anywhere,) * 3,
            scratch_shapes=scratch),
        compiler_params=pltpu.CompilerParams(dimension_semantics=('arbitrary',), vmem_limit_bytes=67043328,
                                             collective_id=1 + int(last_layer), has_side_effects=True),
    )(whole, mine, rank, gate, x_own, dense, w_gate, w_up, w_down, other)


def settle_kernel(chunks, *refs):
    n = len(chunks)
    sources, outs, bufs = refs[:n], refs[n:2 * n], refs[2 * n:3 * n]
    in_sem, out_sem = refs[3 * n:]
    loads, stores = [], []
    for src, out, buf, count in zip(sources, outs, bufs, chunks):
        rows = src.shape[0] // count
        for at in range(count):
            here = pl.ds(at * rows, rows)
            loads.append(pltpu.make_async_copy(src.at[here], buf.at[here], in_sem.at[len(loads)]))
            stores.append(pltpu.make_async_copy(buf.at[here], out.at[here], out_sem.at[len(stores)]))
    for load in loads:
        load.start()
    for load, store in zip(loads, stores):
        load.wait()
        store.start()
    for store in stores:
        store.wait()


def settle(*arrays):
    chunks = tuple(8 if array.ndim == 3 else 1 for array in arrays)
    anywhere = pl.BlockSpec(memory_space=pl.ANY)
    return pl.pallas_call(
        functools.partial(settle_kernel, chunks),
        out_shape=tuple(jax.ShapeDtypeStruct(array.shape, array.dtype) for array in arrays),
        in_specs=[anywhere] * len(arrays), out_specs=(anywhere,) * len(arrays),
        scratch_shapes=[pltpu.VMEM(array.shape, array.dtype) for array in arrays] + [dma_sems(sum(chunks))] * 2,
        compiler_params=pltpu.CompilerParams(vmem_limit_bytes=67043328),
    )(*arrays)


def solution(mesh):
    fine = Mesh(mesh.devices.reshape(2, CHIPS, CORES), ('y', 'x', 'c'))
    tok_spec = P(ALL, None)
    exp_spec = P('y', None, None)
    layer_specs = (P(None, None), tok_spec, tok_spec, exp_spec, exp_spec, exp_spec)
    grad_specs = (P(ALL, None), P('y', ('x', 'c'), None), P('y', ('x', 'c'), None), P('y', None, ('x', 'c')))

    def local_step(tokens, dy_out, dense_w1, route_idx1, route_gate1, w_gate1, w_up1, w_down1, dense_w2, route_idx2, route_gate2, w_gate2, w_up2, w_down2):
        w_gate1, w_up1, w_gate2, w_up2 = (jnp.swapaxes(w, 1, 2) for w in (w_gate1, w_up1, w_gate2, w_up2))
        y_one, u_two, u_all, dy_all, rank1, gate1, rank2, gate2 = layer_forward(
            tokens, dy_out, route_idx1.T, route_idx2.T, route_gate1.T, route_gate2.T, dense_w1, dense_w2, w_gate1, w_up1, w_down1)
        grad_mid, part_two, *grads_two = layer_backward(
            False, dy_all, u_two, rank2, gate2, y_one, dense_w2, w_gate2, w_up2, w_down2, dy_out)
        grad_tok, dense_one, dense_two, *grads_one = layer_backward(
            True, u_all, grad_mid, rank1, gate1, tokens, dense_w1, w_gate1, w_up1, w_down1, part_two)
        (grad_tok, dense_one, gate_one, up_one, down_one, dense_two, gate_two, up_two, down_two) = settle(
            grad_tok, dense_one, *grads_one, dense_two, *grads_two)
        gate_one, up_one, gate_two, up_two = (jnp.swapaxes(g, 1, 2) for g in (gate_one, up_one, gate_two, up_two))
        return (grad_tok, dense_one, gate_one, up_one, down_one, dense_two, gate_two, up_two, down_two)

    return jax.shard_map(local_step, mesh=fine, in_specs=(tok_spec, tok_spec) + layer_specs + layer_specs,
                         out_specs=(tok_spec,) + grad_specs + grad_specs, check_vma=False)
```

```python
import functools

import jax
import jax.numpy as jnp
from jax import lax
from jax.experimental import pallas as pl
from jax.experimental.pallas import tpu as pltpu
from jax.sharding import Mesh, PartitionSpec as P

F32 = jnp.float32
BF16 = jnp.bfloat16
CAP = 64
GROUP = 8
LANES = 256
CORES = 2
CHIPS = 2
ALL = ('x', 'c', 'y')
MESH = pl.DeviceIdType.MESH
FLIPS = ((0, 0), (0, 0), (0, 1), (0, 0), (0, 1), (1, 0), (1, 1))
ROUTE = 'yxxcccc'


def matmul(lhs, rhs, lhs_dim=1, rhs_dim=0):
    return lax.dot_general(lhs, rhs, (((lhs_dim,), (rhs_dim,)), ((), ())), preferred_element_type=F32)


def position():
    return tuple(lax.axis_index(name) for name in ALL)


def send(src, dst, sems, at, axis):
    return pltpu.make_async_remote_copy(src, dst, sems[0].at[at], sems[1].at[at],
                                        device_id={axis: 1 - lax.axis_index(axis)}, device_id_type=MESH)


def spreader(mine_ref, peer_ref, sems):
    ix, ic, iy = position()

    def copy(at):
        flip_x, flip_y = FLIPS[at]
        x = 1 - ix if flip_x else ix
        y = 1 - iy if flip_y else iy
        block = peer_ref.at[(x * CORES + ic) * 2 + y]
        return send(block if flip_x or flip_y else mine_ref, block, sems, at, ROUTE[at])

    return copy


def adder(p_ref, rs_ref, sems):
    ix, ic, iy = position()

    def copy(at):
        part = ((1 - ic) * 2 + 1 - iy, (1 - ic) * 2 + iy, ic * 2 + 1 - iy)[at]
        return send(p_ref.at[part], rs_ref.at[at], sems, at, 'ccy'[at])

    return copy


def greet(everyone):
    barrier = pltpu.get_barrier_semaphore()
    if everyone:
        others = [target(hop) for hop in range(1, 8)]
    else:
        others = [{axis: 1 - lax.axis_index(axis)} for axis in ALL]
    for other in others:
        pl.semaphore_signal(barrier, inc=1, device_id=other, device_id_type=MESH)
    pl.semaphore_wait(barrier, len(others))


def rank_of(x, c, y):
    return (x * CORES + c) * 2 + y


def target(hop):
    goal = lax.rem(rank_of(*position()) + hop, 8)
    return {'x': lax.div(goal, 4), 'c': lax.rem(lax.div(goal, 2), 2), 'y': lax.rem(goal, 2)}


def weight_copies(sources, w_ref, sems, step, n_group):
    slot = lax.rem(step, 2)
    rows = pl.ds((lax.axis_index('c') * n_group + lax.rem(step, n_group)) * GROUP, GROUP)
    return [pltpu.make_async_copy(src.at[rows], w_ref.at[slot, kind], sems.at[slot, kind]) for kind, src in enumerate(sources)]


def next_weights(sources, w_ref, sems, n_group, n_step):
    step = pl.program_id(0)

    @pl.when(step + 1 < n_step)
    def _():
        for copy in weight_copies(sources, w_ref, sems, step + 1, n_group):
            copy.start()

    for copy in weight_copies(sources, w_ref, sems, step, n_group):
        copy.wait()


def at_step(number):
    return pl.when(pl.program_id(0) == number)


def side_by_side(first, second):
    pad = jnp.zeros((LANES - first.shape[0], first.shape[1]), first.dtype)
    return jnp.concatenate([first, pad, second, pad], axis=0)


def select_rows(rank_ref, gate_ref, group, src):
    n_tok = rank_ref.shape[-1]
    slot = lax.broadcasted_iota(jnp.int32, (CAP, n_tok), 0)
    picks, gates = [], []
    for exp in range(GROUP):
        row = pl.ds(group * GROUP + exp, 1)
        hit = slot == rank_ref[src, row, :]
        picks.append(jnp.where(hit, 1.0, 0.0).astype(BF16))
        gates.append(jnp.sum(jnp.where(hit, gate_ref[src, row, :], 0.0), axis=1, keepdims=True))
    return jnp.concatenate(picks, axis=0), jnp.concatenate(gates, axis=0)


def route_table(route_ref, before_ref, src, layer, rank_ref, gate_ref, n_exp):
    _, ic, iy = position()
    n_tok = route_ref.shape[-1]
    experts = ((iy * CORES + ic) * n_exp + lax.broadcasted_iota(jnp.int32, (n_exp, n_tok), 0)).astype(F32)
    member = jnp.zeros((n_exp, n_tok), F32)
    gates = jnp.zeros((n_exp, n_tok), F32)
    for top in range(8):
        hit = experts == route_ref[src, layer * 8 + top:layer * 8 + top + 1, :]
        member = jnp.where(hit, 1.0, member)
        gates = jnp.where(hit, route_ref[src, 16 + layer * 8 + top:17 + layer * 8 + top, :], gates)
    count = matmul(member.astype(BF16), before_ref[...])
    rank_ref[src] = jnp.where(member > 0.0, count, -1.0).astype(jnp.int32)
    gate_ref[src] = gates


def forward_kernel(tok_ref, grad_ref, idx1_ref, idx2_ref, top1_ref, top2_ref, mix_ref, dense_ref, wg_hbm, wu_hbm, wd_hbm,
                   y_ref, u_ref, uall_ref, dall_ref, rank1_ref, gate1_ref, rank2_ref, gate2_ref,
                   raw_ref, us_ref, ds_ref, routes_ref, route_ref, before_ref, pick_ref, row_ref, x_ref, part_ref, p_ref, rs_ref,
                   w_ref, w_sem, u_send, u_recv, d_send, d_recv, t_send, t_recv, rs_send, rs_recv, out_sem):
    n_exp, n_tok = rank1_ref.shape[1:]
    n_group = n_exp // GROUP
    step = pl.program_id(0)
    ix, ic, iy = position()
    me = rank_of(ix, ic, iy)
    spread_u = spreader(tok_ref, raw_ref, (u_send, u_recv))
    spread_d = spreader(grad_ref, ds_ref, (d_send, d_recv))
    spread_t = spreader(routes_ref, route_ref, (t_send, t_recv))
    add_up = adder(p_ref, rs_ref, (rs_send, rs_recv))
    stores = ((us_ref, uall_ref), (ds_ref, dall_ref))
    weights = (wg_hbm, wu_hbm, wd_hbm)
    wg_ref, wu_ref, wd_ref = (w_ref.at[lax.rem(step, 2), kind] for kind in range(3))

    def mixed(x):
        return (x.astype(F32) + matmul(x, mix_ref[...])).astype(BF16)

    def pass_on(copy, arrived, onward):
        copy(arrived).wait_recv()
        for at in onward:
            copy(at).start()

    @at_step(0)
    def _():
        for copy in weight_copies(weights, w_ref, w_sem, 0, n_group):
            copy.start()
        for at, part_in in enumerate((idx1_ref, idx2_ref, top1_ref, top2_ref)):
            routes_ref[at * 8:at * 8 + 8, :] = part_in[...].astype(F32)
        greet(False)
        for copy in (spread_t, spread_u):
            for at in (0, 3, 1):
                copy(at).start()
        us_ref[me] = mixed(tok_ref[...])
        ds_ref[me] = grad_ref[...]
        route_ref[me] = routes_ref[...]
        p_ref[...] = jnp.zeros_like(p_ref)
        before_ref[...] = jnp.where(lax.broadcasted_iota(jnp.int32, (n_tok, n_tok), 0)
                                    < lax.broadcasted_iota(jnp.int32, (n_tok, n_tok), 1), 1.0, 0.0).astype(BF16)
        pass_on(spread_t, 0, (4, 2))
        spread_u(3).wait_recv()
        us_ref[rank_of(ix, 1 - ic, iy)] = mixed(raw_ref[rank_of(ix, 1 - ic, iy)])
        spread_t(3).wait_recv()
        spread_t(4).wait_recv()

        @pl.loop(0, 4)
        def _(src):
            route_table(route_ref, before_ref, ix * 4 + src, 0, rank1_ref, gate1_ref, n_exp)

        pass_on(spread_u, 0, (4, 2))
        for at in (0, 3, 1):
            spread_d(at).start()
        us_ref[rank_of(ix, ic, 1 - iy)] = mixed(raw_ref[rank_of(ix, ic, 1 - iy)])
        spread_u(4).wait_recv()
        us_ref[rank_of(ix, 1 - ic, 1 - iy)] = mixed(raw_ref[rank_of(ix, 1 - ic, 1 - iy)])

    @at_step(n_group // 4)
    def _():
        pass_on(spread_t, 1, (5,))
        pass_on(spread_u, 1, (5,))

    @at_step(n_group // 2)
    def _():
        pass_on(spread_t, 2, (6,))
        pass_on(spread_u, 2, (6,))
        pass_on(spread_d, 0, (4, 2))

    @at_step(n_group - 1)
    def _():
        for copy in (spread_t, spread_u):
            copy(5).wait_recv()
            copy(6).wait_recv()

        @pl.loop(0, 4)
        def _(src):
            us_ref[(1 - ix) * 4 + src] = mixed(raw_ref[(1 - ix) * 4 + src])
            route_table(route_ref, before_ref, (1 - ix) * 4 + src, 0, rank1_ref, gate1_ref, n_exp)

        @pl.loop(0, 8)
        def _(src):
            route_table(route_ref, before_ref, src, 1, rank2_ref, gate2_ref, n_exp)

    @at_step(n_group)
    def _():
        add_up(0).start()
        pltpu.make_async_copy(us_ref, uall_ref, out_sem.at[0]).start()

    @at_step(n_group + n_group // 2)
    def _():
        pass_on(spread_d, 1, (5,))

    @at_step(2 * n_group - 2)
    def _():
        pass_on(spread_d, 2, (6,))

    @at_step(2 * n_group - 1)
    def _():
        for at in (3, 4, 5, 6):
            spread_d(at).wait_recv()
        pltpu.make_async_copy(ds_ref, dall_ref, out_sem.at[1]).start()

    next_weights(weights, w_ref, w_sem, n_group, 2 * n_group)
    group = lax.rem(step, n_group)
    far = 1 - lax.div(step, n_group)
    y_now = jnp.where(far == 1, 1 - iy, iy)

    for core in range(CORES):
        src = rank_of(ix, core, y_now)
        pick, gate = select_rows(rank1_ref, gate1_ref, group, src)
        pick_ref[core] = pick
        rows = matmul(pick, us_ref[src]).astype(BF16)
        at = slice(core * CAP, (core + 1) * CAP)
        for exp in range(GROUP):
            x_ref[exp, at, :] = rows[exp * CAP:(exp + 1) * CAP]
            row_ref[exp, at, :] = jnp.broadcast_to(gate[exp * CAP:(exp + 1) * CAP], (CAP, 128))

    @at_step(n_group)
    def _():
        add_up(0).wait_recv()
        p_ref[ic * 2 + 1 - iy] += rs_ref[0]
        add_up(2).start()

    ff = wg_ref.shape[1]
    pre = {}
    for tick in range(GROUP + 2):
        if tick < GROUP:
            pre[tick] = matmul(x_ref[tick], side_by_side(wg_ref[tick], wu_ref[tick]), 1, 1)
        if 0 < tick <= GROUP:
            both = pre.pop(tick - 1)
            a_pre, b_pre = both[:, :ff], both[:, LANES:LANES + ff]
            pre[tick - 1, 1] = (a_pre * jax.nn.sigmoid(a_pre) * b_pre).astype(BF16)
        if tick > 1:
            exp = tick - 2
            out = matmul(pre.pop((exp, 1)), wd_ref[exp]).astype(BF16).astype(F32) * row_ref[exp][:, :1]
            high = out.astype(BF16)
            rest = out - high.astype(F32)
            mid = rest.astype(BF16)
            low = (rest - mid.astype(F32)).astype(BF16)
            at = slice(exp * CAP, (exp + 1) * CAP)
            for core in range(CORES):
                here = slice(core * CAP, (core + 1) * CAP)
                part_ref[core, 0, at, :] = high[here]
                part_ref[core, 1, at, :] = mid[here]
                part_ref[core, 2, at, :] = low[here]

    for core in range(CORES):
        pick = pick_ref[core]
        total = matmul(pick, part_ref[core, 0], 0, 0)
        total += matmul(pick, part_ref[core, 1], 0, 0) + matmul(pick, part_ref[core, 2], 0, 0)
        p_ref[core * 2 + y_now] += total

    @at_step(2 * n_group - 1)
    def _():
        add_up(1).start()
        add_up(1).wait_recv()
        add_up(2).wait_recv()
        y_own = (us_ref[me].astype(F32) + (p_ref[ic * 2 + iy] + rs_ref[1] + rs_ref[2])).astype(BF16)
        y_ref[...] = y_own
        u_ref[...] = (y_own.astype(F32) + matmul(y_own, dense_ref[...])).astype(BF16)
        for copy in (spread_u, spread_d, spread_t):
            for at in range(7):
                copy(at).wait_send()
        for at in range(3):
            add_up(at).wait_send()
        for at in range(2):
            pltpu.make_async_copy(*stores[at], out_sem.at[at]).wait()


def layer_kernel(last_layer, *refs):
    refs = list(refs)
    whole_hbm, mine_ref, rank_hbm, gate_hbm, x_own_ref, dense_ref, *weights, other_ref = refs[:10]
    del refs[:10]
    grad_own_ref = mine_ref if last_layer else other_ref
    if last_layer:
        one_ref, two_ref = refs[1:3]
        del refs[1:3]
    else:
        part_ref = refs.pop(1)
    gx_out_ref, gg_ref, gu_ref, gd_ref = refs[:4]
    (peer_ref, xo_ref, do_ref, h_ref, ga_ref, gb_ref, pick_ref, gx_ref, p_ref, rs_ref, x_ref, d_ref, stage_ref,
     ag_send, ag_recv, rs_send, rs_recv, keep_sem, give_send, give_recv, late_sem,
     whole_ref, rank_ref, gate_ref, w_ref, w_sem, load_sem) = refs[4:31]
    late_copies = [pltpu.make_async_copy(src, pick_ref.at[at], late_sem.at[at]) for at, src in enumerate((x_own_ref, dense_ref))]
    if last_layer:
        part_ref = gx_ref.at[0]
        land_ref, land_send, land_recv = refs[31:]
    n_src, _, dim = whole_ref.shape
    own = n_src // CHIPS
    n_group = xo_ref.shape[0] // GROUP
    n_first = 2 * n_group
    n_step = 3 * n_group
    half = dim // CHIPS
    piece = half // CORES
    step = pl.program_id(0)
    ix, ic, iy = position()
    cols = pl.ds(pl.multiple_of(ix * half, half), half)
    wg_ref, wu_ref, wd_ref = (w_ref.at[lax.rem(step, 2), kind] for kind in range(3))
    loads = [pltpu.make_async_copy(src, dst, load_sem.at[at]) for at, (src, dst) in enumerate(
        ((rank_hbm, rank_ref), (gate_hbm, gate_ref), (whole_hbm, whole_ref)))]
    u_ref, dy_ref = (whole_ref, peer_ref) if last_layer else (peer_ref, whole_ref)
    outs = (gg_ref, gu_ref, gd_ref)
    spread = spreader(mine_ref, peer_ref, (ag_send, ag_recv))
    add_up = adder(p_ref, rs_ref, (rs_send, rs_recv))

    def land_copy(layer, hop):
        goal = target(hop)
        rows = dim // 8
        src = (part_ref, other_ref)[layer]
        at = pl.ds(pl.multiple_of(rank_of(goal['x'], goal['c'], goal['y']) * rows, rows), rows)
        return pltpu.make_async_remote_copy(src.at[at, :], land_ref.at[layer, hop], land_send.at[layer, hop],
                                            land_recv.at[layer, hop], device_id=goal, device_id_type=MESH)

    def land_sum(layer, out_ref):
        rows = dim // 8
        at = pl.ds(pl.multiple_of(rank_of(ix, ic, iy) * rows, rows), rows)
        total = (part_ref, other_ref)[layer][at, :].astype(F32)
        for hop in range(1, 8):
            land_copy(layer, hop).wait_recv()
            total += land_ref[layer, hop].astype(F32)
        out_ref[...] = total.astype(BF16)

    def store_copies(group, moved):
        buf = lax.rem(group, 2)
        rows = pl.ds(ic * n_group * GROUP + group * GROUP, GROUP)
        for kind in range(3):
            dst = outs[kind].at[rows]
            if moved:
                yield pltpu.make_async_remote_copy(
                    stage_ref.at[buf, 1 - ic, kind], dst, give_send.at[buf, kind], give_recv.at[group, kind],
                    device_id={'c': 1 - ic}, device_id_type=MESH)
            else:
                yield pltpu.make_async_copy(stage_ref.at[buf, ic, kind], dst, keep_sem.at[buf, kind])

    def store_start(group):
        for moved in (True, False):
            for copy in store_copies(group, moved):
                copy.start()

    def store_wait(group):
        for copy in store_copies(group, True):
            copy.wait_send()
        for copy in store_copies(group, False):
            copy.wait()

    def pull(src, group, at, keep):
        pick, gate = select_rows(rank_ref, gate_ref, group, src)
        if keep:
            pick_ref[at] = pick
        x_rows = matmul(pick, u_ref[src]).astype(BF16)
        d_rows = (matmul(pick, dy_ref[src]) * gate).astype(BF16)
        for exp in range(GROUP):
            x_ref[exp, at * CAP:(at + 1) * CAP, :] = x_rows[exp * CAP:(exp + 1) * CAP]
            d_ref[exp, at * CAP:(at + 1) * CAP, :] = d_rows[exp * CAP:(exp + 1) * CAP]

    def hidden_pre(x_rows, d_rows, exp):
        ff = wg_ref.shape[1]
        both = matmul(x_rows, side_by_side(wg_ref[exp], wu_ref[exp]), 1, 1)
        return both[:, :ff], both[:, LANES:LANES + ff], matmul(d_rows, wd_ref[exp], 1, 1)

    def hidden_grads(a_pre, b_pre, back):
        sigma = jax.nn.sigmoid(a_pre)
        silu = a_pre * sigma
        grad_hidden = back.astype(BF16).astype(F32)
        grad_a = (grad_hidden * b_pre * sigma * (1.0 + a_pre * (1.0 - sigma))).astype(BF16)
        return (silu * b_pre).astype(BF16), grad_a, (grad_hidden * silu).astype(BF16)

    @at_step(0)
    def _():
        for copy in loads + weight_copies(weights, w_ref, w_sem, 0, n_group):
            copy.start()
        greet(last_layer)
        for at in (0, 3, 1):
            spread(at).start()
        if last_layer:
            for hop in range(1, 8):
                land_copy(1, hop).start()
        peer_ref[rank_of(ix, ic, iy)] = mine_ref[...]
        p_ref[...] = jnp.zeros_like(p_ref)
        for copy in loads:
            copy.wait()
        spread(3).wait_recv()

    next_weights(weights, w_ref, w_sem, n_group, n_step)

    @at_step(n_group - 1)
    def _():
        spread(0).wait_recv()
        spread(4).start()
        spread(2).start()

    @at_step(n_group)
    def _():
        spread(4).wait_recv()

    @at_step(n_group + n_group // 2)
    def _():
        spread(1).wait_recv()
        spread(5).start()

    @at_step(n_first - 1)
    def _():
        spread(2).wait_recv()
        spread(6).start()

    @pl.when(step < n_first)
    def _():
        group = lax.rem(step, n_group)
        late = lax.div(step, n_group)
        y_now = jnp.where(late == 1, 1 - iy, iy)
        base = group * GROUP
        rows = pl.ds(pl.multiple_of(late * CORES * CAP, CORES * CAP), CORES * CAP)

        for core in range(CORES):
            pull(rank_of(ix, core, y_now), group, core, True)

        near = CORES * CAP
        pre = {}
        for tick in range(GROUP + 2):
            if tick < GROUP:
                pre[tick] = hidden_pre(x_ref[tick, :near, :], d_ref[tick, :near, :], tick)
            if 0 < tick <= GROUP:
                exp = tick - 1
                hidden, grad_a, grad_b = hidden_grads(*pre.pop(exp))
                xo_ref[base + exp, rows, :] = x_ref[exp, :near, cols]
                do_ref[base + exp, rows, :] = d_ref[exp, :near, cols]
                h_ref[base + exp, rows, :] = hidden
                ga_ref[base + exp, rows, :] = grad_a
                gb_ref[base + exp, rows, :] = grad_b
                pre[exp, 1] = None
            if tick > 1:
                exp = tick - 2
                grad_x = (matmul(ga_ref[base + exp, rows, :], wg_ref[exp]) + matmul(gb_ref[base + exp, rows, :], wu_ref[exp])).astype(BF16)
                at = slice(exp * CAP, (exp + 1) * CAP)
                for core in range(CORES):
                    gx_ref[core, at, :] = grad_x[core * CAP:(core + 1) * CAP]

        for core in range(CORES):
            p_ref[core * 2 + y_now] += matmul(pick_ref[core], gx_ref[core], 0, 0)

    @at_step(n_first)
    def _():
        add_up(0).start()
        add_up(1).start()
        spread(5).wait_recv()
        spread(6).wait_recv()
        for copy in late_copies:
            copy.start()

    @pl.when(step >= n_first)
    def _():
        group = step - n_first

        @pl.when(group >= 2)
        def _():
            store_wait(group - 2)

        @pl.when(group >= 1)
        def _():
            store_start(group - 1)

        for src in range(own):
            pull((1 - ix) * own + src, group, src, False)

        @at_step(n_first)
        def _():
            add_up(0).wait_recv()
            p_ref[ic * 2 + 1 - iy] += rs_ref[0]
            add_up(2).start()

        @at_step(n_step - 1)
        def _():
            for copy in late_copies:
                copy.wait()
            add_up(1).wait_recv()
            add_up(2).wait_recv()
            total = p_ref[ic * 2 + iy] + rs_ref[1] + rs_ref[2]
            grad = (grad_own_ref[...].astype(F32) + total).astype(BF16)
            part_ref[...] = matmul(pick_ref[0], grad, 0, 0).astype(BF16)
            gx_out_ref[...] = (grad.astype(F32) + matmul(grad, pick_ref[1], 1, 1)).astype(BF16)
            if last_layer:
                for hop in range(1, 8):
                    land_copy(0, hop).start()

        buf = lax.rem(group, 2)

        pre = {}
        for tick in range(GROUP + 2):
            if tick < GROUP:
                pre[tick] = hidden_pre(x_ref[tick], d_ref[tick], tick)
            if 0 < tick <= GROUP:
                exp = tick - 1
                pre[exp, 1] = hidden_grads(*pre.pop(exp))
            if tick > 1:
                exp = tick - 2
                base = group * GROUP + exp
                hidden, grad_a, grad_b = pre.pop((exp, 1))
                x_own, x_far = xo_ref[base], x_ref[exp, :, cols]
                d_own, d_far = do_ref[base], d_ref[exp, :, cols]
                grads = (matmul(ga_ref[base], x_own, 0, 0) + matmul(grad_a, x_far, 0, 0),
                         matmul(gb_ref[base], x_own, 0, 0) + matmul(grad_b, x_far, 0, 0),
                         matmul(h_ref[base], d_own, 0, 0) + matmul(hidden, d_far, 0, 0))
                for kind in range(3):
                    for core in range(CORES):
                        stage_ref[buf, core, kind, exp] = grads[kind][:, core * piece:(core + 1) * piece].astype(BF16)

    @at_step(n_step - 1)
    def _():
        last = n_group - 1
        store_wait(last - 1)
        store_start(last)
        if last_layer:
            land_sum(1, two_ref)
            land_sum(0, one_ref)
            for layer in range(2):
                for hop in range(1, 8):
                    land_copy(layer, hop).wait_send()
        for at in range(7):
            spread(at).wait_send()
        for at in range(3):
            add_up(at).wait_send()
        store_wait(last)
        for group in range(n_group):
            for copy in store_copies(group, True):
                copy.wait_recv()


def fixed(*shape):
    return pl.BlockSpec(shape, lambda s: (0,) * len(shape), pipeline_mode=pl.Buffered(1))


def dma_sems(*shape):
    return pltpu.SemaphoreType.DMA(shape)


def sums_scratch(own, n_tok, dim):
    return [pltpu.VMEM((own, n_tok, dim), F32), pltpu.VMEM((3, n_tok, dim), F32)]


def layer_forward(tokens, grad, idx1, idx2, top1, top2, dense1, dense2, w_gate, w_up, w_down):
    n_tok, dim = tokens.shape
    top = idx1.shape[0]
    n_all, ff, _ = w_gate.shape
    n_exp = n_all // CORES
    n_src = 8
    own = n_src // CHIPS
    groups = n_exp // GROUP
    table = fixed(n_src, n_exp, n_tok)
    block = jax.ShapeDtypeStruct((n_tok, dim), BF16)
    every = jax.ShapeDtypeStruct((n_src, n_tok, dim), BF16)
    ranks = jax.ShapeDtypeStruct((n_src, n_exp, n_tok), jnp.int32)
    gates = jax.ShapeDtypeStruct((n_src, n_exp, n_tok), F32)
    anywhere = pl.BlockSpec(memory_space=pl.ANY)
    rows = CORES * CAP
    return pl.pallas_call(
        forward_kernel,
        out_shape=(block, block, every, every, ranks, gates, ranks, gates),
        grid_spec=pltpu.PrefetchScalarGridSpec(
            num_scalar_prefetch=0, grid=(2 * groups,),
            in_specs=[fixed(n_tok, dim)] * 2 + [fixed(top, n_tok)] * 4 + [fixed(dim, dim)] * 2 + [anywhere] * 3,
            out_specs=(fixed(n_tok, dim), fixed(n_tok, dim), anywhere, anywhere, table, table, table, table),
            scratch_shapes=[pltpu.VMEM((n_src, n_tok, dim), BF16)] * 3
            + [pltpu.VMEM((4 * top, n_tok), F32), pltpu.VMEM((n_src, 4 * top, n_tok), F32), pltpu.VMEM((n_tok, n_tok), BF16),
                            pltpu.VMEM((CORES, GROUP * CAP, n_tok), BF16), pltpu.VMEM((GROUP, rows, 128), F32),
                            pltpu.VMEM((GROUP, rows, dim), BF16), pltpu.VMEM((CORES, 3, GROUP * CAP, dim), BF16)]
            + sums_scratch(own, n_tok, dim)
            + [pltpu.VMEM((2, 3, GROUP, ff, dim), BF16), dma_sems(2, 3)]
            + [dma_sems(7)] * 6 + [dma_sems(3)] * 2 + [dma_sems(2)]),
        compiler_params=pltpu.CompilerParams(dimension_semantics=('arbitrary',), vmem_limit_bytes=62 << 20,
                                             collective_id=0, has_side_effects=True),
    )(tokens, grad, idx1, idx2, top1, top2, dense1, dense2, w_gate, w_up, w_down)


def layer_backward(last_layer, whole, mine, rank, gate, x_own, dense, w_gate, w_up, w_down, other):
    n_src, n_tok, dim = whole.shape
    n_all, ff, _ = w_gate.shape
    n_exp = rank.shape[1]
    own = n_src // CHIPS
    piece = dim // (CHIPS * CORES)
    groups = n_exp // GROUP
    kept = own * CAP
    block = fixed(n_tok, dim)
    square = fixed(dim, dim)
    slab = fixed(dim // 8, dim)
    grad_shape = jax.ShapeDtypeStruct((n_all, ff, piece), BF16)
    part_shape = jax.ShapeDtypeStruct((dim, dim), BF16)
    slab_shape = jax.ShapeDtypeStruct((dim // 8, dim), BF16)
    extra_shapes = (slab_shape, slab_shape) if last_layer else (part_shape,)
    extra_specs = (slab, slab) if last_layer else (square,)
    half = dim // CHIPS
    scratch = [pltpu.VMEM((n_src, n_tok, dim), BF16), pltpu.VMEM((n_exp, kept, half), BF16),
               pltpu.VMEM((n_exp, kept, half), BF16), pltpu.VMEM((n_exp, kept, ff), BF16),
               pltpu.VMEM((n_exp, kept, ff), BF16), pltpu.VMEM((n_exp, kept, ff), BF16),
               pltpu.VMEM((CORES, GROUP * CAP, n_tok), BF16), pltpu.VMEM((CORES, GROUP * CAP, dim), BF16)]
    scratch += sums_scratch(own, n_tok, dim)
    scratch += [pltpu.VMEM((GROUP, kept, dim), BF16), pltpu.VMEM((GROUP, kept, dim), BF16),
                pltpu.VMEM((2, CORES, 3, GROUP, ff, piece), BF16),
                dma_sems(7), dma_sems(7), dma_sems(3), dma_sems(3), dma_sems(2, 3), dma_sems(2, 3), dma_sems(groups, 3), dma_sems(2),
                pltpu.VMEM((n_src, n_tok, dim), BF16), pltpu.VMEM(rank.shape, rank.dtype), pltpu.VMEM(gate.shape, gate.dtype),
                pltpu.VMEM((2, 3, GROUP, ff, dim), BF16), dma_sems(2, 3), dma_sems(3)]
    if last_layer:
        scratch += [pltpu.VMEM((2, 8, dim // 8, dim), BF16), dma_sems(2, 8), dma_sems(2, 8)]
    anywhere = pl.BlockSpec(memory_space=pl.ANY)
    return pl.pallas_call(
        functools.partial(layer_kernel, last_layer),
        out_shape=(jax.ShapeDtypeStruct((n_tok, dim), BF16),) + extra_shapes + (grad_shape,) * 3,
        grid_spec=pltpu.PrefetchScalarGridSpec(
            num_scalar_prefetch=0, grid=(3 * groups,),
            in_specs=[anywhere, block] + [anywhere] * 7 + [square],
            out_specs=(block,) + extra_specs + (anywhere,) * 3,
            scratch_shapes=scratch),
        compiler_params=pltpu.CompilerParams(dimension_semantics=('arbitrary',), vmem_limit_bytes=67043328,
                                             collective_id=1 + int(last_layer), has_side_effects=True),
    )(whole, mine, rank, gate, x_own, dense, w_gate, w_up, w_down, other)


def settle_kernel(chunks, *refs):
    n = len(chunks)
    sources, outs, bufs = refs[:n], refs[n:2 * n], refs[2 * n:3 * n]
    in_sem, out_sem = refs[3 * n:]
    loads, stores = [], []
    for src, out, buf, count in zip(sources, outs, bufs, chunks):
        rows = src.shape[0] // count
        for at in range(count):
            here = pl.ds(at * rows, rows)
            loads.append(pltpu.make_async_copy(src.at[here], buf.at[here], in_sem.at[len(loads)]))
            stores.append(pltpu.make_async_copy(buf.at[here], out.at[here], out_sem.at[len(stores)]))
    for load in loads:
        load.start()
    for load, store in zip(loads, stores):
        load.wait()
        store.start()
    for store in stores:
        store.wait()


def settle(*arrays):
    chunks = tuple(8 if array.ndim == 3 else 1 for array in arrays)
    anywhere = pl.BlockSpec(memory_space=pl.ANY)
    return pl.pallas_call(
        functools.partial(settle_kernel, chunks),
        out_shape=tuple(jax.ShapeDtypeStruct(array.shape, array.dtype) for array in arrays),
        in_specs=[anywhere] * len(arrays), out_specs=(anywhere,) * len(arrays),
        scratch_shapes=[pltpu.VMEM(array.shape, array.dtype) for array in arrays] + [dma_sems(sum(chunks))] * 2,
        compiler_params=pltpu.CompilerParams(vmem_limit_bytes=67043328),
    )(*arrays)


def solution(mesh):
    fine = Mesh(mesh.devices.reshape(2, CHIPS, CORES), ('y', 'x', 'c'))
    tok_spec = P(ALL, None)
    exp_spec = P('y', None, None)
    layer_specs = (P(None, None), tok_spec, tok_spec, exp_spec, exp_spec, exp_spec)
    grad_specs = (P(ALL, None), P('y', ('x', 'c'), None), P('y', ('x', 'c'), None), P('y', None, ('x', 'c')))

    def local_step(tokens, dy_out, dense_w1, route_idx1, route_gate1, w_gate1, w_up1, w_down1, dense_w2, route_idx2, route_gate2, w_gate2, w_up2, w_down2):
        w_gate1, w_up1, w_gate2, w_up2 = (jnp.swapaxes(w, 1, 2) for w in (w_gate1, w_up1, w_gate2, w_up2))
        y_one, u_two, u_all, dy_all, rank1, gate1, rank2, gate2 = layer_forward(
            tokens, dy_out, route_idx1.T, route_idx2.T, route_gate1.T, route_gate2.T, dense_w1, dense_w2, w_gate1, w_up1, w_down1)
        grad_mid, part_two, *grads_two = layer_backward(
            False, dy_all, u_two, rank2, gate2, y_one, dense_w2, w_gate2, w_up2, w_down2, dy_out)
        grad_tok, dense_one, dense_two, *grads_one = layer_backward(
            True, u_all, grad_mid, rank1, gate1, tokens, dense_w1, w_gate1, w_up1, w_down1, part_two)
        (grad_tok, dense_one, gate_one, up_one, down_one, dense_two, gate_two, up_two, down_two) = settle(
            grad_tok, dense_one, *grads_one, dense_two, *grads_two)
        gate_one, up_one, gate_two, up_two = (jnp.swapaxes(g, 1, 2) for g in (gate_one, up_one, gate_two, up_two))
        return (grad_tok, dense_one, gate_one, up_one, down_one, dense_two, gate_two, up_two, down_two)

    return jax.shard_map(local_step, mesh=fine, in_specs=(tok_spec, tok_spec) + layer_specs + layer_specs,
                         out_specs=(tok_spec,) + grad_specs + grad_specs, check_vma=False)
```

```python
import functools

import jax
import jax.numpy as jnp
from jax import lax
from jax.experimental import pallas as pl
from jax.experimental.pallas import tpu as pltpu
from jax.sharding import Mesh, PartitionSpec as P

F32 = jnp.float32
BF16 = jnp.bfloat16
CAP = 64
GROUP = 8
LANES = 256
CORES = 2
CHIPS = 2
ALL = ('x', 'c', 'y')
MESH = pl.DeviceIdType.MESH
FLIPS = ((0, 0), (0, 0), (0, 1), (0, 0), (0, 1), (1, 0), (1, 1))
ROUTE = 'yxxcccc'


def matmul(lhs, rhs, lhs_dim=1, rhs_dim=0):
    return lax.dot_general(lhs, rhs, (((lhs_dim,), (rhs_dim,)), ((), ())), preferred_element_type=F32)


def position():
    return tuple(lax.axis_index(name) for name in ALL)


def send(src, dst, sems, at, axis):
    return pltpu.make_async_remote_copy(src, dst, sems[0].at[at], sems[1].at[at],
                                        device_id={axis: 1 - lax.axis_index(axis)}, device_id_type=MESH)


def spreader(mine_ref, peer_ref, sems):
    ix, ic, iy = position()

    def copy(at):
        flip_x, flip_y = FLIPS[at]
        x = 1 - ix if flip_x else ix
        y = 1 - iy if flip_y else iy
        block = peer_ref.at[(x * CORES + ic) * 2 + y]
        return send(block if flip_x or flip_y else mine_ref, block, sems, at, ROUTE[at])

    return copy


def adder(p_ref, rs_ref, sems):
    ix, ic, iy = position()

    def copy(at):
        part = ((1 - ic) * 2 + 1 - iy, (1 - ic) * 2 + iy, ic * 2 + 1 - iy)[at]
        return send(p_ref.at[part], rs_ref.at[at], sems, at, 'ccy'[at])

    return copy


def greet(everyone):
    barrier = pltpu.get_barrier_semaphore()
    if everyone:
        others = [target(hop) for hop in range(1, 8)]
    else:
        others = [{axis: 1 - lax.axis_index(axis)} for axis in ALL]
    for other in others:
        pl.semaphore_signal(barrier, inc=1, device_id=other, device_id_type=MESH)
    pl.semaphore_wait(barrier, len(others))


def rank_of(x, c, y):
    return (x * CORES + c) * 2 + y


def target(hop):
    goal = lax.rem(rank_of(*position()) + hop, 8)
    return {'x': lax.div(goal, 4), 'c': lax.rem(lax.div(goal, 2), 2), 'y': lax.rem(goal, 2)}


def weight_copies(sources, w_ref, sems, step, n_group):
    slot = lax.rem(step, 2)
    rows = pl.ds((lax.axis_index('c') * n_group + lax.rem(step, n_group)) * GROUP, GROUP)
    return [pltpu.make_async_copy(src.at[rows], w_ref.at[slot, kind], sems.at[slot, kind]) for kind, src in enumerate(sources)]


def next_weights(sources, w_ref, sems, n_group, n_step):
    step = pl.program_id(0)

    @pl.when(step + 1 < n_step)
    def _():
        for copy in weight_copies(sources, w_ref, sems, step + 1, n_group):
            copy.start()

    for copy in weight_copies(sources, w_ref, sems, step, n_group):
        copy.wait()


def at_step(number):
    return pl.when(pl.program_id(0) == number)


def side_by_side(first, second):
    pad = jnp.zeros((LANES - first.shape[0], first.shape[1]), first.dtype)
    return jnp.concatenate([first, pad, second, pad], axis=0)


def select_rows(rank_ref, gate_ref, group, src):
    n_tok = rank_ref.shape[-1]
    slot = lax.broadcasted_iota(jnp.int32, (CAP, n_tok), 0)
    picks, gates = [], []
    for exp in range(GROUP):
        row = pl.ds(group * GROUP + exp, 1)
        hit = slot == rank_ref[src, row, :]
        picks.append(jnp.where(hit, 1.0, 0.0).astype(BF16))
        gates.append(jnp.sum(jnp.where(hit, gate_ref[src, row, :], 0.0), axis=1, keepdims=True))
    return jnp.concatenate(picks, axis=0), jnp.concatenate(gates, axis=0)


def route_table(route_ref, before_ref, src, layer, rank_ref, gate_ref, n_exp):
    _, ic, iy = position()
    n_tok = route_ref.shape[-1]
    experts = ((iy * CORES + ic) * n_exp + lax.broadcasted_iota(jnp.int32, (n_exp, n_tok), 0)).astype(F32)
    member = jnp.zeros((n_exp, n_tok), F32)
    gates = jnp.zeros((n_exp, n_tok), F32)
    for top in range(8):
        hit = experts == route_ref[src, layer * 8 + top:layer * 8 + top + 1, :]
        member = jnp.where(hit, 1.0, member)
        gates = jnp.where(hit, route_ref[src, 16 + layer * 8 + top:17 + layer * 8 + top, :], gates)
    count = matmul(member.astype(BF16), before_ref[...])
    rank_ref[src] = jnp.where(member > 0.0, count, -1.0).astype(jnp.int32)
    gate_ref[src] = gates


def forward_kernel(tok_ref, grad_ref, idx1_ref, idx2_ref, top1_ref, top2_ref, mix_ref, dense_ref, wg_hbm, wu_hbm, wd_hbm,
                   y_ref, u_ref, uall_ref, dall_ref, rank1_ref, gate1_ref, rank2_ref, gate2_ref,
                   raw_ref, us_ref, ds_ref, routes_ref, route_ref, before_ref, pick_ref, row_ref, x_ref, part_ref, p_ref, rs_ref,
                   w_ref, w_sem, u_send, u_recv, d_send, d_recv, t_send, t_recv, rs_send, rs_recv, out_sem):
    n_exp, n_tok = rank1_ref.shape[1:]
    n_group = n_exp // GROUP
    step = pl.program_id(0)
    ix, ic, iy = position()
    me = rank_of(ix, ic, iy)
    spread_u = spreader(tok_ref, raw_ref, (u_send, u_recv))
    spread_d = spreader(grad_ref, ds_ref, (d_send, d_recv))
    spread_t = spreader(routes_ref, route_ref, (t_send, t_recv))
    add_up = adder(p_ref, rs_ref, (rs_send, rs_recv))
    stores = ((us_ref, uall_ref), (ds_ref, dall_ref))
    weights = (wg_hbm, wu_hbm, wd_hbm)
    wg_ref, wu_ref, wd_ref = (w_ref.at[lax.rem(step, 2), kind] for kind in range(3))

    def mixed(x):
        return (x.astype(F32) + matmul(x, mix_ref[...])).astype(BF16)

    def pass_on(copy, arrived, onward):
        copy(arrived).wait_recv()
        for at in onward:
            copy(at).start()

    @at_step(0)
    def _():
        for copy in weight_copies(weights, w_ref, w_sem, 0, n_group):
            copy.start()
        for at, part_in in enumerate((idx1_ref, idx2_ref, top1_ref, top2_ref)):
            routes_ref[at * 8:at * 8 + 8, :] = part_in[...].astype(F32)
        greet(False)
        for copy in (spread_t, spread_u):
            for at in (0, 3, 1):
                copy(at).start()
        us_ref[me] = mixed(tok_ref[...])
        ds_ref[me] = grad_ref[...]
        route_ref[me] = routes_ref[...]
        p_ref[...] = jnp.zeros_like(p_ref)
        before_ref[...] = jnp.where(lax.broadcasted_iota(jnp.int32, (n_tok, n_tok), 0)
                                    < lax.broadcasted_iota(jnp.int32, (n_tok, n_tok), 1), 1.0, 0.0).astype(BF16)
        pass_on(spread_t, 0, (4, 2))
        spread_u(3).wait_recv()
        us_ref[rank_of(ix, 1 - ic, iy)] = mixed(raw_ref[rank_of(ix, 1 - ic, iy)])
        spread_t(3).wait_recv()
        spread_t(4).wait_recv()

        @pl.loop(0, 4)
        def _(src):
            route_table(route_ref, before_ref, ix * 4 + src, 0, rank1_ref, gate1_ref, n_exp)

        pass_on(spread_u, 0, (4, 2))
        for at in (0, 3, 1):
            spread_d(at).start()
        us_ref[rank_of(ix, ic, 1 - iy)] = mixed(raw_ref[rank_of(ix, ic, 1 - iy)])
        spread_u(4).wait_recv()
        us_ref[rank_of(ix, 1 - ic, 1 - iy)] = mixed(raw_ref[rank_of(ix, 1 - ic, 1 - iy)])

    @at_step(n_group // 4)
    def _():
        pass_on(spread_t, 1, (5,))
        pass_on(spread_u, 1, (5,))

    @at_step(n_group // 2)
    def _():
        pass_on(spread_t, 2, (6,))
        pass_on(spread_u, 2, (6,))
        pass_on(spread_d, 0, (4, 2))

    @at_step(n_group + 1)
    def _():
        for copy in (spread_t, spread_u):
            copy(5).wait_recv()
            copy(6).wait_recv()

        @pl.loop(0, 4)
        def _(src):
            us_ref[(1 - ix) * 4 + src] = mixed(raw_ref[(1 - ix) * 4 + src])
            route_table(route_ref, before_ref, (1 - ix) * 4 + src, 0, rank1_ref, gate1_ref, n_exp)

        @pl.loop(0, 8)
        def _(src):
            route_table(route_ref, before_ref, src, 1, rank2_ref, gate2_ref, n_exp)

    @at_step(n_group)
    def _():
        add_up(0).start()

    @at_step(n_group + n_group // 2)
    def _():
        pass_on(spread_d, 1, (5,))

    @at_step(2 * n_group - 2)
    def _():
        pass_on(spread_d, 2, (6,))
        pltpu.make_async_copy(us_ref, uall_ref, out_sem.at[0]).start()

    @at_step(2 * n_group - 1)
    def _():
        for at in (3, 4, 5, 6):
            spread_d(at).wait_recv()
        pltpu.make_async_copy(ds_ref, dall_ref, out_sem.at[1]).start()

    next_weights(weights, w_ref, w_sem, n_group, 2 * n_group)
    group = lax.rem(step, n_group)
    far = 1 - lax.div(step, n_group)
    y_now = jnp.where(far == 1, 1 - iy, iy)

    for core in range(CORES):
        src = rank_of(ix, core, y_now)
        pick, gate = select_rows(rank1_ref, gate1_ref, group, src)
        pick_ref[core] = pick
        rows = matmul(pick, us_ref[src]).astype(BF16)
        at = slice(core * CAP, (core + 1) * CAP)
        for exp in range(GROUP):
            x_ref[exp, at, :] = rows[exp * CAP:(exp + 1) * CAP]
            row_ref[exp, at, :] = jnp.broadcast_to(gate[exp * CAP:(exp + 1) * CAP], (CAP, 128))

    @at_step(n_group)
    def _():
        add_up(0).wait_recv()
        p_ref[ic * 2 + 1 - iy] += rs_ref[0]
        add_up(2).start()

    ff = wg_ref.shape[1]
    pre = {}
    for tick in range(GROUP + 2):
        if tick < GROUP:
            pre[tick] = matmul(x_ref[tick], side_by_side(wg_ref[tick], wu_ref[tick]), 1, 1)
        if 0 < tick <= GROUP:
            both = pre.pop(tick - 1)
            a_pre, b_pre = both[:, :ff], both[:, LANES:LANES + ff]
            pre[tick - 1, 1] = (a_pre * jax.nn.sigmoid(a_pre) * b_pre).astype(BF16)
        if tick > 1:
            exp = tick - 2
            out = matmul(pre.pop((exp, 1)), wd_ref[exp]).astype(BF16).astype(F32) * row_ref[exp][:, :1]
            high = out.astype(BF16)
            rest = out - high.astype(F32)
            mid = rest.astype(BF16)
            low = (rest - mid.astype(F32)).astype(BF16)
            at = slice(exp * CAP, (exp + 1) * CAP)
            for core in range(CORES):
                here = slice(core * CAP, (core + 1) * CAP)
                part_ref[core, 0, at, :] = high[here]
                part_ref[core, 1, at, :] = mid[here]
                part_ref[core, 2, at, :] = low[here]

    for core in range(CORES):
        pick = pick_ref[core]
        total = matmul(pick, part_ref[core, 0], 0, 0)
        total += matmul(pick, part_ref[core, 1], 0, 0) + matmul(pick, part_ref[core, 2], 0, 0)
        p_ref[core * 2 + y_now] += total

    @at_step(2 * n_group - 1)
    def _():
        add_up(1).start()
        add_up(1).wait_recv()
        add_up(2).wait_recv()
        y_own = (us_ref[me].astype(F32) + (p_ref[ic * 2 + iy] + rs_ref[1] + rs_ref[2])).astype(BF16)
        y_ref[...] = y_own
        u_ref[...] = (y_own.astype(F32) + matmul(y_own, dense_ref[...])).astype(BF16)
        for copy in (spread_u, spread_d, spread_t):
            for at in range(7):
                copy(at).wait_send()
        for at in range(3):
            add_up(at).wait_send()
        for at in range(2):
            pltpu.make_async_copy(*stores[at], out_sem.at[at]).wait()


def layer_kernel(last_layer, *refs):
    refs = list(refs)
    whole_hbm, mine_ref, rank_hbm, gate_hbm, x_own_ref, dense_ref, *weights, other_ref = refs[:10]
    del refs[:10]
    grad_own_ref = mine_ref if last_layer else other_ref
    if last_layer:
        one_ref, two_ref = refs[1:3]
        del refs[1:3]
    else:
        part_ref = refs.pop(1)
    gx_out_ref, gg_ref, gu_ref, gd_ref = refs[:4]
    (peer_ref, xo_ref, do_ref, h_ref, ga_ref, gb_ref, pick_ref, gx_ref, p_ref, rs_ref, x_ref, d_ref, stage_ref,
     ag_send, ag_recv, rs_send, rs_recv, keep_sem, give_send, give_recv, late_sem,
     whole_ref, rank_ref, gate_ref, w_ref, w_sem, load_sem) = refs[4:31]
    late_copies = [pltpu.make_async_copy(src, pick_ref.at[at], late_sem.at[at]) for at, src in enumerate((x_own_ref, dense_ref))]
    if last_layer:
        part_ref = gx_ref.at[0]
        land_ref, land_send, land_recv = refs[31:]
    n_src, _, dim = whole_ref.shape
    own = n_src // CHIPS
    n_group = xo_ref.shape[0] // GROUP
    n_first = 2 * n_group
    n_step = 3 * n_group
    half = dim // CHIPS
    piece = half // CORES
    step = pl.program_id(0)
    ix, ic, iy = position()
    cols = pl.ds(pl.multiple_of(ix * half, half), half)
    wg_ref, wu_ref, wd_ref = (w_ref.at[lax.rem(step, 2), kind] for kind in range(3))
    loads = [pltpu.make_async_copy(src, dst, load_sem.at[at]) for at, (src, dst) in enumerate(
        ((rank_hbm, rank_ref), (gate_hbm, gate_ref), (whole_hbm, whole_ref)))]
    u_ref, dy_ref = (whole_ref, peer_ref) if last_layer else (peer_ref, whole_ref)
    outs = (gg_ref, gu_ref, gd_ref)
    spread = spreader(mine_ref, peer_ref, (ag_send, ag_recv))
    add_up = adder(p_ref, rs_ref, (rs_send, rs_recv))

    def land_copy(layer, hop):
        goal = target(hop)
        rows = dim // 8
        src = (part_ref, other_ref)[layer]
        at = pl.ds(pl.multiple_of(rank_of(goal['x'], goal['c'], goal['y']) * rows, rows), rows)
        return pltpu.make_async_remote_copy(src.at[at, :], land_ref.at[layer, hop], land_send.at[layer, hop],
                                            land_recv.at[layer, hop], device_id=goal, device_id_type=MESH)

    def land_sum(layer, out_ref):
        rows = dim // 8
        at = pl.ds(pl.multiple_of(rank_of(ix, ic, iy) * rows, rows), rows)
        total = (part_ref, other_ref)[layer][at, :].astype(F32)
        for hop in range(1, 8):
            land_copy(layer, hop).wait_recv()
            total += land_ref[layer, hop].astype(F32)
        out_ref[...] = total.astype(BF16)

    def store_copies(group, moved):
        buf = lax.rem(group, 2)
        rows = pl.ds(ic * n_group * GROUP + group * GROUP, GROUP)
        for kind in range(3):
            dst = outs[kind].at[rows]
            if moved:
                yield pltpu.make_async_remote_copy(
                    stage_ref.at[buf, 1 - ic, kind], dst, give_send.at[buf, kind], give_recv.at[group, kind],
                    device_id={'c': 1 - ic}, device_id_type=MESH)
            else:
                yield pltpu.make_async_copy(stage_ref.at[buf, ic, kind], dst, keep_sem.at[buf, kind])

    def store_start(group):
        for moved in (True, False):
            for copy in store_copies(group, moved):
                copy.start()

    def store_wait(group):
        for copy in store_copies(group, True):
            copy.wait_send()
        for copy in store_copies(group, False):
            copy.wait()

    def pull(src, group, at, keep):
        pick, gate = select_rows(rank_ref, gate_ref, group, src)
        if keep:
            pick_ref[at] = pick
        x_rows = matmul(pick, u_ref[src]).astype(BF16)
        d_rows = (matmul(pick, dy_ref[src]) * gate).astype(BF16)
        for exp in range(GROUP):
            x_ref[exp, at * CAP:(at + 1) * CAP, :] = x_rows[exp * CAP:(exp + 1) * CAP]
            d_ref[exp, at * CAP:(at + 1) * CAP, :] = d_rows[exp * CAP:(exp + 1) * CAP]

    def hidden_pre(x_rows, d_rows, exp):
        ff = wg_ref.shape[1]
        both = matmul(x_rows, side_by_side(wg_ref[exp], wu_ref[exp]), 1, 1)
        return both[:, :ff], both[:, LANES:LANES + ff], matmul(d_rows, wd_ref[exp], 1, 1)

    def hidden_grads(a_pre, b_pre, back):
        sigma = jax.nn.sigmoid(a_pre)
        silu = a_pre * sigma
        grad_hidden = back.astype(BF16).astype(F32)
        grad_a = (grad_hidden * b_pre * sigma * (1.0 + a_pre * (1.0 - sigma))).astype(BF16)
        return (silu * b_pre).astype(BF16), grad_a, (grad_hidden * silu).astype(BF16)

    @at_step(0)
    def _():
        for copy in loads + weight_copies(weights, w_ref, w_sem, 0, n_group):
            copy.start()
        greet(last_layer)
        for at in (0, 3, 1):
            spread(at).start()
        if last_layer:
            for hop in range(1, 8):
                land_copy(1, hop).start()
        peer_ref[rank_of(ix, ic, iy)] = mine_ref[...]
        p_ref[...] = jnp.zeros_like(p_ref)
        for copy in loads:
            copy.wait()
        spread(3).wait_recv()

    next_weights(weights, w_ref, w_sem, n_group, n_step)

    @at_step(n_group - 1)
    def _():
        spread(0).wait_recv()
        spread(4).start()
        spread(2).start()

    @at_step(n_group)
    def _():
        spread(4).wait_recv()

    @at_step(n_group + n_group // 2)
    def _():
        spread(1).wait_recv()
        spread(5).start()

    @at_step(n_first - 1)
    def _():
        spread(2).wait_recv()
        spread(6).start()

    @pl.when(step < n_first)
    def _():
        group = lax.rem(step, n_group)
        late = lax.div(step, n_group)
        y_now = jnp.where(late == 1, 1 - iy, iy)
        base = group * GROUP
        rows = pl.ds(pl.multiple_of(late * CORES * CAP, CORES * CAP), CORES * CAP)

        for core in range(CORES):
            pull(rank_of(ix, core, y_now), group, core, True)

        near = CORES * CAP
        pre = {}
        for tick in range(GROUP + 2):
            if tick < GROUP:
                pre[tick] = hidden_pre(x_ref[tick, :near, :], d_ref[tick, :near, :], tick)
            if 0 < tick <= GROUP:
                exp = tick - 1
                hidden, grad_a, grad_b = hidden_grads(*pre.pop(exp))
                xo_ref[base + exp, rows, :] = x_ref[exp, :near, cols]
                do_ref[base + exp, rows, :] = d_ref[exp, :near, cols]
                h_ref[base + exp, rows, :] = hidden
                ga_ref[base + exp, rows, :] = grad_a
                gb_ref[base + exp, rows, :] = grad_b
                pre[exp, 1] = None
            if tick > 1:
                exp = tick - 2
                grad_x = (matmul(ga_ref[base + exp, rows, :], wg_ref[exp]) + matmul(gb_ref[base + exp, rows, :], wu_ref[exp])).astype(BF16)
                at = slice(exp * CAP, (exp + 1) * CAP)
                for core in range(CORES):
                    gx_ref[core, at, :] = grad_x[core * CAP:(core + 1) * CAP]

        for core in range(CORES):
            p_ref[core * 2 + y_now] += matmul(pick_ref[core], gx_ref[core], 0, 0)

    @at_step(n_first)
    def _():
        add_up(0).start()
        add_up(1).start()
        spread(5).wait_recv()
        spread(6).wait_recv()
        for copy in late_copies:
            copy.start()

    @pl.when(step >= n_first)
    def _():
        group = step - n_first

        @pl.when(group >= 2)
        def _():
            store_wait(group - 2)

        @pl.when(group >= 1)
        def _():
            store_start(group - 1)

        for src in range(own):
            pull((1 - ix) * own + src, group, src, False)

        @at_step(n_first)
        def _():
            add_up(0).wait_recv()
            p_ref[ic * 2 + 1 - iy] += rs_ref[0]
            add_up(2).start()

        @at_step(n_step - 1)
        def _():
            for copy in late_copies:
                copy.wait()
            add_up(1).wait_recv()
            add_up(2).wait_recv()
            total = p_ref[ic * 2 + iy] + rs_ref[1] + rs_ref[2]
            grad = (grad_own_ref[...].astype(F32) + total).astype(BF16)
            part_ref[...] = matmul(pick_ref[0], grad, 0, 0).astype(BF16)
            gx_out_ref[...] = (grad.astype(F32) + matmul(grad, pick_ref[1], 1, 1)).astype(BF16)
            if last_layer:
                for hop in range(1, 8):
                    land_copy(0, hop).start()

        buf = lax.rem(group, 2)

        pre = {}
        for tick in range(GROUP + 2):
            if tick < GROUP:
                pre[tick] = hidden_pre(x_ref[tick], d_ref[tick], tick)
            if 0 < tick <= GROUP:
                exp = tick - 1
                pre[exp, 1] = hidden_grads(*pre.pop(exp))
            if tick > 1:
                exp = tick - 2
                base = group * GROUP + exp
                hidden, grad_a, grad_b = pre.pop((exp, 1))
                x_own, x_far = xo_ref[base], x_ref[exp, :, cols]
                d_own, d_far = do_ref[base], d_ref[exp, :, cols]
                grads = (matmul(ga_ref[base], x_own, 0, 0) + matmul(grad_a, x_far, 0, 0),
                         matmul(gb_ref[base], x_own, 0, 0) + matmul(grad_b, x_far, 0, 0),
                         matmul(h_ref[base], d_own, 0, 0) + matmul(hidden, d_far, 0, 0))
                for kind in range(3):
                    for core in range(CORES):
                        stage_ref[buf, core, kind, exp] = grads[kind][:, core * piece:(core + 1) * piece].astype(BF16)

    @at_step(n_step - 1)
    def _():
        last = n_group - 1
        store_wait(last - 1)
        store_start(last)
        if last_layer:
            land_sum(1, two_ref)
            land_sum(0, one_ref)
            for layer in range(2):
                for hop in range(1, 8):
                    land_copy(layer, hop).wait_send()
        for at in range(7):
            spread(at).wait_send()
        for at in range(3):
            add_up(at).wait_send()
        store_wait(last)
        for group in range(n_group):
            for copy in store_copies(group, True):
                copy.wait_recv()


def fixed(*shape):
    return pl.BlockSpec(shape, lambda s: (0,) * len(shape), pipeline_mode=pl.Buffered(1))


def dma_sems(*shape):
    return pltpu.SemaphoreType.DMA(shape)


def sums_scratch(own, n_tok, dim):
    return [pltpu.VMEM((own, n_tok, dim), F32), pltpu.VMEM((3, n_tok, dim), F32)]


def layer_forward(tokens, grad, idx1, idx2, top1, top2, dense1, dense2, w_gate, w_up, w_down):
    n_tok, dim = tokens.shape
    top = idx1.shape[0]
    n_all, ff, _ = w_gate.shape
    n_exp = n_all // CORES
    n_src = 8
    own = n_src // CHIPS
    groups = n_exp // GROUP
    table = fixed(n_src, n_exp, n_tok)
    block = jax.ShapeDtypeStruct((n_tok, dim), BF16)
    every = jax.ShapeDtypeStruct((n_src, n_tok, dim), BF16)
    ranks = jax.ShapeDtypeStruct((n_src, n_exp, n_tok), jnp.int32)
    gates = jax.ShapeDtypeStruct((n_src, n_exp, n_tok), F32)
    anywhere = pl.BlockSpec(memory_space=pl.ANY)
    rows = CORES * CAP
    return pl.pallas_call(
        forward_kernel,
        out_shape=(block, block, every, every, ranks, gates, ranks, gates),
        grid_spec=pltpu.PrefetchScalarGridSpec(
            num_scalar_prefetch=0, grid=(2 * groups,),
            in_specs=[fixed(n_tok, dim)] * 2 + [fixed(top, n_tok)] * 4 + [fixed(dim, dim)] * 2 + [anywhere] * 3,
            out_specs=(fixed(n_tok, dim), fixed(n_tok, dim), anywhere, anywhere, table, table, table, table),
            scratch_shapes=[pltpu.VMEM((n_src, n_tok, dim), BF16)] * 3
            + [pltpu.VMEM((4 * top, n_tok), F32), pltpu.VMEM((n_src, 4 * top, n_tok), F32), pltpu.VMEM((n_tok, n_tok), BF16),
                            pltpu.VMEM((CORES, GROUP * CAP, n_tok), BF16), pltpu.VMEM((GROUP, rows, 128), F32),
                            pltpu.VMEM((GROUP, rows, dim), BF16), pltpu.VMEM((CORES, 3, GROUP * CAP, dim), BF16)]
            + sums_scratch(own, n_tok, dim)
            + [pltpu.VMEM((2, 3, GROUP, ff, dim), BF16), dma_sems(2, 3)]
            + [dma_sems(7)] * 6 + [dma_sems(3)] * 2 + [dma_sems(2)]),
        compiler_params=pltpu.CompilerParams(dimension_semantics=('arbitrary',), vmem_limit_bytes=62 << 20,
                                             collective_id=0, has_side_effects=True),
    )(tokens, grad, idx1, idx2, top1, top2, dense1, dense2, w_gate, w_up, w_down)


def layer_backward(last_layer, whole, mine, rank, gate, x_own, dense, w_gate, w_up, w_down, other):
    n_src, n_tok, dim = whole.shape
    n_all, ff, _ = w_gate.shape
    n_exp = rank.shape[1]
    own = n_src // CHIPS
    piece = dim // (CHIPS * CORES)
    groups = n_exp // GROUP
    kept = own * CAP
    block = fixed(n_tok, dim)
    square = fixed(dim, dim)
    slab = fixed(dim // 8, dim)
    grad_shape = jax.ShapeDtypeStruct((n_all, ff, piece), BF16)
    part_shape = jax.ShapeDtypeStruct((dim, dim), BF16)
    slab_shape = jax.ShapeDtypeStruct((dim // 8, dim), BF16)
    extra_shapes = (slab_shape, slab_shape) if last_layer else (part_shape,)
    extra_specs = (slab, slab) if last_layer else (square,)
    half = dim // CHIPS
    scratch = [pltpu.VMEM((n_src, n_tok, dim), BF16), pltpu.VMEM((n_exp, kept, half), BF16),
               pltpu.VMEM((n_exp, kept, half), BF16), pltpu.VMEM((n_exp, kept, ff), BF16),
               pltpu.VMEM((n_exp, kept, ff), BF16), pltpu.VMEM((n_exp, kept, ff), BF16),
               pltpu.VMEM((CORES, GROUP * CAP, n_tok), BF16), pltpu.VMEM((CORES, GROUP * CAP, dim), BF16)]
    scratch += sums_scratch(own, n_tok, dim)
    scratch += [pltpu.VMEM((GROUP, kept, dim), BF16), pltpu.VMEM((GROUP, kept, dim), BF16),
                pltpu.VMEM((2, CORES, 3, GROUP, ff, piece), BF16),
                dma_sems(7), dma_sems(7), dma_sems(3), dma_sems(3), dma_sems(2, 3), dma_sems(2, 3), dma_sems(groups, 3), dma_sems(2),
                pltpu.VMEM((n_src, n_tok, dim), BF16), pltpu.VMEM(rank.shape, rank.dtype), pltpu.VMEM(gate.shape, gate.dtype),
                pltpu.VMEM((2, 3, GROUP, ff, dim), BF16), dma_sems(2, 3), dma_sems(3)]
    if last_layer:
        scratch += [pltpu.VMEM((2, 8, dim // 8, dim), BF16), dma_sems(2, 8), dma_sems(2, 8)]
    anywhere = pl.BlockSpec(memory_space=pl.ANY)
    return pl.pallas_call(
        functools.partial(layer_kernel, last_layer),
        out_shape=(jax.ShapeDtypeStruct((n_tok, dim), BF16),) + extra_shapes + (grad_shape,) * 3,
        grid_spec=pltpu.PrefetchScalarGridSpec(
            num_scalar_prefetch=0, grid=(3 * groups,),
            in_specs=[anywhere, block] + [anywhere] * 7 + [square],
            out_specs=(block,) + extra_specs + (anywhere,) * 3,
            scratch_shapes=scratch),
        compiler_params=pltpu.CompilerParams(dimension_semantics=('arbitrary',), vmem_limit_bytes=67043328,
                                             collective_id=1 + int(last_layer), has_side_effects=True),
    )(whole, mine, rank, gate, x_own, dense, w_gate, w_up, w_down, other)


def settle_kernel(chunks, *refs):
    n = len(chunks)
    sources, outs, bufs = refs[:n], refs[n:2 * n], refs[2 * n:3 * n]
    in_sem, out_sem = refs[3 * n:]
    loads, stores = [], []
    for src, out, buf, count in zip(sources, outs, bufs, chunks):
        rows = src.shape[0] // count
        for at in range(count):
            here = pl.ds(at * rows, rows)
            loads.append(pltpu.make_async_copy(src.at[here], buf.at[here], in_sem.at[len(loads)]))
            stores.append(pltpu.make_async_copy(buf.at[here], out.at[here], out_sem.at[len(stores)]))
    for load in loads:
        load.start()
    for load, store in zip(loads, stores):
        load.wait()
        store.start()
    for store in stores:
        store.wait()


def settle(*arrays):
    chunks = tuple(8 if array.ndim == 3 else 1 for array in arrays)
    anywhere = pl.BlockSpec(memory_space=pl.ANY)
    return pl.pallas_call(
        functools.partial(settle_kernel, chunks),
        out_shape=tuple(jax.ShapeDtypeStruct(array.shape, array.dtype) for array in arrays),
        in_specs=[anywhere] * len(arrays), out_specs=(anywhere,) * len(arrays),
        scratch_shapes=[pltpu.VMEM(array.shape, array.dtype) for array in arrays] + [dma_sems(sum(chunks))] * 2,
        compiler_params=pltpu.CompilerParams(vmem_limit_bytes=67043328),
    )(*arrays)


def solution(mesh):
    fine = Mesh(mesh.devices.reshape(2, CHIPS, CORES), ('y', 'x', 'c'))
    tok_spec = P(ALL, None)
    exp_spec = P('y', None, None)
    layer_specs = (P(None, None), tok_spec, tok_spec, exp_spec, exp_spec, exp_spec)
    grad_specs = (P(ALL, None), P('y', ('x', 'c'), None), P('y', ('x', 'c'), None), P('y', None, ('x', 'c')))

    def local_step(tokens, dy_out, dense_w1, route_idx1, route_gate1, w_gate1, w_up1, w_down1, dense_w2, route_idx2, route_gate2, w_gate2, w_up2, w_down2):
        w_gate1, w_up1, w_gate2, w_up2 = (jnp.swapaxes(w, 1, 2) for w in (w_gate1, w_up1, w_gate2, w_up2))
        y_one, u_two, u_all, dy_all, rank1, gate1, rank2, gate2 = layer_forward(
            tokens, dy_out, route_idx1.T, route_idx2.T, route_gate1.T, route_gate2.T, dense_w1, dense_w2, w_gate1, w_up1, w_down1)
        grad_mid, part_two, *grads_two = layer_backward(
            False, dy_all, u_two, rank2, gate2, y_one, dense_w2, w_gate2, w_up2, w_down2, dy_out)
        grad_tok, dense_one, dense_two, *grads_one = layer_backward(
            True, u_all, grad_mid, rank1, gate1, tokens, dense_w1, w_gate1, w_up1, w_down1, part_two)
        (grad_tok, dense_one, gate_one, up_one, down_one, dense_two, gate_two, up_two, down_two) = settle(
            grad_tok, dense_one, *grads_one, dense_two, *grads_two)
        gate_one, up_one, gate_two, up_two = (jnp.swapaxes(g, 1, 2) for g in (gate_one, up_one, gate_two, up_two))
        return (grad_tok, dense_one, gate_one, up_one, down_one, dense_two, gate_two, up_two, down_two)

    return jax.shard_map(local_step, mesh=fine, in_specs=(tok_spec, tok_spec) + layer_specs + layer_specs,
                         out_specs=(tok_spec,) + grad_specs + grad_specs, check_vma=False)
```

```python
import functools

import jax
import jax.numpy as jnp
from jax import lax
from jax.experimental import pallas as pl
from jax.experimental.pallas import tpu as pltpu
from jax.sharding import Mesh, PartitionSpec as P

F32 = jnp.float32
BF16 = jnp.bfloat16
CAP = 64
GROUP = 8
LANES = 256
CORES = 2
CHIPS = 2
ALL = ('x', 'c', 'y')
MESH = pl.DeviceIdType.MESH
FLIPS = ((0, 0), (0, 0), (0, 1), (0, 0), (0, 1), (1, 0), (1, 1))
ROUTE = 'yxxcccc'


def matmul(lhs, rhs, lhs_dim=1, rhs_dim=0):
    return lax.dot_general(lhs, rhs, (((lhs_dim,), (rhs_dim,)), ((), ())), preferred_element_type=F32)


def position():
    return tuple(lax.axis_index(name) for name in ALL)


def send(src, dst, sems, at, axis):
    return pltpu.make_async_remote_copy(src, dst, sems[0].at[at], sems[1].at[at],
                                        device_id={axis: 1 - lax.axis_index(axis)}, device_id_type=MESH)


def spreader(mine_ref, peer_ref, sems):
    ix, ic, iy = position()

    def copy(at):
        flip_x, flip_y = FLIPS[at]
        x = 1 - ix if flip_x else ix
        y = 1 - iy if flip_y else iy
        block = peer_ref.at[(x * CORES + ic) * 2 + y]
        return send(block if flip_x or flip_y else mine_ref, block, sems, at, ROUTE[at])

    return copy


def adder(p_ref, rs_ref, sems):
    ix, ic, iy = position()

    def copy(at):
        part = ((1 - ic) * 2 + 1 - iy, (1 - ic) * 2 + iy, ic * 2 + 1 - iy)[at]
        return send(p_ref.at[part], rs_ref.at[at], sems, at, 'ccy'[at])

    return copy


def greet(everyone):
    barrier = pltpu.get_barrier_semaphore()
    if everyone:
        others = [target(hop) for hop in range(1, 8)]
    else:
        others = [{axis: 1 - lax.axis_index(axis)} for axis in ALL]
    for other in others:
        pl.semaphore_signal(barrier, inc=1, device_id=other, device_id_type=MESH)
    pl.semaphore_wait(barrier, len(others))


def rank_of(x, c, y):
    return (x * CORES + c) * 2 + y


def target(hop):
    goal = lax.rem(rank_of(*position()) + hop, 8)
    return {'x': lax.div(goal, 4), 'c': lax.rem(lax.div(goal, 2), 2), 'y': lax.rem(goal, 2)}


def weight_copies(sources, w_ref, sems, step, n_group):
    slot = lax.rem(step, 2)
    rows = pl.ds((lax.axis_index('c') * n_group + lax.rem(step, n_group)) * GROUP, GROUP)
    return [pltpu.make_async_copy(src.at[rows], w_ref.at[slot, kind], sems.at[slot, kind]) for kind, src in enumerate(sources)]


def next_weights(sources, w_ref, sems, n_group, n_step):
    step = pl.program_id(0)

    @pl.when(step + 1 < n_step)
    def _():
        for copy in weight_copies(sources, w_ref, sems, step + 1, n_group):
            copy.start()

    for copy in weight_copies(sources, w_ref, sems, step, n_group):
        copy.wait()


def at_step(number):
    return pl.when(pl.program_id(0) == number)


def side_by_side(first, second):
    pad = jnp.zeros((LANES - first.shape[0], first.shape[1]), first.dtype)
    return jnp.concatenate([first, pad, second, pad], axis=0)


def select_rows(rank_ref, gate_ref, group, src):
    n_tok = rank_ref.shape[-1]
    slot = lax.broadcasted_iota(jnp.int32, (CAP, n_tok), 0)
    picks, gates = [], []
    for exp in range(GROUP):
        row = pl.ds(group * GROUP + exp, 1)
        hit = slot == rank_ref[src, row, :]
        picks.append(jnp.where(hit, 1.0, 0.0).astype(BF16))
        gates.append(jnp.sum(jnp.where(hit, gate_ref[src, row, :], 0.0), axis=1, keepdims=True))
    return jnp.concatenate(picks, axis=0), jnp.concatenate(gates, axis=0)


def route_table(route_ref, before_ref, src, layer, rank_ref, gate_ref, n_exp):
    _, ic, iy = position()
    n_tok = route_ref.shape[-1]
    experts = ((iy * CORES + ic) * n_exp + lax.broadcasted_iota(jnp.int32, (n_exp, n_tok), 0)).astype(F32)
    member = jnp.zeros((n_exp, n_tok), F32)
    gates = jnp.zeros((n_exp, n_tok), F32)
    for top in range(8):
        hit = experts == route_ref[src, layer * 8 + top:layer * 8 + top + 1, :]
        member = jnp.where(hit, 1.0, member)
        gates = jnp.where(hit, route_ref[src, 16 + layer * 8 + top:17 + layer * 8 + top, :], gates)
    count = matmul(member.astype(BF16), before_ref[...])
    rank_ref[src] = jnp.where(member > 0.0, count, -1.0).astype(jnp.int32)
    gate_ref[src] = gates


def forward_kernel(tok_ref, grad_ref, idx1_ref, idx2_ref, top1_ref, top2_ref, mix_ref, dense_ref, wg_hbm, wu_hbm, wd_hbm,
                   y_ref, u_ref, uall_ref, dall_ref, rank1_ref, gate1_ref, rank2_ref, gate2_ref,
                   raw_ref, us_ref, ds_ref, routes_ref, route_ref, before_ref, pick_ref, row_ref, x_ref, part_ref, p_ref, rs_ref,
                   w_ref, w_sem, u_send, u_recv, d_send, d_recv, t_send, t_recv, rs_send, rs_recv, out_sem):
    n_exp, n_tok = rank1_ref.shape[1:]
    n_group = n_exp // GROUP
    step = pl.program_id(0)
    ix, ic, iy = position()
    me = rank_of(ix, ic, iy)
    spread_u = spreader(tok_ref, raw_ref, (u_send, u_recv))
    spread_d = spreader(grad_ref, ds_ref, (d_send, d_recv))
    spread_t = spreader(routes_ref, route_ref, (t_send, t_recv))
    add_up = adder(p_ref, rs_ref, (rs_send, rs_recv))
    stores = ((us_ref, uall_ref), (ds_ref, dall_ref))
    weights = (wg_hbm, wu_hbm, wd_hbm)
    wg_ref, wu_ref, wd_ref = (w_ref.at[lax.rem(step, 2), kind] for kind in range(3))

    def mixed(x):
        return (x.astype(F32) + matmul(x, mix_ref[...])).astype(BF16)

    def pass_on(copy, arrived, onward):
        copy(arrived).wait_recv()
        for at in onward:
            copy(at).start()

    @at_step(0)
    def _():
        for copy in weight_copies(weights, w_ref, w_sem, 0, n_group):
            copy.start()
        for at, part_in in enumerate((idx1_ref, idx2_ref, top1_ref, top2_ref)):
            routes_ref[at * 8:at * 8 + 8, :] = part_in[...].astype(F32)
        greet(False)
        for copy in (spread_t, spread_u):
            for at in (0, 3, 1):
                copy(at).start()
        us_ref[me] = mixed(tok_ref[...])
        ds_ref[me] = grad_ref[...]
        route_ref[me] = routes_ref[...]
        p_ref[...] = jnp.zeros_like(p_ref)
        before_ref[...] = jnp.where(lax.broadcasted_iota(jnp.int32, (n_tok, n_tok), 0)
                                    < lax.broadcasted_iota(jnp.int32, (n_tok, n_tok), 1), 1.0, 0.0).astype(BF16)
        pass_on(spread_t, 0, (4, 2))
        spread_u(3).wait_recv()
        us_ref[rank_of(ix, 1 - ic, iy)] = mixed(raw_ref[rank_of(ix, 1 - ic, iy)])
        spread_t(3).wait_recv()
        spread_t(4).wait_recv()

        @pl.loop(0, 4)
        def _(src):
            route_table(route_ref, before_ref, ix * 4 + src, 0, rank1_ref, gate1_ref, n_exp)

        pass_on(spread_u, 0, (4, 2))
        for at in (0, 3, 1):
            spread_d(at).start()
        us_ref[rank_of(ix, ic, 1 - iy)] = mixed(raw_ref[rank_of(ix, ic, 1 - iy)])
        spread_u(4).wait_recv()
        us_ref[rank_of(ix, 1 - ic, 1 - iy)] = mixed(raw_ref[rank_of(ix, 1 - ic, 1 - iy)])

    @at_step(n_group // 4)
    def _():
        pass_on(spread_t, 1, (5,))
        pass_on(spread_u, 1, (5,))

    @at_step(n_group // 2)
    def _():
        pass_on(spread_t, 2, (6,))
        pass_on(spread_u, 2, (6,))
        pass_on(spread_d, 0, (4, 2))

    @at_step(n_group + 1)
    def _():
        for copy in (spread_t, spread_u):
            copy(5).wait_recv()
            copy(6).wait_recv()

        @pl.loop(0, 4)
        def _(src):
            us_ref[(1 - ix) * 4 + src] = mixed(raw_ref[(1 - ix) * 4 + src])
            route_table(route_ref, before_ref, (1 - ix) * 4 + src, 0, rank1_ref, gate1_ref, n_exp)

        @pl.loop(0, 8)
        def _(src):
            route_table(route_ref, before_ref, src, 1, rank2_ref, gate2_ref, n_exp)

    @at_step(n_group)
    def _():
        add_up(0).start()

    @at_step(n_group + n_group // 2)
    def _():
        pass_on(spread_d, 1, (5,))

    @at_step(2 * n_group - 2)
    def _():
        pass_on(spread_d, 2, (6,))
        pltpu.make_async_copy(us_ref, uall_ref, out_sem.at[0]).start()

    @at_step(2 * n_group - 1)
    def _():
        for at in (3, 4, 5, 6):
            spread_d(at).wait_recv()
        pltpu.make_async_copy(ds_ref, dall_ref, out_sem.at[1]).start()

    next_weights(weights, w_ref, w_sem, n_group, 2 * n_group)
    group = lax.rem(step, n_group)
    far = 1 - lax.div(step, n_group)
    y_now = jnp.where(far == 1, 1 - iy, iy)

    for core in range(CORES):
        src = rank_of(ix, core, y_now)
        pick, gate = select_rows(rank1_ref, gate1_ref, group, src)
        pick_ref[core] = pick
        rows = matmul(pick, us_ref[src]).astype(BF16)
        at = slice(core * CAP, (core + 1) * CAP)
        for exp in range(GROUP):
            x_ref[exp, at, :] = rows[exp * CAP:(exp + 1) * CAP]
            row_ref[exp, at, :] = jnp.broadcast_to(gate[exp * CAP:(exp + 1) * CAP], (CAP, 128))

    @at_step(n_group)
    def _():
        add_up(0).wait_recv()
        p_ref[ic * 2 + 1 - iy] += rs_ref[0]
        add_up(2).start()

    ff = wg_ref.shape[1]
    pre = {}
    for tick in range(GROUP + 2):
        if tick < GROUP:
            pre[tick] = matmul(x_ref[tick], side_by_side(wg_ref[tick], wu_ref[tick]), 1, 1)
        if 0 < tick <= GROUP:
            both = pre.pop(tick - 1)
            a_pre, b_pre = both[:, :ff], both[:, LANES:LANES + ff]
            pre[tick - 1, 1] = (a_pre * jax.nn.sigmoid(a_pre) * b_pre).astype(BF16)
        if tick > 1:
            exp = tick - 2
            out = matmul(pre.pop((exp, 1)), wd_ref[exp]).astype(BF16).astype(F32) * row_ref[exp][:, :1]
            high = out.astype(BF16)
            rest = out - high.astype(F32)
            mid = rest.astype(BF16)
            low = (rest - mid.astype(F32)).astype(BF16)
            at = slice(exp * CAP, (exp + 1) * CAP)
            for core in range(CORES):
                here = slice(core * CAP, (core + 1) * CAP)
                part_ref[core, 0, at, :] = high[here]
                part_ref[core, 1, at, :] = mid[here]
                part_ref[core, 2, at, :] = low[here]

    for core in range(CORES):
        pick = pick_ref[core]
        total = matmul(pick, part_ref[core, 0], 0, 0)
        total += matmul(pick, part_ref[core, 1], 0, 0) + matmul(pick, part_ref[core, 2], 0, 0)
        p_ref[core * 2 + y_now] += total

    @at_step(2 * n_group - 1)
    def _():
        add_up(1).start()
        add_up(1).wait_recv()
        add_up(2).wait_recv()
        y_own = (us_ref[me].astype(F32) + (p_ref[ic * 2 + iy] + rs_ref[1] + rs_ref[2])).astype(BF16)
        y_ref[...] = y_own
        u_ref[...] = (y_own.astype(F32) + matmul(y_own, dense_ref[...])).astype(BF16)
        for copy in (spread_u, spread_d, spread_t):
            for at in range(7):
                copy(at).wait_send()
        for at in range(3):
            add_up(at).wait_send()
        for at in range(2):
            pltpu.make_async_copy(*stores[at], out_sem.at[at]).wait()


def layer_kernel(last_layer, *refs):
    refs = list(refs)
    whole_hbm, mine_ref, rank_hbm, gate_hbm, x_own_ref, dense_ref, *weights, other_ref = refs[:10]
    del refs[:10]
    grad_own_ref = mine_ref if last_layer else other_ref
    if last_layer:
        one_ref, two_ref = refs[1:3]
        del refs[1:3]
    else:
        part_ref = refs.pop(1)
    gx_out_ref, gg_ref, gu_ref, gd_ref = refs[:4]
    (peer_ref, xo_ref, do_ref, h_ref, ga_ref, gb_ref, pick_ref, gx_ref, p_ref, rs_ref, x_ref, d_ref, stage_ref,
     ag_send, ag_recv, rs_send, rs_recv, keep_sem, give_send, give_recv, late_sem,
     whole_ref, rank_ref, gate_ref, w_ref, w_sem, load_sem) = refs[4:31]
    late_copies = [pltpu.make_async_copy(src, pick_ref.at[at], late_sem.at[at]) for at, src in enumerate((x_own_ref, dense_ref))]
    if last_layer:
        part_ref = gx_ref.at[0]
        land_ref, land_send, land_recv = refs[31:]
    n_src, _, dim = whole_ref.shape
    own = n_src // CHIPS
    n_group = xo_ref.shape[0] // GROUP
    n_first = 2 * n_group
    n_step = 3 * n_group
    half = dim // CHIPS
    piece = half // CORES
    step = pl.program_id(0)
    ix, ic, iy = position()
    cols = pl.ds(pl.multiple_of(ix * half, half), half)
    wg_ref, wu_ref, wd_ref = (w_ref.at[lax.rem(step, 2), kind] for kind in range(3))
    loads = [pltpu.make_async_copy(src, dst, load_sem.at[at]) for at, (src, dst) in enumerate(
        ((rank_hbm, rank_ref), (gate_hbm, gate_ref), (whole_hbm.at[pl.ds(ix * own, own)], whole_ref.at[pl.ds(ix * own, own)])))]
    far_rows = pl.ds((1 - ix) * own, own)
    far_load = pltpu.make_async_copy(whole_hbm.at[far_rows], whole_ref.at[far_rows], load_sem.at[3])
    u_ref, dy_ref = (whole_ref, peer_ref) if last_layer else (peer_ref, whole_ref)
    outs = (gg_ref, gu_ref, gd_ref)
    spread = spreader(mine_ref, peer_ref, (ag_send, ag_recv))
    add_up = adder(p_ref, rs_ref, (rs_send, rs_recv))

    def land_copy(layer, hop):
        goal = target(hop)
        rows = dim // 8
        src = (part_ref, other_ref)[layer]
        at = pl.ds(pl.multiple_of(rank_of(goal['x'], goal['c'], goal['y']) * rows, rows), rows)
        return pltpu.make_async_remote_copy(src.at[at, :], land_ref.at[layer, hop], land_send.at[layer, hop],
                                            land_recv.at[layer, hop], device_id=goal, device_id_type=MESH)

    def land_sum(layer, out_ref):
        rows = dim // 8
        at = pl.ds(pl.multiple_of(rank_of(ix, ic, iy) * rows, rows), rows)
        total = (part_ref, other_ref)[layer][at, :].astype(F32)
        for hop in range(1, 8):
            land_copy(layer, hop).wait_recv()
            total += land_ref[layer, hop].astype(F32)
        out_ref[...] = total.astype(BF16)

    def store_copies(group, moved):
        buf = lax.rem(group, 2)
        rows = pl.ds(ic * n_group * GROUP + group * GROUP, GROUP)
        for kind in range(3):
            dst = outs[kind].at[rows]
            if moved:
                yield pltpu.make_async_remote_copy(
                    stage_ref.at[buf, 1 - ic, kind], dst, give_send.at[buf, kind], give_recv.at[group, kind],
                    device_id={'c': 1 - ic}, device_id_type=MESH)
            else:
                yield pltpu.make_async_copy(stage_ref.at[buf, ic, kind], dst, keep_sem.at[buf, kind])

    def store_start(group):
        for moved in (True, False):
            for copy in store_copies(group, moved):
                copy.start()

    def store_wait(group):
        for copy in store_copies(group, True):
            copy.wait_send()
        for copy in store_copies(group, False):
            copy.wait()

    def pull(src, group, at, keep):
        pick, gate = select_rows(rank_ref, gate_ref, group, src)
        if keep:
            pick_ref[at] = pick
        x_rows = matmul(pick, u_ref[src]).astype(BF16)
        d_rows = (matmul(pick, dy_ref[src]) * gate).astype(BF16)
        for exp in range(GROUP):
            x_ref[exp, at * CAP:(at + 1) * CAP, :] = x_rows[exp * CAP:(exp + 1) * CAP]
            d_ref[exp, at * CAP:(at + 1) * CAP, :] = d_rows[exp * CAP:(exp + 1) * CAP]

    def hidden_pre(x_rows, d_rows, exp):
        ff = wg_ref.shape[1]
        both = matmul(x_rows, side_by_side(wg_ref[exp], wu_ref[exp]), 1, 1)
        return both[:, :ff], both[:, LANES:LANES + ff], matmul(d_rows, wd_ref[exp], 1, 1)

    def hidden_grads(a_pre, b_pre, back):
        sigma = jax.nn.sigmoid(a_pre)
        silu = a_pre * sigma
        grad_hidden = back.astype(BF16).astype(F32)
        grad_a = (grad_hidden * b_pre * sigma * (1.0 + a_pre * (1.0 - sigma))).astype(BF16)
        return (silu * b_pre).astype(BF16), grad_a, (grad_hidden * silu).astype(BF16)

    @at_step(0)
    def _():
        for copy in loads + weight_copies(weights, w_ref, w_sem, 0, n_group) + [far_load]:
            copy.start()
        greet(last_layer)
        for at in (0, 3, 1):
            spread(at).start()
        if last_layer:
            for hop in range(1, 8):
                land_copy(1, hop).start()
        peer_ref[rank_of(ix, ic, iy)] = mine_ref[...]
        p_ref[...] = jnp.zeros_like(p_ref)
        for copy in loads:
            copy.wait()
        spread(3).wait_recv()

    next_weights(weights, w_ref, w_sem, n_group, n_step)

    @at_step(n_group - 1)
    def _():
        spread(0).wait_recv()
        spread(4).start()
        spread(2).start()

    @at_step(n_group)
    def _():
        spread(4).wait_recv()

    @at_step(n_group + n_group // 2)
    def _():
        spread(1).wait_recv()
        spread(5).start()

    @at_step(n_first - 1)
    def _():
        spread(2).wait_recv()
        spread(6).start()

    @pl.when(step < n_first)
    def _():
        group = lax.rem(step, n_group)
        late = lax.div(step, n_group)
        y_now = jnp.where(late == 1, 1 - iy, iy)
        base = group * GROUP
        rows = pl.ds(pl.multiple_of(late * CORES * CAP, CORES * CAP), CORES * CAP)

        for core in range(CORES):
            pull(rank_of(ix, core, y_now), group, core, True)

        near = CORES * CAP
        pre = {}
        for tick in range(GROUP + 2):
            if tick < GROUP:
                pre[tick] = hidden_pre(x_ref[tick, :near, :], d_ref[tick, :near, :], tick)
            if 0 < tick <= GROUP:
                exp = tick - 1
                hidden, grad_a, grad_b = hidden_grads(*pre.pop(exp))
                xo_ref[base + exp, rows, :] = x_ref[exp, :near, cols]
                do_ref[base + exp, rows, :] = d_ref[exp, :near, cols]
                h_ref[base + exp, rows, :] = hidden
                ga_ref[base + exp, rows, :] = grad_a
                gb_ref[base + exp, rows, :] = grad_b
                pre[exp, 1] = None
            if tick > 1:
                exp = tick - 2
                grad_x = (matmul(ga_ref[base + exp, rows, :], wg_ref[exp]) + matmul(gb_ref[base + exp, rows, :], wu_ref[exp])).astype(BF16)
                at = slice(exp * CAP, (exp + 1) * CAP)
                for core in range(CORES):
                    gx_ref[core, at, :] = grad_x[core * CAP:(core + 1) * CAP]

        for core in range(CORES):
            p_ref[core * 2 + y_now] += matmul(pick_ref[core], gx_ref[core], 0, 0)

    @at_step(n_first)
    def _():
        add_up(0).start()
        add_up(1).start()
        far_load.wait()
        spread(5).wait_recv()
        spread(6).wait_recv()
        for copy in late_copies:
            copy.start()

    @pl.when(step >= n_first)
    def _():
        group = step - n_first

        @pl.when(group >= 2)
        def _():
            store_wait(group - 2)

        @pl.when(group >= 1)
        def _():
            store_start(group - 1)

        for src in range(own):
            pull((1 - ix) * own + src, group, src, False)

        @at_step(n_first)
        def _():
            add_up(0).wait_recv()
            p_ref[ic * 2 + 1 - iy] += rs_ref[0]
            add_up(2).start()

        @at_step(n_step - 1)
        def _():
            for copy in late_copies:
                copy.wait()
            add_up(1).wait_recv()
            add_up(2).wait_recv()
            total = p_ref[ic * 2 + iy] + rs_ref[1] + rs_ref[2]
            grad = (grad_own_ref[...].astype(F32) + total).astype(BF16)
            part_ref[...] = matmul(pick_ref[0], grad, 0, 0).astype(BF16)
            gx_out_ref[...] = (grad.astype(F32) + matmul(grad, pick_ref[1], 1, 1)).astype(BF16)
            if last_layer:
                for hop in range(1, 8):
                    land_copy(0, hop).start()

        buf = lax.rem(group, 2)

        pre = {}
        for tick in range(GROUP + 2):
            if tick < GROUP:
                pre[tick] = hidden_pre(x_ref[tick], d_ref[tick], tick)
            if 0 < tick <= GROUP:
                exp = tick - 1
                pre[exp, 1] = hidden_grads(*pre.pop(exp))
            if tick > 1:
                exp = tick - 2
                base = group * GROUP + exp
                hidden, grad_a, grad_b = pre.pop((exp, 1))
                x_own, x_far = xo_ref[base], x_ref[exp, :, cols]
                d_own, d_far = do_ref[base], d_ref[exp, :, cols]
                grads = (matmul(ga_ref[base], x_own, 0, 0) + matmul(grad_a, x_far, 0, 0),
                         matmul(gb_ref[base], x_own, 0, 0) + matmul(grad_b, x_far, 0, 0),
                         matmul(h_ref[base], d_own, 0, 0) + matmul(hidden, d_far, 0, 0))
                for kind in range(3):
                    for core in range(CORES):
                        stage_ref[buf, core, kind, exp] = grads[kind][:, core * piece:(core + 1) * piece].astype(BF16)

    @at_step(n_step - 1)
    def _():
        last = n_group - 1
        store_wait(last - 1)
        store_start(last)
        if last_layer:
            land_sum(1, two_ref)
            land_sum(0, one_ref)
            for layer in range(2):
                for hop in range(1, 8):
                    land_copy(layer, hop).wait_send()
        for at in range(7):
            spread(at).wait_send()
        for at in range(3):
            add_up(at).wait_send()
        store_wait(last)
        for group in range(n_group):
            for copy in store_copies(group, True):
                copy.wait_recv()


def fixed(*shape):
    return pl.BlockSpec(shape, lambda s: (0,) * len(shape), pipeline_mode=pl.Buffered(1))


def dma_sems(*shape):
    return pltpu.SemaphoreType.DMA(shape)


def sums_scratch(own, n_tok, dim):
    return [pltpu.VMEM((own, n_tok, dim), F32), pltpu.VMEM((3, n_tok, dim), F32)]


def layer_forward(tokens, grad, idx1, idx2, top1, top2, dense1, dense2, w_gate, w_up, w_down):
    n_tok, dim = tokens.shape
    top = idx1.shape[0]
    n_all, ff, _ = w_gate.shape
    n_exp = n_all // CORES
    n_src = 8
    own = n_src // CHIPS
    groups = n_exp // GROUP
    table = fixed(n_src, n_exp, n_tok)
    block = jax.ShapeDtypeStruct((n_tok, dim), BF16)
    every = jax.ShapeDtypeStruct((n_src, n_tok, dim), BF16)
    ranks = jax.ShapeDtypeStruct((n_src, n_exp, n_tok), jnp.int32)
    gates = jax.ShapeDtypeStruct((n_src, n_exp, n_tok), F32)
    anywhere = pl.BlockSpec(memory_space=pl.ANY)
    rows = CORES * CAP
    return pl.pallas_call(
        forward_kernel,
        out_shape=(block, block, every, every, ranks, gates, ranks, gates),
        grid_spec=pltpu.PrefetchScalarGridSpec(
            num_scalar_prefetch=0, grid=(2 * groups,),
            in_specs=[fixed(n_tok, dim)] * 2 + [fixed(top, n_tok)] * 4 + [fixed(dim, dim)] * 2 + [anywhere] * 3,
            out_specs=(fixed(n_tok, dim), fixed(n_tok, dim), anywhere, anywhere, table, table, table, table),
            scratch_shapes=[pltpu.VMEM((n_src, n_tok, dim), BF16)] * 3
            + [pltpu.VMEM((4 * top, n_tok), F32), pltpu.VMEM((n_src, 4 * top, n_tok), F32), pltpu.VMEM((n_tok, n_tok), BF16),
                            pltpu.VMEM((CORES, GROUP * CAP, n_tok), BF16), pltpu.VMEM((GROUP, rows, 128), F32),
                            pltpu.VMEM((GROUP, rows, dim), BF16), pltpu.VMEM((CORES, 3, GROUP * CAP, dim), BF16)]
            + sums_scratch(own, n_tok, dim)
            + [pltpu.VMEM((2, 3, GROUP, ff, dim), BF16), dma_sems(2, 3)]
            + [dma_sems(7)] * 6 + [dma_sems(3)] * 2 + [dma_sems(2)]),
        compiler_params=pltpu.CompilerParams(dimension_semantics=('arbitrary',), vmem_limit_bytes=62 << 20,
                                             collective_id=0, has_side_effects=True),
    )(tokens, grad, idx1, idx2, top1, top2, dense1, dense2, w_gate, w_up, w_down)


def layer_backward(last_layer, whole, mine, rank, gate, x_own, dense, w_gate, w_up, w_down, other):
    n_src, n_tok, dim = whole.shape
    n_all, ff, _ = w_gate.shape
    n_exp = rank.shape[1]
    own = n_src // CHIPS
    piece = dim // (CHIPS * CORES)
    groups = n_exp // GROUP
    kept = own * CAP
    block = fixed(n_tok, dim)
    square = fixed(dim, dim)
    slab = fixed(dim // 8, dim)
    grad_shape = jax.ShapeDtypeStruct((n_all, ff, piece), BF16)
    part_shape = jax.ShapeDtypeStruct((dim, dim), BF16)
    slab_shape = jax.ShapeDtypeStruct((dim // 8, dim), BF16)
    extra_shapes = (slab_shape, slab_shape) if last_layer else (part_shape,)
    extra_specs = (slab, slab) if last_layer else (square,)
    half = dim // CHIPS
    scratch = [pltpu.VMEM((n_src, n_tok, dim), BF16), pltpu.VMEM((n_exp, kept, half), BF16),
               pltpu.VMEM((n_exp, kept, half), BF16), pltpu.VMEM((n_exp, kept, ff), BF16),
               pltpu.VMEM((n_exp, kept, ff), BF16), pltpu.VMEM((n_exp, kept, ff), BF16),
               pltpu.VMEM((CORES, GROUP * CAP, n_tok), BF16), pltpu.VMEM((CORES, GROUP * CAP, dim), BF16)]
    scratch += sums_scratch(own, n_tok, dim)
    scratch += [pltpu.VMEM((GROUP, kept, dim), BF16), pltpu.VMEM((GROUP, kept, dim), BF16),
                pltpu.VMEM((2, CORES, 3, GROUP, ff, piece), BF16),
                dma_sems(7), dma_sems(7), dma_sems(3), dma_sems(3), dma_sems(2, 3), dma_sems(2, 3), dma_sems(groups, 3), dma_sems(2),
                pltpu.VMEM((n_src, n_tok, dim), BF16), pltpu.VMEM(rank.shape, rank.dtype), pltpu.VMEM(gate.shape, gate.dtype),
                pltpu.VMEM((2, 3, GROUP, ff, dim), BF16), dma_sems(2, 3), dma_sems(4)]
    if last_layer:
        scratch += [pltpu.VMEM((2, 8, dim // 8, dim), BF16), dma_sems(2, 8), dma_sems(2, 8)]
    anywhere = pl.BlockSpec(memory_space=pl.ANY)
    return pl.pallas_call(
        functools.partial(layer_kernel, last_layer),
        out_shape=(jax.ShapeDtypeStruct((n_tok, dim), BF16),) + extra_shapes + (grad_shape,) * 3,
        grid_spec=pltpu.PrefetchScalarGridSpec(
            num_scalar_prefetch=0, grid=(3 * groups,),
            in_specs=[anywhere, block] + [anywhere] * 7 + [square],
            out_specs=(block,) + extra_specs + (anywhere,) * 3,
            scratch_shapes=scratch),
        compiler_params=pltpu.CompilerParams(dimension_semantics=('arbitrary',), vmem_limit_bytes=67043328,
                                             collective_id=1 + int(last_layer), has_side_effects=True),
    )(whole, mine, rank, gate, x_own, dense, w_gate, w_up, w_down, other)


def settle_kernel(chunks, *refs):
    n = len(chunks)
    sources, outs, bufs = refs[:n], refs[n:2 * n], refs[2 * n:3 * n]
    in_sem, out_sem = refs[3 * n:]
    loads, stores = [], []
    for src, out, buf, count in zip(sources, outs, bufs, chunks):
        rows = src.shape[0] // count
        for at in range(count):
            here = pl.ds(at * rows, rows)
            loads.append(pltpu.make_async_copy(src.at[here], buf.at[here], in_sem.at[len(loads)]))
            stores.append(pltpu.make_async_copy(buf.at[here], out.at[here], out_sem.at[len(stores)]))
    for load in loads:
        load.start()
    for load, store in zip(loads, stores):
        load.wait()
        store.start()
    for store in stores:
        store.wait()


def settle(*arrays):
    chunks = tuple(8 if array.ndim == 3 else 1 for array in arrays)
    anywhere = pl.BlockSpec(memory_space=pl.ANY)
    return pl.pallas_call(
        functools.partial(settle_kernel, chunks),
        out_shape=tuple(jax.ShapeDtypeStruct(array.shape, array.dtype) for array in arrays),
        in_specs=[anywhere] * len(arrays), out_specs=(anywhere,) * len(arrays),
        scratch_shapes=[pltpu.VMEM(array.shape, array.dtype) for array in arrays] + [dma_sems(sum(chunks))] * 2,
        compiler_params=pltpu.CompilerParams(vmem_limit_bytes=67043328),
    )(*arrays)


def solution(mesh):
    fine = Mesh(mesh.devices.reshape(2, CHIPS, CORES), ('y', 'x', 'c'))
    tok_spec = P(ALL, None)
    exp_spec = P('y', None, None)
    layer_specs = (P(None, None), tok_spec, tok_spec, exp_spec, exp_spec, exp_spec)
    grad_specs = (P(ALL, None), P('y', ('x', 'c'), None), P('y', ('x', 'c'), None), P('y', None, ('x', 'c')))

    def local_step(tokens, dy_out, dense_w1, route_idx1, route_gate1, w_gate1, w_up1, w_down1, dense_w2, route_idx2, route_gate2, w_gate2, w_up2, w_down2):
        w_gate1, w_up1, w_gate2, w_up2 = (jnp.swapaxes(w, 1, 2) for w in (w_gate1, w_up1, w_gate2, w_up2))
        y_one, u_two, u_all, dy_all, rank1, gate1, rank2, gate2 = layer_forward(
            tokens, dy_out, route_idx1.T, route_idx2.T, route_gate1.T, route_gate2.T, dense_w1, dense_w2, w_gate1, w_up1, w_down1)
        grad_mid, part_two, *grads_two = layer_backward(
            False, dy_all, u_two, rank2, gate2, y_one, dense_w2, w_gate2, w_up2, w_down2, dy_out)
        grad_tok, dense_one, dense_two, *grads_one = layer_backward(
            True, u_all, grad_mid, rank1, gate1, tokens, dense_w1, w_gate1, w_up1, w_down1, part_two)
        (grad_tok, dense_one, gate_one, up_one, down_one, dense_two, gate_two, up_two, down_two) = settle(
            grad_tok, dense_one, *grads_one, dense_two, *grads_two)
        gate_one, up_one, gate_two, up_two = (jnp.swapaxes(g, 1, 2) for g in (gate_one, up_one, gate_two, up_two))
        return (grad_tok, dense_one, gate_one, up_one, down_one, dense_two, gate_two, up_two, down_two)

    return jax.shard_map(local_step, mesh=fine, in_specs=(tok_spec, tok_spec) + layer_specs + layer_specs,
                         out_specs=(tok_spec,) + grad_specs + grad_specs, check_vma=False)
```
